128 devices in a mesh: row: 8 (over x, core), col: 16 (over z, y).
Axes of the slice: x: 4, y: 4, z: 4, core: 2. Of those that a mesh axis runs over, the one named last changes fastest.
Arguments:
- blocks: float32 [16384, 9216], P(('row', 'col')), may hold values from -6 to 20, as said below
- connect: int32 [16384, 96], P(('row', 'col')), may hold values from 0 to 32767, as said below
- owner_map: int32 [16384], P(('row', 'col')), may hold values from 0 to 127, as said below
- right_side: float32 [32768, 2048], P(('row', 'col')), may hold values from -1000 to 1000
Outputs:
- solution: float32 [32768, 2048], P(('row', 'col'))
- residual: float32 [32768, 2048], P(('row', 'col'))
The draws below stay inside these ranges and needn't reach their ends.
Inputs may be any that keep to these rules, and one draw needn't show every extreme that they name: `blocks`: each row, read as a 96 x 96 matrix, is symmetric positive definite. `connect`: the 96 ids of a subdomain are distinct and lie among the 512 ids that begin at 256 times its owner, counted modulo 32768. `owner_map`: among the subdomains of one device, no owner is named more than 2 times, and some owner exactly 2 times.
All inputs are finite; a program needn't handle non-finite values.
Results may differ from the reference program's by a relative error of at most 0.0003.
Values sent between devices are 32-bit elements; how exact they have to be, the bound alone decides.
No kernel may reach another device: no remote copies, remote signals or barrier semaphores. Data moves between devices by JAX's collectives and lax.ppermute only.
A program may use at most 128 MiB of HBM per device.

```python
import math
import jax
import jax.numpy as jnp
from jax import lax

NSUB = 96
NCD = 256
SUB_DEV = 128
NRHS = 2048
ITERS = 3
CAP = 2
SUBS = 16384
NC = 32768
N_ROW = 8
N_COL = 16


def owner_block(key):
    slot_total = N_ROW * N_COL * CAP
    key_one, key_two = jax.random.split(key)
    shuffled = jax.random.permutation(key_one, slot_total).astype(jnp.int32)
    first_slot = shuffled[0]
    partner = first_slot // CAP * CAP + (first_slot % CAP + 1) % CAP
    ordering = jnp.argsort((shuffled == partner).astype(jnp.int32), stable=True)
    remaining = shuffled[ordering]
    chosen = jnp.concatenate([jnp.stack([first_slot, partner]), remaining[1:SUB_DEV - 1]])
    placing = jax.random.permutation(key_two, SUB_DEV)
    return (chosen[placing] // CAP).astype(jnp.int32)


def owner_all(key):
    key_list = jax.random.split(jax.random.fold_in(key, 11), N_ROW * N_COL)
    return jax.vmap(owner_block)(key_list).reshape(-1).astype(jnp.int32)


def window_draw(one_key):
    return jax.random.permutation(one_key, 2 * NCD)[:NSUB].astype(jnp.int32)


def draw_owner_map(key, part):
    return owner_all(key)


def draw_connect(key, part):
    owners = owner_all(key)
    key_list = jax.random.split(jax.random.fold_in(key, 12), SUBS)
    window_ids = jax.vmap(window_draw)(key_list)
    return ((owners[:, None] * NCD + window_ids) % NC).astype(jnp.int32)


def draw_blocks(key, part):
    key_one, key_two = jax.random.split(jax.random.fold_in(key, 13))
    entries = jnp.clip(jax.random.normal(key_one, (SUBS, NSUB, NSUB), jnp.float32), -4.0, 4.0)
    weight = jnp.exp(jax.random.uniform(key_two, (SUBS,), jnp.float32, math.log(0.5), math.log(5.0)))
    product_part = jnp.einsum('sik,sjk->sij', entries, entries) / NSUB
    identity_mat = jnp.eye(NSUB, dtype=jnp.float32)
    coupling = identity_mat - 1.0 / NSUB
    matrices = weight[:, None, None] * coupling[None] + 0.3 * product_part + 0.05 * identity_mat[None]
    return jnp.clip(matrices, -6.0, 20.0).reshape(SUBS, NSUB * NSUB).astype(jnp.float32)


def draw_right_side(key, part):
    rows_pos = jnp.arange(NC, dtype=jnp.float32)
    growth = jnp.exp(math.log(3.0) * rows_pos / NC)[:, None]
    key_one = jax.random.fold_in(jax.random.fold_in(key, 14), 0)
    values = jnp.clip(jax.random.normal(key_one, (NC, NRHS), jnp.float32), -5.0, 5.0)
    result = values * growth * 40.0
    return jnp.clip(result, -1000.0, 1000.0).astype(jnp.float32)


def setup_inputs(seed: int = 0) -> dict:
    arg_keys = jax.random.split(jax.random.key(seed), 5)
    return {
        "blocks": draw_blocks(jax.random.fold_in(arg_keys[4], 71), 0),
        "connect": draw_connect(jax.random.fold_in(arg_keys[4], 71), 0),
        "owner_map": draw_owner_map(jax.random.fold_in(arg_keys[4], 71), 0),
        "right_side": draw_right_side(jax.random.fold_in(arg_keys[4], 71), 0),
    }


def solve_block(factor, vector):
    halfway = jax.scipy.linalg.solve_triangular(factor, vector, lower=True)
    return jax.scipy.linalg.solve_triangular(factor, halfway, lower=True, trans=1)

def reference(blocks, connect, owner_map, right_side):
    devices = N_ROW * N_COL
    window = 2 * NCD
    window_ids = ((connect - owner_map[:, None] * NCD) % NC).astype(jnp.int32)
    flat_index = (owner_map[:, None, None] * (window * window) + window_ids[:, :, None] * window + window_ids[:, None, :]).astype(jnp.int32)
    summed = jnp.zeros((devices * window * window,), jnp.float32).at[flat_index.reshape(-1)].add(blocks.reshape(-1))
    summed = summed.reshape(devices, window, window)
    upper_half = summed[:, :NCD]
    lower_half = jnp.roll(summed[:, NCD:], 1, axis=0)
    center = upper_half[:, :, :NCD] + lower_half[:, :, NCD:] + jnp.eye(NCD, dtype=jnp.float32)[None]
    band_rows = jnp.concatenate([lower_half[:, :, :NCD], center, upper_half[:, :, NCD:]], axis=2)
    factors = jax.vmap(jnp.linalg.cholesky)(center)

    def matvec(vector):
        stacked = jnp.concatenate([jnp.roll(vector, 1, axis=0), vector, jnp.roll(vector, -1, axis=0)], axis=1)
        return jnp.einsum('dij,djk->dik', band_rows, stacked, precision=lax.Precision.HIGHEST)

    def inverse(vector):
        return jax.vmap(solve_block)(factors, vector)

    def column_sums(left_vec, right_vec):
        return jnp.sum(left_vec * right_vec, axis=(0, 1))
    residual = right_side.reshape(devices, NCD, NRHS)
    solution = jnp.zeros_like(residual)
    precond = inverse(residual)
    direction = precond
    norm_now = column_sums(residual, precond)
    for iteration in range(ITERS):
        applied = matvec(direction)
        step_size = norm_now / column_sums(direction, applied)
        solution = solution + step_size * direction
        residual = residual - step_size * applied
        if iteration + 1 < ITERS:
            precond = inverse(residual)
            norm_next = column_sums(residual, precond)
            direction = precond + norm_next / norm_now * direction
            norm_now = norm_next
    return (solution.reshape(NC, NRHS), residual.reshape(NC, NRHS))
```

```python
import jax
import jax.numpy as jnp
from jax import lax
from jax.experimental import pallas as pl
from jax.experimental.pallas import tpu as pltpu
from jax.sharding import PartitionSpec as P

AXES = ("row", "col")
NB = 96
HALF = 48
ROWS = 40
GROUP = 4
HI = lax.Precision.HIGHEST
MID = lax.Precision.HIGH


def split2(x):
    high = x.astype(jnp.bfloat16)
    low = (x - high.astype(jnp.float32)).astype(jnp.bfloat16)
    return high, low


def pack_kernel(owner_ref, ids_ref, x_ref, s0_ref, s1_ref, tail_ref):
    subs = x_ref.shape[0]
    devs = s0_ref.shape[0] // ROWS
    sub = lax.broadcasted_iota(jnp.int32, (devs, subs), 0)
    here = sub == owner_ref[...]
    before = lax.broadcasted_iota(jnp.int32, (subs, subs), 0) < lax.broadcasted_iota(
        jnp.int32, (subs, subs), 1
    )
    count = jnp.dot(
        here.astype(jnp.bfloat16), before.astype(jnp.bfloat16), preferred_element_type=jnp.float32
    )
    first = jnp.where(here & (count < 0.5), 1.0, 0.0).astype(jnp.bfloat16)
    second = jnp.where(here & (count > 0.5), 1.0, 0.0).astype(jnp.bfloat16)
    pick = jnp.concatenate([first, second], axis=0)
    pick = jnp.concatenate([pick, pick], axis=1)
    lane = lax.broadcasted_iota(jnp.int32, (subs, 128), 1)

    def flat(start):
        tile, off = divmod(start, 128)
        if off == 0:
            return x_ref[:, tile * 128 : tile * 128 + 128]
        one = pltpu.roll(x_ref[:, tile * 128 : tile * 128 + 128], 128 - off, 1)
        if (tile + 1) * 128 >= x_ref.shape[1]:
            return one
        two = pltpu.roll(x_ref[:, tile * 128 + 128 : tile * 128 + 256], 128 - off, 1)
        return jnp.where(lane < 128 - off, one, two)

    diag = jnp.zeros((subs, 128), jnp.float32)

    def wrow(i, diag):
        top = flat(NB * i)
        bottom = flat(NB * (i + HALF) + HALF)
        row = jnp.where(lane < i, bottom, jnp.where(lane == i, 0.5 * top, top))
        return row, jnp.where(lane == i, 0.5 * bottom, diag)

    for m in range(8):
        row, diag = wrow(ROWS + m, diag)
        tail_ref[m] = row
    order = [i for i in range(0, ROWS, 2) if i not in (26, 28)] + [26, 28]
    kept = {}
    for i in (26, 27, 28, 29):
        kept[i], diag = wrow(i, diag)
    for i0 in order:
        tiles = []
        for i in (i0, i0 + 1):
            if i in kept:
                row = kept[i]
            else:
                row, diag = wrow(i, diag)
            if i < 24:
                extra = pltpu.roll(tail_ref[i % 8], 96 - 32 * (i // 8), 1)
            elif i < 27:
                extra = pltpu.roll(ids_ref[...], 96 - 32 * (i - 24), 1)
            elif i < 29:
                extra = pltpu.roll(diag, 96 - 32 * (i - 27), 1)
            else:
                extra = jnp.zeros_like(row)
            tiles.append(jnp.where(lane < NB, row, extra))
        high, low = split2(jnp.concatenate(tiles, axis=1))
        out = jnp.dot(
            pick, jnp.concatenate([high, low], axis=0), preferred_element_type=jnp.float32
        )
        for k in range(2):
            part = out[:, 128 * k : 128 * k + 128]
            s0_ref[pl.ds(i0 + k, devs, stride=ROWS), :] = part[:devs]
            s1_ref[pl.ds(i0 + k, devs, stride=ROWS), :] = part[devs:]


def pack(owner_map, ids, blocks, devices):
    shape = jax.ShapeDtypeStruct((devices * ROWS, 128), jnp.float32)
    return pl.pallas_call(
        pack_kernel,
        out_shape=(shape, shape),
        scratch_shapes=[pltpu.VMEM((8, blocks.shape[0], 128), jnp.float32)],
        name="pack",
    )(owner_map.reshape(1, -1), ids, blocks)


def assemble_kernel(window, finish, flag_ref, got_ref, *rest):
    if finish:
        prev_ref, out_ref, place_ref, spread_ref, list_ref, acc_ref = rest
        acc_ref[...] = prev_ref[...]
    else:
        out_ref, place_ref, spread_ref, list_ref = rest
        acc_ref = out_ref
        acc_ref[...] = jnp.zeros_like(acc_ref)
    slots = got_ref.shape[0] // ROWS

    def clear(i, last_free):
        free = flag_ref[i] == 0
        return jnp.where(free, i, last_free)

    spare = lax.fori_loop(0, slots, clear, 0)

    def note(i, count):
        list_ref[count] = i
        return count + jnp.where(flag_ref[i] > 0, 1, 0)

    count = lax.fori_loop(0, slots, note, 0)
    for k in range(GROUP):
        list_ref[count + k] = spare

    lane = lax.broadcasted_iota(jnp.int32, (HALF, 128), 1)
    row = lax.broadcasted_iota(jnp.int32, (HALF, 128), 0)
    lane1 = lax.broadcasted_iota(jnp.int32, (1, 128), 1)
    lane8 = lax.broadcasted_iota(jnp.int32, (8, 128), 1)
    target = (lax.broadcasted_iota(jnp.int32, (window, 128), 0) + 1).astype(jnp.float32)
    blank = jnp.zeros((128 - NB, 128), jnp.bfloat16)

    def step(g, carry):
        for k in range(GROUP):
            slot = list_ref[g * GROUP + k]
            base = pl.multiple_of(slot * ROWS, 8)
            got = got_ref[pl.ds(base, ROWS), :]
            r24, r25, r26 = got[24:25], got[25:26], got[26:27]
            ids = jnp.where(
                lane1 < 32,
                pltpu.roll(r24, 32, 1),
                jnp.where(
                    lane1 < 64,
                    pltpu.roll(r25, 64, 1),
                    jnp.where(lane1 < NB, pltpu.roll(r26, 96, 1), 0.0),
                ),
            )
            half_diag = jnp.where(
                lane1 < 80, pltpu.roll(got[27:28], 80, 1), pltpu.roll(got[28:29], 112, 1)
            )
            tail = jnp.where(
                lane8 < 32,
                pltpu.roll(got[0:8], 32, 1),
                jnp.where(lane8 < 64, pltpu.roll(got[8:16], 64, 1), pltpu.roll(got[16:24], 96, 1)),
            )
            full = jnp.concatenate([got, tail], axis=0)
            top = jnp.where(lane >= row, full, 0.0)
            bottom = jnp.where(
                lane == row + HALF,
                half_diag,
                jnp.where((lane >= HALF) & (lane < row + HALF), pltpu.roll(full, HALF, 1), 0.0),
            )
            high, low = split2(jnp.concatenate([top, bottom], axis=0))
            left = jnp.concatenate([high, blank, low, blank], axis=0)
            place = jnp.where(target == ids, 1.0, 0.0).astype(jnp.bfloat16)
            spread = lax.dot_general(
                left, place, (((1,), (1,)), ((), ())), preferred_element_type=jnp.float32
            )
            place_ref[:, 256 * k : 256 * k + 128] = place
            place_ref[:, 256 * k + 128 : 256 * k + 256] = place
            spread_ref[256 * k : 256 * k + 256, :] = spread.astype(jnp.bfloat16)
        acc_ref[...] += jnp.dot(
            place_ref[...], spread_ref[...], preferred_element_type=jnp.float32
        )
        return carry

    lax.fori_loop(0, (count + GROUP - 1) // GROUP, step, 0)
    if finish:
        total = acc_ref[...]
        out_ref[...] = total + total.T


def assemble(got, flags, window, prev=None):
    slots = flags.shape[0]
    finish = prev is not None
    scratch = [
        pltpu.VMEM((window, 256 * GROUP), jnp.bfloat16),
        pltpu.VMEM((256 * GROUP, window), jnp.bfloat16),
        pltpu.SMEM((slots + GROUP,), jnp.int32),
    ]
    if finish:
        scratch.append(pltpu.VMEM((window, window), jnp.float32))
    vmem = pl.BlockSpec(memory_space=pltpu.VMEM)
    return pl.pallas_call(
        lambda *refs: assemble_kernel(window, finish, *refs),
        out_shape=jax.ShapeDtypeStruct((window, window), jnp.float32),
        in_specs=[pl.BlockSpec(memory_space=pltpu.SMEM), vmem] + ([vmem] if finish else []),
        out_specs=vmem,
        scratch_shapes=scratch,
        name="assemble_last" if finish else "assemble_first",
    )(*((flags, got, prev) if finish else (flags, got)))


def inverse_kernel(upper_ref, lower_ref, out_ref, mat_ref):
    size = upper_ref.shape[0]
    eye = jnp.where(
        lax.broadcasted_iota(jnp.int32, (size, size), 0)
        == lax.broadcasted_iota(jnp.int32, (size, size), 1),
        1.0,
        0.0,
    )
    mat = upper_ref[...] + lower_ref[...] + eye
    mat_ref[...] = mat
    norm = jnp.max(jnp.sum(jnp.abs(mat), axis=0, keepdims=True))
    out_ref[...] = eye * (2.0 / (norm + 1.0))

    def cond(state):
        turn, gap = state
        return (turn < 48) & (gap > 1e-8)

    def turn(state):
        now = out_ref[...]
        miss = eye - jnp.dot(mat_ref[...], now, precision=HI, preferred_element_type=jnp.float32)
        out_ref[...] = now + jnp.dot(now, miss, precision=HI, preferred_element_type=jnp.float32)
        return state[0] + 1, jnp.sum(miss * miss)

    lax.while_loop(cond, turn, (0, jnp.float32(1.0)))


def invert(upper, lower):
    return pl.pallas_call(
        inverse_kernel,
        out_shape=jax.ShapeDtypeStruct(upper.shape, jnp.float32),
        scratch_shapes=[pltpu.VMEM(upper.shape, jnp.float32)],
        name="invert",
    )(upper, lower)


def mm(left, right, precision=MID):
    return jnp.dot(left, right, precision=precision, preferred_element_type=jnp.float32)


def column_sums(left, right):
    return jnp.sum(left * right, axis=0)


def safe(num, den):
    return jnp.where(den > 0, num / jnp.where(den > 0, den, 1.0), 0.0)


def coefficients(mu):
    m0, m1, m2, m3, m4, m5 = mu
    l1, l2 = safe(m1, m0), safe(m2, m0)
    d1 = m2 - l1 * m1
    e = m3 - l1 * m2
    l21 = safe(e, d1)
    d2 = m4 - l2 * m2 - l21 * e
    y0 = -m3
    y1 = -m4 - l1 * y0
    y2 = -m5 - l2 * y0 - l21 * y1
    b2 = safe(y2, d2)
    b1 = safe(y1, d1) - l21 * b2
    b0 = safe(y0, m0) - l1 * b1 - l2 * b2
    scale = 1.0 / (b0 - b1 + b2 - 1.0)
    c0, c1, c2, c3 = b0 * scale, b1 * scale, b2 * scale, scale
    return (1.0 - c0, c3 - c2, -c3), (c0, c1, c2, c3)


def body(blocks, connect, owner_map, right_side):
    devices = lax.axis_size(AXES)
    own = right_side.shape[0]
    window = 2 * own
    up = [(i, (i + 1) % devices) for i in range(devices)]
    down = [(b, a) for a, b in up]

    def from_below(x):
        return lax.ppermute(x, AXES, up)

    def from_above(x):
        return lax.ppermute(x, AXES, down)

    ids = (connect - owner_map[:, None] * own) % (own * devices) + 1
    ids = jnp.pad(ids.astype(jnp.float32), ((0, 0), (0, 128 - NB)))
    send0, send1 = pack(owner_map, ids, blocks, devices)

    def exchange(send):
        got = lax.all_to_all(
            send.reshape(devices, ROWS, 128), AXES, split_axis=0, concat_axis=0, tiled=True
        )
        flags = (got[:, 24, NB] > 0.5).astype(jnp.int32)
        return got.reshape(devices * ROWS, 128), flags

    got0, flags0 = exchange(send0)
    got1, flags1 = exchange(send1)
    right_low, right_high = from_below(right_side), from_above(right_side)
    part = assemble(got0, flags0, window)
    summed = assemble(got1, flags1, window, part)
    lower = from_below(summed[own:])
    low_band, high_band = lower[:, :own], summed[:own, own:]
    inv = invert(summed[:own, :own], lower[:, own:])
    inv_low, inv_high = from_below(inv), from_above(inv)
    near = jnp.concatenate([mm(low_band, inv_low, HI), mm(high_band, inv_high, HI)], axis=1)
    band = jnp.concatenate([low_band, high_band], axis=1)

    v0 = right_side
    v1 = mm(near, jnp.concatenate([right_low, right_high], axis=0))
    w1 = mm(inv, v1)
    w1_low, w1_high = from_below(w1), from_above(w1)
    w0 = mm(inv, v0)
    v2 = mm(band, jnp.concatenate([w1_low, w1_high], axis=0))
    w2 = mm(inv, v2)
    w2_low, w2_high = from_below(w2), from_above(w2)
    early = jnp.stack(
        [
            column_sums(v0, w0),
            column_sums(v1, w0),
            column_sums(v1, w1),
            column_sums(v2, w1),
            column_sums(v2, w2),
        ]
    )
    early = lax.psum(early, AXES)
    v3 = mm(band, jnp.concatenate([w2_low, w2_high], axis=0))
    late = lax.psum(column_sums(v3, w2), AXES)
    xs, cs = coefficients([early[k] for k in range(5)] + [late])
    solution = xs[0] * w0 + xs[1] * w1 + xs[2] * w2
    residual = cs[0] * v0 + cs[1] * v1 + cs[2] * v2 + cs[3] * v3
    return (solution, residual)


def solution(mesh):
    both = P(AXES, None)
    return jax.shard_map(
        body,
        mesh=mesh,
        in_specs=(both, both, P(AXES), both),
        out_specs=(both, both),
        check_vma=False,
    )
```

```python
import jax
import jax.numpy as jnp
from jax import lax
from jax.experimental import pallas as pl
from jax.experimental.pallas import tpu as pltpu
from jax.sharding import PartitionSpec as P

AXES = ("row", "col")
NB = 96
HALF = 48
ROWS = 40
GROUP = 4
HI = lax.Precision.HIGHEST
MID = lax.Precision.HIGH


def split2(x):
    high = x.astype(jnp.bfloat16)
    low = (x - high.astype(jnp.float32)).astype(jnp.bfloat16)
    return high, low


def pack_kernel(owner_ref, ids_ref, x_ref, out_ref, tail_ref):
    subs = x_ref.shape[0]
    devs = out_ref.shape[0] // (2 * ROWS)
    sub = lax.broadcasted_iota(jnp.int32, (devs, subs), 0)
    here = sub == owner_ref[...]
    before = lax.broadcasted_iota(jnp.int32, (subs, subs), 0) < lax.broadcasted_iota(
        jnp.int32, (subs, subs), 1
    )
    count = jnp.dot(
        here.astype(jnp.bfloat16), before.astype(jnp.bfloat16), preferred_element_type=jnp.float32
    )
    first = jnp.where(here & (count < 0.5), 1.0, 0.0).astype(jnp.bfloat16)
    second = jnp.where(here & (count > 0.5), 1.0, 0.0).astype(jnp.bfloat16)
    pick = jnp.concatenate([first, second], axis=0)
    pick = jnp.concatenate([pick, pick], axis=1)
    lane = lax.broadcasted_iota(jnp.int32, (subs, 128), 1)

    def flat(start):
        tile, off = divmod(start, 128)
        if off == 0:
            return x_ref[:, tile * 128 : tile * 128 + 128]
        one = pltpu.roll(x_ref[:, tile * 128 : tile * 128 + 128], 128 - off, 1)
        if (tile + 1) * 128 >= x_ref.shape[1]:
            return one
        two = pltpu.roll(x_ref[:, tile * 128 + 128 : tile * 128 + 256], 128 - off, 1)
        return jnp.where(lane < 128 - off, one, two)

    diag = jnp.zeros((subs, 128), jnp.float32)

    def wrow(i, diag):
        top = flat(NB * i)
        bottom = flat(NB * (i + HALF) + HALF)
        row = jnp.where(lane < i, bottom, jnp.where(lane == i, 0.5 * top, top))
        return row, jnp.where(lane == i, 0.5 * bottom, diag)

    for m in range(8):
        row, diag = wrow(ROWS + m, diag)
        tail_ref[m] = row
    order = [i for i in range(0, ROWS, 2) if i not in (26, 28)] + [26, 28]
    kept = {}
    for i in (26, 27, 28, 29):
        kept[i], diag = wrow(i, diag)
    for i0 in order:
        tiles = []
        for i in (i0, i0 + 1):
            if i in kept:
                row = kept[i]
            else:
                row, diag = wrow(i, diag)
            if i < 24:
                extra = pltpu.roll(tail_ref[i % 8], 96 - 32 * (i // 8), 1)
            elif i < 27:
                extra = pltpu.roll(ids_ref[...], 96 - 32 * (i - 24), 1)
            elif i < 29:
                extra = pltpu.roll(diag, 96 - 32 * (i - 27), 1)
            else:
                extra = jnp.zeros_like(row)
            tiles.append(jnp.where(lane < NB, row, extra))
        high, low = split2(jnp.concatenate(tiles, axis=1))
        out = jnp.dot(
            pick, jnp.concatenate([high, low], axis=0), preferred_element_type=jnp.float32
        )
        for k in range(2):
            part = out[:, 128 * k : 128 * k + 128]
            out_ref[pl.ds(i0 + k, devs, stride=2 * ROWS), :] = part[:devs]
            out_ref[pl.ds(ROWS + i0 + k, devs, stride=2 * ROWS), :] = part[devs:]


def pack(owner_map, ids, blocks, devices):
    return pl.pallas_call(
        pack_kernel,
        out_shape=jax.ShapeDtypeStruct((devices * 2 * ROWS, 128), jnp.float32),
        scratch_shapes=[pltpu.VMEM((8, blocks.shape[0], 128), jnp.float32)],
        name="pack",
    )(owner_map.reshape(1, -1), ids, blocks)


def assemble_kernel(got_ref, s11_ref, s12_ref, low_ref, acc_ref, place_ref, spread_ref, vec_ref, list_ref, sem):
    window = acc_ref.shape[0]
    half = window // 2
    slots = got_ref.shape[0] // ROWS
    lane = lax.broadcasted_iota(jnp.int32, (slots, slots), 1)
    sub = lax.broadcasted_iota(jnp.int32, (slots, slots), 0)
    filled = got_ref[pl.ds(24, slots, stride=ROWS), :][:, NB : NB + 1] > 0.5
    filled = jnp.broadcast_to(jnp.where(filled, 1.0, 0.0), (slots, slots))
    rank = jnp.dot(
        jnp.where(lane < sub, 1.0, 0.0).astype(jnp.bfloat16),
        filled.astype(jnp.bfloat16),
        preferred_element_type=jnp.float32,
    )
    subf = sub.astype(jnp.float32)
    hit = (filled > 0.5) & (rank == lane.astype(jnp.float32))
    count = jnp.sum(filled, axis=0, keepdims=True)
    spare = jnp.max(jnp.where(filled > 0.5, 0.0, subf), axis=0, keepdims=True)
    chosen = jnp.sum(jnp.where(hit, subf, 0.0), axis=0, keepdims=True)
    chosen = jnp.where(lane[:1].astype(jnp.float32) < count, chosen, spare)
    first_row = lax.broadcasted_iota(jnp.int32, (8, slots), 0) == 0
    vec_ref[...] = jnp.where(first_row, chosen, count).astype(jnp.int32)
    copy = pltpu.make_async_copy(vec_ref, list_ref, sem)
    copy.start()
    acc_ref[...] = jnp.zeros_like(acc_ref)
    place_ref[1] = jnp.zeros(place_ref.shape[1:], jnp.bfloat16)
    spread_ref[1] = jnp.zeros(spread_ref.shape[1:], jnp.bfloat16)
    copy.wait()

    lane = lax.broadcasted_iota(jnp.int32, (HALF, 128), 1)
    row = lax.broadcasted_iota(jnp.int32, (HALF, 128), 0)
    lane1 = lax.broadcasted_iota(jnp.int32, (1, 128), 1)
    lane8 = lax.broadcasted_iota(jnp.int32, (8, 128), 1)
    target = (lax.broadcasted_iota(jnp.int32, (window, 128), 0) + 1).astype(jnp.float32)

    def lanes(pieces):
        out = pieces[3]
        for k in (2, 1, 0):
            out = jnp.where(lane1 < 32 * (k + 1), pieces[k], out)
        return out

    def onehot(ids):
        return jnp.where(target == ids, 1.0, 0.0).astype(jnp.bfloat16)

    def generate(buf, first):
        pieces = []
        for k in range(GROUP):
            slot = list_ref[0, first + k]
            base = pl.multiple_of(slot * ROWS, 8)
            got = got_ref[pl.ds(base, ROWS), :]
            rows = [got[24 + m : 25 + m] for m in range(3)]
            pieces += rows
            ids = lanes([pltpu.roll(rows[m], 32 * (m + 1), 1) for m in range(3)] + [jnp.zeros_like(rows[0])])
            half_diag = jnp.where(
                lane1 < 80, pltpu.roll(got[27:28], 80, 1), pltpu.roll(got[28:29], 112, 1)
            )
            tail = jnp.where(
                lane8 < 32,
                pltpu.roll(got[0:8], 32, 1),
                jnp.where(lane8 < 64, pltpu.roll(got[8:16], 64, 1), pltpu.roll(got[16:24], 96, 1)),
            )
            full = jnp.concatenate([got, tail], axis=0)
            top = jnp.where(lane >= row, full, 0.0)
            bottom = jnp.where(
                lane == row + HALF,
                half_diag,
                jnp.where((lane >= HALF) & (lane < row + HALF), pltpu.roll(full, HALF, 1), 0.0),
            )
            high, low = split2(jnp.concatenate([top, bottom], axis=0))
            spread = lax.dot_general(
                jnp.concatenate([high, low], axis=0),
                onehot(ids),
                (((1,), (1,)), ((), ())),
                preferred_element_type=jnp.float32,
            ).astype(jnp.bfloat16)
            spread_ref[buf, NB * k : NB * k + NB, :] = spread[:NB]
            spread_ref[buf, NB * (GROUP + k) : NB * (GROUP + k) + NB, :] = spread[NB:]
        for t in range(3):
            moved = [
                pltpu.roll(pieces[4 * t + q], (32 * (q + 1)) % 128, 1) if q < 3 else pieces[4 * t + q]
                for q in range(4)
            ]
            place = onehot(lanes(moved))
            place_ref[buf, :, 128 * t : 128 * t + 128] = place
            place_ref[buf, :, 128 * (t + 3) : 128 * (t + 3) + 128] = place

    def absorb(buf):
        acc_ref[...] += jnp.dot(
            place_ref[buf], spread_ref[buf], preferred_element_type=jnp.float32
        )

    def step(g, carry):
        generate(0, g * 2 * GROUP)
        absorb(1)
        generate(1, g * 2 * GROUP + GROUP)
        absorb(0)
        return carry

    lax.fori_loop(0, (list_ref[1, 0] + 2 * GROUP - 1) // (2 * GROUP), step, 0)
    absorb(1)
    a11, a22 = acc_ref[:half, :half], acc_ref[half:, half:]
    s11_ref[...] = a11 + a11.T
    s12 = acc_ref[:half, half:] + acc_ref[half:, :half].T
    s12_ref[...] = s12
    low_ref[:, :half] = s12.T
    low_ref[:, half:] = a22 + a22.T


def assemble(got, window):
    slots = got.shape[0] // ROWS
    half = window // 2
    square = jax.ShapeDtypeStruct((half, half), jnp.float32)
    return pl.pallas_call(
        assemble_kernel,
        out_shape=(square, square, jax.ShapeDtypeStruct((half, window), jnp.float32)),
        scratch_shapes=[
            pltpu.VMEM((window, window), jnp.float32),
            pltpu.VMEM((2, window, 2 * NB * GROUP), jnp.bfloat16),
            pltpu.VMEM((2, 2 * NB * GROUP, window), jnp.bfloat16),
            pltpu.VMEM((8, slots), jnp.int32),
            pltpu.SMEM((8, slots), jnp.int32),
            pltpu.SemaphoreType.DMA,
        ],
        name="assemble",
    )(got)


def inverse_kernel(upper_ref, lower_ref, out_ref, mat_ref):
    size = upper_ref.shape[0]
    eye = jnp.where(
        lax.broadcasted_iota(jnp.int32, (size, size), 0)
        == lax.broadcasted_iota(jnp.int32, (size, size), 1),
        1.0,
        0.0,
    )
    mat = upper_ref[...] + lower_ref[:, size:] + eye
    mat_ref[...] = mat
    norm = jnp.max(jnp.sum(jnp.abs(mat), axis=0, keepdims=True))
    out_ref[...] = eye * (2.0 / (norm + 1.0))

    def cond(state):
        turn, gap = state
        return (turn < 48) & (gap > 1e-8)

    def turn(state):
        now = out_ref[...]
        miss = eye - jnp.dot(mat_ref[...], now, precision=HI, preferred_element_type=jnp.float32)
        out_ref[...] = now + jnp.dot(now, miss, precision=HI, preferred_element_type=jnp.float32)
        return state[0] + 1, jnp.sum(miss * miss)

    lax.while_loop(cond, turn, (0, jnp.float32(1.0)))


def invert(upper, lower):
    return pl.pallas_call(
        inverse_kernel,
        out_shape=jax.ShapeDtypeStruct(upper.shape, jnp.float32),
        scratch_shapes=[pltpu.VMEM(upper.shape, jnp.float32)],
        name="invert",
    )(upper, lower)


def mm(left, right, precision=MID):
    return jnp.dot(left, right, precision=precision, preferred_element_type=jnp.float32)


def column_sums(left, right):
    return jnp.sum(left * right, axis=0)


def safe(num, den):
    return jnp.where(den > 0, num / jnp.where(den > 0, den, 1.0), 0.0)


def coefficients(mu):
    m0, m1, m2, m3, m4, m5 = mu
    l1, l2 = safe(m1, m0), safe(m2, m0)
    d1 = m2 - l1 * m1
    e = m3 - l1 * m2
    l21 = safe(e, d1)
    d2 = m4 - l2 * m2 - l21 * e
    y0 = -m3
    y1 = -m4 - l1 * y0
    y2 = -m5 - l2 * y0 - l21 * y1
    b2 = safe(y2, d2)
    b1 = safe(y1, d1) - l21 * b2
    b0 = safe(y0, m0) - l1 * b1 - l2 * b2
    scale = 1.0 / (b0 - b1 + b2 - 1.0)
    c0, c1, c2, c3 = b0 * scale, b1 * scale, b2 * scale, scale
    return (1.0 - c0, c3 - c2, -c3), (c0, c1, c2, c3)


def body(blocks, connect, owner_map, right_side):
    devices = lax.axis_size(AXES)
    own = right_side.shape[0]
    window = 2 * own
    up = [(i, (i + 1) % devices) for i in range(devices)]
    down = [(b, a) for a, b in up]

    def from_below(x):
        return lax.ppermute(x, AXES, up)

    def from_above(x):
        return lax.ppermute(x, AXES, down)

    ids = (connect - owner_map[:, None] * own) % (own * devices) + 1
    ids = jnp.pad(ids.astype(jnp.float32), ((0, 0), (0, 128 - NB)))
    send = pack(owner_map, ids, blocks, devices)
    got = lax.all_to_all(
        send.reshape(devices, 2 * ROWS, 128), AXES, split_axis=0, concat_axis=0, tiled=True
    )
    got = got.reshape(devices * 2 * ROWS, 128)
    v0 = right_side
    v0, got = lax.optimization_barrier((v0, got))
    v0_low, v0_high = from_below(v0), from_above(v0)
    center, high_band, lower = assemble(got, window)
    lower = from_below(lower)
    low_band = lower[:, :own]
    inv = invert(center, lower)
    inv_low, inv_high = from_below(inv), from_above(inv)
    near_low, near_high = mm(low_band, inv_low, HI), mm(high_band, inv_high, HI)

    def reach(low, high, x_low, x_high):
        return mm(low, x_low) + mm(high, x_high)

    v1 = reach(near_low, near_high, v0_low, v0_high)
    w1 = mm(inv, v1)
    w1_low, w1_high = from_below(w1), from_above(w1)
    w0 = mm(inv, v0)
    v2 = reach(low_band, high_band, w1_low, w1_high)
    w2 = mm(inv, v2)
    w2_low, w2_high = from_below(w2), from_above(w2)
    early = jnp.stack(
        [
            column_sums(v0, w0),
            column_sums(v1, w0),
            column_sums(v1, w1),
            column_sums(v2, w1),
            column_sums(v2, w2),
        ]
    )
    v3 = reach(low_band, high_band, w2_low, w2_high)
    sums = jnp.concatenate([early, column_sums(v3, w2)[None]], axis=0)
    bit = 1
    while bit < devices:
        sums = sums + lax.ppermute(sums, AXES, [(i, i ^ bit) for i in range(devices)])
        bit *= 2
    xs, cs = coefficients([sums[k] for k in range(6)])
    solution = xs[0] * w0 + xs[1] * w1 + xs[2] * w2
    residual = cs[0] * v0 + cs[1] * v1 + cs[2] * v2 + cs[3] * v3
    return (solution, residual)


def solution(mesh):
    both = P(AXES, None)
    return jax.shard_map(
        body,
        mesh=mesh,
        in_specs=(both, both, P(AXES), both),
        out_specs=(both, both),
        check_vma=False,
    )
```

```python
import jax
import jax.numpy as jnp
from jax import lax
from jax.experimental import pallas as pl
from jax.experimental.pallas import tpu as pltpu
from jax.sharding import PartitionSpec as P


AXES = ("row", "col")
NB = 96
HALF = 48
ROWS = 40
GROUP = 4
HI = lax.Precision.HIGHEST
MID = lax.Precision.HIGH
CHUNKS = 4


def split2(x):
    high = x.astype(jnp.bfloat16)
    low = (x - high.astype(jnp.float32)).astype(jnp.bfloat16)
    return high, low


def pack_kernel(owner_ref, ids_ref, x_ref, out0_ref, out1_ref, tail_ref):
    subs = x_ref.shape[0]
    devs = out0_ref.shape[0] // ROWS
    sub = lax.broadcasted_iota(jnp.int32, (devs, subs), 0)
    here = sub == owner_ref[...]
    before = lax.broadcasted_iota(jnp.int32, (subs, subs), 0) < lax.broadcasted_iota(
        jnp.int32, (subs, subs), 1
    )
    count = jnp.dot(
        here.astype(jnp.bfloat16), before.astype(jnp.bfloat16), preferred_element_type=jnp.float32
    )
    first = jnp.where(here & (count < 0.5), 1.0, 0.0).astype(jnp.bfloat16)
    second = jnp.where(here & (count > 0.5), 1.0, 0.0).astype(jnp.bfloat16)
    pick = jnp.concatenate([first, second], axis=0)
    pick = jnp.concatenate([pick, pick], axis=1)
    lane = lax.broadcasted_iota(jnp.int32, (subs, 128), 1)

    def flat(start):
        tile, off = divmod(start, 128)
        if off == 0:
            return x_ref[:, tile * 128 : tile * 128 + 128]
        one = pltpu.roll(x_ref[:, tile * 128 : tile * 128 + 128], 128 - off, 1)
        if (tile + 1) * 128 >= x_ref.shape[1]:
            return one
        two = pltpu.roll(x_ref[:, tile * 128 + 128 : tile * 128 + 256], 128 - off, 1)
        return jnp.where(lane < 128 - off, one, two)

    diag = jnp.zeros((subs, 128), jnp.float32)

    def wrow(i, diag):
        top = flat(NB * i)
        bottom = flat(NB * (i + HALF) + HALF)
        row = jnp.where(lane < i, bottom, jnp.where(lane == i, 0.5 * top, top))
        return row, jnp.where(lane == i, 0.5 * bottom, diag)

    for m in range(8):
        row, diag = wrow(ROWS + m, diag)
        tail_ref[m] = row
    order = [i for i in range(0, ROWS, 2) if i not in (26, 28)] + [26, 28]
    kept = {}
    for i in (26, 27, 28, 29):
        kept[i], diag = wrow(i, diag)
    for i0 in order:
        tiles = []
        for i in (i0, i0 + 1):
            if i in kept:
                row = kept[i]
            else:
                row, diag = wrow(i, diag)
            if i < 24:
                extra = pltpu.roll(tail_ref[i % 8], 96 - 32 * (i // 8), 1)
            elif i < 27:
                extra = pltpu.roll(ids_ref[...], 96 - 32 * (i - 24), 1)
            elif i < 29:
                extra = pltpu.roll(diag, 96 - 32 * (i - 27), 1)
            else:
                extra = jnp.zeros_like(row)
            tiles.append(jnp.where(lane < NB, row, extra))
        high, low = split2(jnp.concatenate(tiles, axis=1))
        out = jnp.dot(
            pick, jnp.concatenate([high, low], axis=0), preferred_element_type=jnp.float32
        )
        for k in range(2):
            part = out[:, 128 * k : 128 * k + 128]
            out0_ref[pl.ds(i0 + k, devs, stride=ROWS), :] = part[:devs]
            out1_ref[pl.ds(i0 + k, devs, stride=ROWS), :] = part[devs:]


def pack(owner_map, ids, blocks, devices):
    shape = jax.ShapeDtypeStruct((devices * ROWS, 128), jnp.float32)
    return pl.pallas_call(
        pack_kernel,
        out_shape=(shape, shape),
        scratch_shapes=[pltpu.VMEM((8, blocks.shape[0], 128), jnp.float32)],
        name="pack",
    )(owner_map.reshape(1, -1), ids, blocks)


def assemble_kernel(last, got_ref, *refs):
    place_ref, spread_ref, vec_ref, list_ref, sem = refs[-5:]
    if last:
        prev_ref, s11_ref, s12_ref, low_ref, acc_ref = refs[:5]
    else:
        acc_ref = refs[0]
    window = acc_ref.shape[0]
    half = window // 2
    slots = got_ref.shape[0] // ROWS
    lane = lax.broadcasted_iota(jnp.int32, (slots, slots), 1)
    sub = lax.broadcasted_iota(jnp.int32, (slots, slots), 0)
    filled = got_ref[pl.ds(24, slots, stride=ROWS), :][:, NB : NB + 1] > 0.5
    filled = jnp.broadcast_to(jnp.where(filled, 1.0, 0.0), (slots, slots))
    rank = jnp.dot(
        jnp.where(lane < sub, 1.0, 0.0).astype(jnp.bfloat16),
        filled.astype(jnp.bfloat16),
        preferred_element_type=jnp.float32,
    )
    subf = sub.astype(jnp.float32)
    hit = (filled > 0.5) & (rank == lane.astype(jnp.float32))
    count = jnp.sum(filled, axis=0, keepdims=True)
    spare = jnp.max(jnp.where(filled > 0.5, 0.0, subf), axis=0, keepdims=True)
    chosen = jnp.sum(jnp.where(hit, subf, 0.0), axis=0, keepdims=True)
    chosen = jnp.where(lane[:1].astype(jnp.float32) < count, chosen, spare)
    first_row = lax.broadcasted_iota(jnp.int32, (8, slots), 0) == 0
    vec_ref[...] = jnp.where(first_row, chosen, count).astype(jnp.int32)
    copy = pltpu.make_async_copy(vec_ref, list_ref, sem)
    copy.start()
    acc_ref[...] = prev_ref[...] if last else jnp.zeros_like(acc_ref)
    place_ref[1] = jnp.zeros(place_ref.shape[1:], jnp.bfloat16)
    spread_ref[1] = jnp.zeros(spread_ref.shape[1:], jnp.bfloat16)
    copy.wait()

    lane = lax.broadcasted_iota(jnp.int32, (HALF, 128), 1)
    row = lax.broadcasted_iota(jnp.int32, (HALF, 128), 0)
    lane1 = lax.broadcasted_iota(jnp.int32, (1, 128), 1)
    lane8 = lax.broadcasted_iota(jnp.int32, (8, 128), 1)
    target = (lax.broadcasted_iota(jnp.int32, (window, 128), 0) + 1).astype(jnp.float32)

    def lanes(pieces):
        out = pieces[3]
        for k in (2, 1, 0):
            out = jnp.where(lane1 < 32 * (k + 1), pieces[k], out)
        return out

    def onehot(ids):
        return jnp.where(target == ids, 1.0, 0.0).astype(jnp.bfloat16)

    def generate(buf, first):
        pieces = []
        for k in range(GROUP):
            slot = list_ref[0, first + k]
            base = pl.multiple_of(slot * ROWS, 8)
            got = got_ref[pl.ds(base, ROWS), :]
            rows = [got[24 + m : 25 + m] for m in range(3)]
            pieces += rows
            ids = lanes([pltpu.roll(rows[m], 32 * (m + 1), 1) for m in range(3)] + [jnp.zeros_like(rows[0])])
            half_diag = jnp.where(
                lane1 < 80, pltpu.roll(got[27:28], 80, 1), pltpu.roll(got[28:29], 112, 1)
            )
            tail = jnp.where(
                lane8 < 32,
                pltpu.roll(got[0:8], 32, 1),
                jnp.where(lane8 < 64, pltpu.roll(got[8:16], 64, 1), pltpu.roll(got[16:24], 96, 1)),
            )
            full = jnp.concatenate([got, tail], axis=0)
            top = jnp.where(lane >= row, full, 0.0)
            bottom = jnp.where(
                lane == row + HALF,
                half_diag,
                jnp.where((lane >= HALF) & (lane < row + HALF), pltpu.roll(full, HALF, 1), 0.0),
            )
            high, low = split2(jnp.concatenate([top, bottom], axis=0))
            spread = lax.dot_general(
                jnp.concatenate([high, low], axis=0),
                onehot(ids),
                (((1,), (1,)), ((), ())),
                preferred_element_type=jnp.float32,
            ).astype(jnp.bfloat16)
            spread_ref[buf, NB * k : NB * k + NB, :] = spread[:NB]
            spread_ref[buf, NB * (GROUP + k) : NB * (GROUP + k) + NB, :] = spread[NB:]
        for t in range(3):
            moved = [
                pltpu.roll(pieces[4 * t + q], (32 * (q + 1)) % 128, 1) if q < 3 else pieces[4 * t + q]
                for q in range(4)
            ]
            place = onehot(lanes(moved))
            place_ref[buf, :, 128 * t : 128 * t + 128] = place
            place_ref[buf, :, 128 * (t + 3) : 128 * (t + 3) + 128] = place

    def absorb(buf):
        acc_ref[...] += jnp.dot(
            place_ref[buf], spread_ref[buf], preferred_element_type=jnp.float32
        )

    def step(g, carry):
        generate(0, g * 2 * GROUP)
        absorb(1)
        generate(1, g * 2 * GROUP + GROUP)
        absorb(0)
        return carry

    lax.fori_loop(0, (list_ref[1, 0] + 2 * GROUP - 1) // (2 * GROUP), step, 0)
    absorb(1)
    if not last:
        return
    a11, a22 = acc_ref[:half, :half], acc_ref[half:, half:]
    s11_ref[...] = a11 + a11.T
    s12 = acc_ref[:half, half:] + acc_ref[half:, :half].T
    s12_ref[...] = s12
    low_ref[:, :half] = s12.T
    low_ref[:, half:] = a22 + a22.T


def assemble(got, window, prev=None):
    slots = got.shape[0] // ROWS
    half = window // 2
    last = prev is not None
    square = jax.ShapeDtypeStruct((half, half), jnp.float32)
    whole = jax.ShapeDtypeStruct((window, window), jnp.float32)
    scratch = [
        pltpu.VMEM((2, window, 2 * NB * GROUP), jnp.bfloat16),
        pltpu.VMEM((2, 2 * NB * GROUP, window), jnp.bfloat16),
        pltpu.VMEM((8, slots), jnp.int32),
        pltpu.SMEM((8, slots), jnp.int32),
        pltpu.SemaphoreType.DMA,
    ]
    if last:
        scratch = [pltpu.VMEM((window, window), jnp.float32)] + scratch
    out = (square, square, jax.ShapeDtypeStruct((half, window), jnp.float32)) if last else whole
    return pl.pallas_call(
        lambda *refs: assemble_kernel(last, *refs),
        out_shape=out,
        scratch_shapes=scratch,
        name="assemble_last" if last else "assemble_first",
    )(*((got, prev) if last else (got,)))


def inverse_kernel(upper_ref, lower_ref, out_ref, mat_ref):
    size = upper_ref.shape[0]
    eye = jnp.where(
        lax.broadcasted_iota(jnp.int32, (size, size), 0)
        == lax.broadcasted_iota(jnp.int32, (size, size), 1),
        1.0,
        0.0,
    )
    mat = upper_ref[...] + lower_ref[:, size:] + eye
    mat_ref[...] = mat
    norm = jnp.max(jnp.sum(jnp.abs(mat), axis=0, keepdims=True))
    out_ref[...] = eye * (2.0 / (norm + 1.0))

    def cond(state):
        turn, gap = state
        return (turn < 48) & (gap > 1e-8)

    def turn(state):
        now = out_ref[...]
        miss = eye - jnp.dot(mat_ref[...], now, precision=HI, preferred_element_type=jnp.float32)
        out_ref[...] = now + jnp.dot(now, miss, precision=HI, preferred_element_type=jnp.float32)
        return state[0] + 1, jnp.sum(miss * miss)

    lax.while_loop(cond, turn, (0, jnp.float32(1.0)))


def invert(upper, lower):
    return pl.pallas_call(
        inverse_kernel,
        out_shape=jax.ShapeDtypeStruct(upper.shape, jnp.float32),
        scratch_shapes=[pltpu.VMEM(upper.shape, jnp.float32)],
        name="invert",
    )(upper, lower)


def mm(left, right, precision=MID):
    return jnp.dot(left, right, precision=precision, preferred_element_type=jnp.float32)


def column_sums(left, right):
    return jnp.sum(left * right, axis=0)


def safe(num, den):
    return jnp.where(den > 0, num / jnp.where(den > 0, den, 1.0), 0.0)


def coefficients(mu):
    m0, m1, m2, m3, m4, m5 = mu
    l1, l2 = safe(m1, m0), safe(m2, m0)
    d1 = m2 - l1 * m1
    e = m3 - l1 * m2
    l21 = safe(e, d1)
    d2 = m4 - l2 * m2 - l21 * e
    y0 = -m3
    y1 = -m4 - l1 * y0
    y2 = -m5 - l2 * y0 - l21 * y1
    b2 = safe(y2, d2)
    b1 = safe(y1, d1) - l21 * b2
    b0 = safe(y0, m0) - l1 * b1 - l2 * b2
    scale = 1.0 / (b0 - b1 + b2 - 1.0)
    c0, c1, c2, c3 = b0 * scale, b1 * scale, b2 * scale, scale
    return (1.0 - c0, c3 - c2, -c3), (c0, c1, c2, c3)


def finish_kernel(coef_ref, v0, v1, v2, t0, t1, w0, w1, w2, sol_in, res_in, sol_ref, res_ref):
    x = [coef_ref[k : k + 1, :] for k in range(7)]
    sol_ref[...] = x[0] * w0[...] + x[1] * w1[...] + x[2] * w2[...]
    res_ref[...] = (
        x[3] * v0[...] + x[4] * v1[...] + x[5] * v2[...] + x[6] * (t0[...] + t1[...])
    )


def finish(c, coef, v0, parts, sol, res):
    rows, width = parts[0].shape
    step = rows // 4
    part = pl.BlockSpec((step, width), lambda i: (i, 0))
    place = pl.BlockSpec((step, width), lambda i: (i, c))
    anywhere = pl.BlockSpec(memory_space=pl.ANY)
    return pl.pallas_call(
        finish_kernel,
        grid=(4,),
        in_specs=[pl.BlockSpec((8, width), lambda i: (0, 0)), place]
        + [part] * len(parts)
        + [anywhere, anywhere],
        out_specs=(place, place),
        out_shape=(jax.ShapeDtypeStruct(sol.shape, sol.dtype),) * 2,
        input_output_aliases={2 + len(parts): 0, 3 + len(parts): 1},
    )(coef, v0, *parts, sol, res)


def first_finish_kernel(coef_ref, v0, v1, v2, t0, t1, w0, w1, w2, sol_ref, res_ref):
    finish_kernel(coef_ref, v0, v1, v2, t0, t1, w0, w1, w2, None, None, sol_ref, res_ref)


def first_finish(c, coef, v0, parts):
    rows, width = parts[0].shape
    step = rows // 4
    part = pl.BlockSpec((step, width), lambda i: (i, 0))
    place = pl.BlockSpec((step, width), lambda i: (i, c))
    return pl.pallas_call(
        first_finish_kernel,
        grid=(4,),
        in_specs=[pl.BlockSpec((8, width), lambda i: (0, 0)), place] + [part] * len(parts),
        out_specs=(place, place),
        out_shape=(jax.ShapeDtypeStruct(v0.shape, v0.dtype),) * 2,
    )(coef, v0, *parts)


def all_sum(x, devices):
    for stride, size in ((32, 4), (4, 4), (16, 2), (1, 4)):
        got = []
        for d in range(1, size):
            pairs = []
            for i in range(devices):
                place = i // stride % size
                pairs.append((i, i + ((place + d) % size - place) * stride))
            got.append(lax.ppermute(x, AXES, pairs))
        for part in got:
            x = x + part
    return x


def body(blocks, connect, owner_map, right_side):
    devices = lax.axis_size(AXES)
    own = right_side.shape[0]
    window = 2 * own
    up = [(i, (i + 1) % devices) for i in range(devices)]
    down = [(b, a) for a, b in up]

    def from_below(x):
        return lax.ppermute(x, AXES, up)

    def from_above(x):
        return lax.ppermute(x, AXES, down)

    ids = (connect - owner_map[:, None] * own) % (own * devices) + 1
    ids = jnp.pad(ids.astype(jnp.float32), ((0, 0), (0, 128 - NB)))
    width = right_side.shape[1] // CHUNKS
    cols = range(CHUNKS)
    half = CHUNKS // 2
    pairwise = [c for k in range(half) for c in (k, k + half)]

    def chunk(x, c):
        return lax.slice_in_dim(x, c * width, (c + 1) * width, axis=1)

    v0 = [chunk(right_side, c) for c in cols]
    v0_low, v0_high = {}, {}
    v0_low[0], v0_high[0] = from_below(v0[0]), from_above(v0[0])
    send0, send1 = pack(owner_map, ids, blocks, devices)

    def exchange(send):
        got = lax.all_to_all(
            send.reshape(devices, ROWS, 128), AXES, split_axis=0, concat_axis=0, tiled=True
        )
        return got.reshape(devices * ROWS, 128)

    got0 = exchange(send0)
    got1 = exchange(send1)
    rest, got0 = lax.optimization_barrier(([v0[c] for c in pairwise[1:]], got0))
    for c, x in zip(pairwise[1:], rest):
        v0_low[c], v0_high[c] = (from_below(x), from_above(x))
    part = assemble(got0, window)
    center, high_band, lower = assemble(got1, window, part)
    lower = from_below(lower)
    low_band = lower[:, :own]
    inv = invert(center, lower)
    inv_low, inv_high = from_below(inv), from_above(inv)
    near_low, near_high = mm(low_band, inv_low, HI), mm(high_band, inv_high, HI)

    v1, w1, w1_low, w1_high = {}, {}, {}, {}
    for c in pairwise:
        v1[c] = mm(near_low, v0_low[c]) + mm(near_high, v0_high[c])
        w1[c] = mm(inv, v1[c])
        w1_low[c] = from_below(w1[c])
        w1_high[c] = from_above(w1[c])
    w0 = {c: mm(inv, v0[c]) for c in cols}
    v2, w2, w2_low, w2_high = {}, {}, {}, {}
    for c in pairwise:
        v2[c] = mm(low_band, w1_low[c]) + mm(high_band, w1_high[c])
        w2[c] = mm(inv, v2[c])
    for k in cols:
        c = (k + half) % CHUNKS
        w2_high[k] = from_above(w2[k])
        w2_low[c] = from_below(w2[c])
    early = [
        jnp.stack(
            [
                column_sums(v0[c], w0[c]),
                column_sums(v1[c], w0[c]),
                column_sums(v1[c], w1[c]),
                column_sums(v2[c], w1[c]),
                column_sums(v2[c], w2[c]),
            ]
        )
        for c in cols
    ]
    early = all_sum(jnp.concatenate(early, axis=1), devices)
    t_high = {c: mm(high_band, w2_high[c]) for c in cols}
    t_low = {c: mm(low_band, w2_low[c]) for c in cols}
    late = [2.0 * column_sums((t_high if c < half else t_low)[c], w2[c]) for c in cols]
    late = all_sum(jnp.concatenate(late)[None], devices)
    xs, cs = coefficients([early[k] for k in range(5)] + [late[0]])
    coef = jnp.stack(list(xs) + list(cs) + [cs[0]])
    outs = None
    for c in pairwise:
        parts = [v1[c], v2[c], t_low[c], t_high[c], w0[c], w1[c], w2[c]]
        if outs is None:
            outs = first_finish(c, chunk(coef, c), right_side, parts)
        else:
            outs = finish(c, chunk(coef, c), right_side, parts, *outs)
    return tuple(outs)


def solution(mesh):
    both = P(AXES, None)
    return jax.shard_map(
        body,
        mesh=mesh,
        in_specs=(both, both, P(AXES), both),
        out_specs=(both, both),
        check_vma=False,
    )
```

```python
import jax
import jax.numpy as jnp
from jax import lax
from jax.experimental import pallas as pl
from jax.experimental.pallas import tpu as pltpu
from jax.sharding import PartitionSpec as P


AXES = ("row", "col")
NB = 96
HALF = 48
ROWS = 40
GROUP = 4
HI = lax.Precision.HIGHEST
MID = lax.Precision.HIGH


def split2(x):
    high = x.astype(jnp.bfloat16)
    low = (x - high.astype(jnp.float32)).astype(jnp.bfloat16)
    return high, low


def pack_kernel(owner_ref, ids_ref, x_ref, out0_ref, out1_ref, tail_ref):
    subs = x_ref.shape[0]
    devs = out0_ref.shape[0] // ROWS
    sub = lax.broadcasted_iota(jnp.int32, (devs, subs), 0)
    here = sub == owner_ref[...]
    before = lax.broadcasted_iota(jnp.int32, (subs, subs), 0) < lax.broadcasted_iota(
        jnp.int32, (subs, subs), 1
    )
    count = jnp.dot(
        here.astype(jnp.bfloat16), before.astype(jnp.bfloat16), preferred_element_type=jnp.float32
    )
    first = jnp.where(here & (count < 0.5), 1.0, 0.0).astype(jnp.bfloat16)
    second = jnp.where(here & (count > 0.5), 1.0, 0.0).astype(jnp.bfloat16)
    pick = jnp.concatenate([first, second], axis=0)
    ids = ids_ref[...].astype(jnp.float32).T + 1.0
    ids = jnp.concatenate([ids, jnp.zeros((subs, 128 - NB), jnp.float32)], axis=1)
    pick = jnp.concatenate([pick, pick], axis=1)
    lane = lax.broadcasted_iota(jnp.int32, (subs, 128), 1)

    def flat(start):
        tile, off = divmod(start, 128)
        if off == 0:
            return x_ref[:, tile * 128 : tile * 128 + 128]
        one = pltpu.roll(x_ref[:, tile * 128 : tile * 128 + 128], 128 - off, 1)
        if (tile + 1) * 128 >= x_ref.shape[1]:
            return one
        two = pltpu.roll(x_ref[:, tile * 128 + 128 : tile * 128 + 256], 128 - off, 1)
        return jnp.where(lane < 128 - off, one, two)

    diag = jnp.zeros((subs, 128), jnp.float32)

    def wrow(i, diag):
        top = flat(NB * i)
        bottom = flat(NB * (i + HALF) + HALF)
        row = jnp.where(lane < i, bottom, jnp.where(lane == i, 0.5 * top, top))
        return row, jnp.where(lane == i, 0.5 * bottom, diag)

    for m in range(8):
        row, diag = wrow(ROWS + m, diag)
        tail_ref[m] = row
    order = [i for i in range(0, ROWS, 2) if i not in (26, 28)] + [26, 28]
    kept = {}
    for i in (26, 27, 28, 29):
        kept[i], diag = wrow(i, diag)
    for i0 in order:
        tiles = []
        for i in (i0, i0 + 1):
            if i in kept:
                row = kept[i]
            else:
                row, diag = wrow(i, diag)
            if i < 24:
                extra = pltpu.roll(tail_ref[i % 8], 96 - 32 * (i // 8), 1)
            elif i < 27:
                extra = pltpu.roll(ids, 96 - 32 * (i - 24), 1)
            elif i < 29:
                extra = pltpu.roll(diag, 96 - 32 * (i - 27), 1)
            else:
                extra = jnp.zeros_like(row)
            tiles.append(jnp.where(lane < NB, row, extra))
        high, low = split2(jnp.concatenate(tiles, axis=1))
        out = jnp.dot(
            pick, jnp.concatenate([high, low], axis=0), preferred_element_type=jnp.float32
        )
        for k in range(2):
            part = out[:, 128 * k : 128 * k + 128]
            out0_ref[pl.ds(i0 + k, devs, stride=ROWS), :] = part[:devs]
            out1_ref[pl.ds(i0 + k, devs, stride=ROWS), :] = part[devs:]


def pack(owner_map, ids, blocks, devices):
    shape = jax.ShapeDtypeStruct((devices * ROWS, 128), jnp.float32)
    return pl.pallas_call(
        pack_kernel,
        out_shape=(shape, shape),
        scratch_shapes=[pltpu.VMEM((8, blocks.shape[0], 128), jnp.float32)],
        name="pack",
    )(owner_map.reshape(1, -1), ids, blocks)


def assemble_kernel(last, base_ref, got_ref, *refs):
    place_ref, spread_ref, vec_ref, list_ref, sem = refs[-5:]
    if last:
        prev_ref, s11_ref, s12_ref, low_ref, acc_ref = refs[:5]
    else:
        acc_ref = refs[0]
    window = acc_ref.shape[0]
    half = window // 2
    slots = got_ref.shape[0] // ROWS
    lane = lax.broadcasted_iota(jnp.int32, (slots, slots), 1)
    sub = lax.broadcasted_iota(jnp.int32, (slots, slots), 0)
    filled = got_ref[pl.ds(24, slots, stride=ROWS), :][:, NB : NB + 1] > 0.5
    filled = jnp.broadcast_to(jnp.where(filled, 1.0, 0.0), (slots, slots))
    rank = jnp.dot(
        jnp.where(lane < sub, 1.0, 0.0).astype(jnp.bfloat16),
        filled.astype(jnp.bfloat16),
        preferred_element_type=jnp.float32,
    )
    subf = sub.astype(jnp.float32)
    hit = (filled > 0.5) & (rank == lane.astype(jnp.float32))
    count = jnp.sum(filled, axis=0, keepdims=True)
    spare = jnp.max(jnp.where(filled > 0.5, 0.0, subf), axis=0, keepdims=True)
    chosen = jnp.sum(jnp.where(hit, subf, 0.0), axis=0, keepdims=True)
    chosen = jnp.where(lane[:1].astype(jnp.float32) < count, chosen, spare)
    first_row = lax.broadcasted_iota(jnp.int32, (8, slots), 0) == 0
    vec_ref[...] = jnp.where(first_row, chosen, count).astype(jnp.int32)
    copy = pltpu.make_async_copy(vec_ref, list_ref, sem)
    copy.start()
    acc_ref[...] = prev_ref[...] if last else jnp.zeros_like(acc_ref)
    place_ref[1] = jnp.zeros(place_ref.shape[1:], jnp.bfloat16)
    spread_ref[1] = jnp.zeros(spread_ref.shape[1:], jnp.bfloat16)
    copy.wait()

    lane = lax.broadcasted_iota(jnp.int32, (HALF, 128), 1)
    row = lax.broadcasted_iota(jnp.int32, (HALF, 128), 0)
    lane1 = lax.broadcasted_iota(jnp.int32, (1, 128), 1)
    lane8 = lax.broadcasted_iota(jnp.int32, (8, 128), 1)
    target = lax.broadcasted_iota(jnp.int32, (window, 128), 0).astype(jnp.float32)
    start = base_ref[0].astype(jnp.float32)
    total = base_ref[1].astype(jnp.float32)

    def local(ids):
        moved = ids - 1.0 - start
        return jnp.where(ids > 0.5, jnp.where(moved < 0.0, moved + total, moved), -1.0)


    def lanes(pieces):
        out = pieces[3]
        for k in (2, 1, 0):
            out = jnp.where(lane1 < 32 * (k + 1), pieces[k], out)
        return out

    def onehot(ids):
        return jnp.where(target == local(ids), 1.0, 0.0).astype(jnp.bfloat16)

    def generate(buf, first):
        pieces = []
        for k in range(GROUP):
            slot = list_ref[0, first + k]
            base = pl.multiple_of(slot * ROWS, 8)
            got = got_ref[pl.ds(base, ROWS), :]
            rows = [got[24 + m : 25 + m] for m in range(3)]
            pieces += rows
            ids = lanes([pltpu.roll(rows[m], 32 * (m + 1), 1) for m in range(3)] + [jnp.zeros_like(rows[0])])
            half_diag = jnp.where(
                lane1 < 80, pltpu.roll(got[27:28], 80, 1), pltpu.roll(got[28:29], 112, 1)
            )
            tail = jnp.where(
                lane8 < 32,
                pltpu.roll(got[0:8], 32, 1),
                jnp.where(lane8 < 64, pltpu.roll(got[8:16], 64, 1), pltpu.roll(got[16:24], 96, 1)),
            )
            full = jnp.concatenate([got, tail], axis=0)
            top = jnp.where(lane >= row, full, 0.0)
            bottom = jnp.where(
                lane == row + HALF,
                half_diag,
                jnp.where((lane >= HALF) & (lane < row + HALF), pltpu.roll(full, HALF, 1), 0.0),
            )
            high, low = split2(jnp.concatenate([top, bottom], axis=0))
            spread = lax.dot_general(
                jnp.concatenate([high, low], axis=0),
                onehot(ids),
                (((1,), (1,)), ((), ())),
                preferred_element_type=jnp.float32,
            ).astype(jnp.bfloat16)
            spread_ref[buf, NB * k : NB * k + NB, :] = spread[:NB]
            spread_ref[buf, NB * (GROUP + k) : NB * (GROUP + k) + NB, :] = spread[NB:]
        for t in range(3):
            moved = [
                pltpu.roll(pieces[4 * t + q], (32 * (q + 1)) % 128, 1) if q < 3 else pieces[4 * t + q]
                for q in range(4)
            ]
            place = onehot(lanes(moved))
            place_ref[buf, :, 128 * t : 128 * t + 128] = place
            place_ref[buf, :, 128 * (t + 3) : 128 * (t + 3) + 128] = place

    def absorb(buf):
        acc_ref[...] += jnp.dot(
            place_ref[buf], spread_ref[buf], preferred_element_type=jnp.float32
        )

    def step(g, carry):
        generate(0, g * 2 * GROUP)
        absorb(1)
        generate(1, g * 2 * GROUP + GROUP)
        absorb(0)
        return carry

    lax.fori_loop(0, (list_ref[1, 0] + 2 * GROUP - 1) // (2 * GROUP), step, 0)
    absorb(1)
    if not last:
        return
    a11, a22 = acc_ref[:half, :half], acc_ref[half:, half:]
    s11_ref[...] = a11 + a11.T
    s12 = acc_ref[:half, half:] + acc_ref[half:, :half].T
    s12_ref[...] = s12
    low_ref[:, :half] = s12.T
    low_ref[:, half:] = a22 + a22.T


def assemble(base, got, window, prev=None):
    slots = got.shape[0] // ROWS
    half = window // 2
    last = prev is not None
    square = jax.ShapeDtypeStruct((half, half), jnp.float32)
    whole = jax.ShapeDtypeStruct((window, window), jnp.float32)
    scratch = [
        pltpu.VMEM((2, window, 2 * NB * GROUP), jnp.bfloat16),
        pltpu.VMEM((2, 2 * NB * GROUP, window), jnp.bfloat16),
        pltpu.VMEM((8, slots), jnp.int32),
        pltpu.SMEM((8, slots), jnp.int32),
        pltpu.SemaphoreType.DMA,
    ]
    if last:
        scratch = [pltpu.VMEM((window, window), jnp.float32)] + scratch
    out = (square, square, jax.ShapeDtypeStruct((half, window), jnp.float32)) if last else whole
    return pl.pallas_call(
        lambda *refs: assemble_kernel(last, *refs),
        out_shape=out,
        in_specs=[pl.BlockSpec(memory_space=pltpu.SMEM)]
        + [pl.BlockSpec(memory_space=pltpu.VMEM)] * (2 if last else 1),
        scratch_shapes=scratch,
        name="assemble_last" if last else "assemble_first",
    )(*((base, got, prev) if last else (base, got)))


def inverse_kernel(upper_ref, lower_ref, out_ref, mat_ref):
    size = upper_ref.shape[0]
    eye = jnp.where(
        lax.broadcasted_iota(jnp.int32, (size, size), 0)
        == lax.broadcasted_iota(jnp.int32, (size, size), 1),
        1.0,
        0.0,
    )
    mat = upper_ref[...] + lower_ref[:, size:] + eye
    mat_ref[...] = mat
    norm = jnp.max(jnp.sum(jnp.abs(mat), axis=0, keepdims=True))
    out_ref[...] = eye * (2.0 / (norm + 1.0))

    def cond(state):
        turn, gap = state
        return (turn < 48) & (gap > 1e-8)

    def turn(state):
        now = out_ref[...]
        miss = eye - jnp.dot(mat_ref[...], now, precision=HI, preferred_element_type=jnp.float32)
        out_ref[...] = now + jnp.dot(now, miss, precision=HI, preferred_element_type=jnp.float32)
        return state[0] + 1, jnp.sum(miss * miss)

    lax.while_loop(cond, turn, (0, jnp.float32(1.0)))


def invert(upper, lower):
    return pl.pallas_call(
        inverse_kernel,
        out_shape=jax.ShapeDtypeStruct(upper.shape, jnp.float32),
        scratch_shapes=[pltpu.VMEM(upper.shape, jnp.float32)],
        name="invert",
    )(upper, lower)


def mm(left, right, precision=MID):
    return jnp.dot(left, right, precision=precision, preferred_element_type=jnp.float32)


def column_sums(left, right):
    return jnp.sum(left * right, axis=0)


def safe(num, den):
    return jnp.where(den > 0, num / jnp.where(den > 0, den, 1.0), 0.0)


def coefficients(mu):
    m0, m1, m2, m3, m4, m5 = mu
    l1, l2 = safe(m1, m0), safe(m2, m0)
    d1 = m2 - l1 * m1
    e = m3 - l1 * m2
    l21 = safe(e, d1)
    d2 = m4 - l2 * m2 - l21 * e
    y0 = -m3
    y1 = -m4 - l1 * y0
    y2 = -m5 - l2 * y0 - l21 * y1
    b2 = safe(y2, d2)
    b1 = safe(y1, d1) - l21 * b2
    b0 = safe(y0, m0) - l1 * b1 - l2 * b2
    scale = 1.0 / (b0 - b1 + b2 - 1.0)
    c0, c1, c2, c3 = b0 * scale, b1 * scale, b2 * scale, scale
    return (1.0 - c0, c3 - c2, -c3), (c0, c1, c2, c3)


def finish_kernel(blocks_half, sums_ref, v0, w0, *refs):
    halves, (sol_ref, res_ref) = (refs[:5], refs[5:10]), refs[10:]
    x, c = coefficients([sums_ref[k : k + 1, :] for k in range(6)])

    def write(v1, v2, v3, w1, w2):
        sol_ref[...] = x[0] * w0[...] + x[1] * w1[...] + x[2] * w2[...]
        res_ref[...] = c[0] * v0[...] + c[1] * v1[...] + c[2] * v2[...] + c[3] * v3[...]

    for k in range(2):
        pl.when(pl.program_id(0) // blocks_half == k)(lambda k=k: write(*halves[k]))


def finish(sums, v0, w0, halves):
    rows, _ = v0.shape
    width = 256
    per = halves[0][0].shape[1] // width
    whole = pl.BlockSpec((rows, width), lambda j: (0, j))
    left = pl.BlockSpec((rows, width), lambda j: (0, jnp.minimum(j, per - 1)))
    right = pl.BlockSpec((rows, width), lambda j: (0, jnp.maximum(j - per, 0)))
    return pl.pallas_call(
        lambda *refs: finish_kernel(per, *refs),
        grid=(2 * per,),
        in_specs=[pl.BlockSpec((sums.shape[0], width), lambda j: (0, j)), whole, whole]
        + [left] * 5
        + [right] * 5,
        out_specs=(whole, whole),
        out_shape=(jax.ShapeDtypeStruct(v0.shape, v0.dtype),) * 2,
        name="finish",
    )(sums, v0, w0, *halves[0], *halves[1])


def butterfly(x, devices, bits):
    for bit in bits:
        x = x + lax.ppermute(x, AXES, [(i, i ^ bit) for i in range(devices)])
    return x


def body(blocks, connect, owner_map, right_side):
    devices = lax.axis_size(AXES)
    own = right_side.shape[0]
    window = 2 * own
    up = [(i, (i + 1) % devices) for i in range(devices)]
    down = [(b, a) for a, b in up]

    def from_below(x):
        return lax.ppermute(x, AXES, up)

    def from_above(x):
        return lax.ppermute(x, AXES, down)

    base = jnp.stack([lax.axis_index(AXES) * own, own * devices]).astype(jnp.int32)
    send0, send1 = pack(owner_map, connect.T, blocks, devices)

    def exchange(send):
        got = lax.all_to_all(
            send.reshape(devices, ROWS, 128), AXES, split_axis=0, concat_axis=0, tiled=True
        )
        return got.reshape(devices * ROWS, 128)

    got0 = exchange(send0)
    got1 = exchange(send1)
    v0, got0 = lax.optimization_barrier((right_side, got0))
    v0_low, v0_high = from_below(v0), from_above(v0)
    part = assemble(base, got0, window)
    center, high_band, lower = assemble(base, got1, window, part)
    lower = from_below(lower)
    low_band = lower[:, :own]
    inv = invert(center, lower)
    inv_low, inv_high = from_below(inv), from_above(inv)
    near_low, near_high = mm(low_band, inv_low, HI), mm(high_band, inv_high, HI)

    width = right_side.shape[1] // 2

    def part_of(x, h):
        return lax.slice_in_dim(x, h * width, (h + 1) * width, axis=1)

    v1, w1, w1_low, w1_high = {}, {}, {}, {}
    for h in range(2):
        v1[h] = mm(near_low, part_of(v0_low, h)) + mm(near_high, part_of(v0_high, h))
        w1[h] = mm(inv, v1[h])
        w1_low[h] = from_below(w1[h])
        w1_high[h] = from_above(w1[h])
    w0 = mm(inv, right_side)
    v2, w2 = {}, {}
    for h in range(2):
        v2[h] = mm(low_band, w1_low[h]) + mm(high_band, w1_high[h])
        w2[h] = mm(inv, v2[h])
    w2_high, w2_low = {}, {}
    w2_high[0] = from_above(w2[0])
    w2_low[1] = from_below(w2[1])
    later0, later1 = lax.optimization_barrier((w2[0], w2[1]))
    w2_low[0] = from_below(later0)
    w2_high[1] = from_above(later1)
    side = {0: mm(high_band, w2_high[0]), 1: mm(low_band, w2_low[1])}
    sums = []
    for h in range(2):
        v0h, w0h = part_of(right_side, h), part_of(w0, h)
        pairs = [(v0h, w0h), (v1[h], w0h), (v1[h], w1[h]), (v2[h], w1[h]), (v2[h], w2[h])]
        rows = [column_sums(*pair) for pair in pairs] + [2.0 * column_sums(side[h], w2[h])]
        sums.append(jnp.stack(rows))
    sums = jnp.concatenate(sums, axis=1)
    sums = butterfly(sums, devices, (64, 32, 8, 4, 16))
    sums, low_late, high_late = lax.optimization_barrier((sums, low_band, high_band))
    v3 = {0: side[0] + mm(low_late, w2_low[0]), 1: side[1] + mm(high_late, w2_high[1])}
    sums = butterfly(sums, devices, (2, 1))
    return finish(sums, right_side, w0, [(v1[h], v2[h], v3[h], w1[h], w2[h]) for h in range(2)])


def solution(mesh):
    both = P(AXES, None)
    return jax.shard_map(
        body,
        mesh=mesh,
        in_specs=(both, both, P(AXES), both),
        out_specs=(both, both),
        check_vma=False,
    )
```

```python
import jax
import jax.numpy as jnp
from jax import lax
from jax.experimental import pallas as pl
from jax.experimental.pallas import tpu as pltpu
from jax.sharding import PartitionSpec as P


AXES = ("row", "col")
NB = 96
HALF = 48
ROWS = 40
GROUP = 4
HI = lax.Precision.HIGHEST
MID = lax.Precision.HIGH


def split2(x):
    high = x.astype(jnp.bfloat16)
    low = (x - high.astype(jnp.float32)).astype(jnp.bfloat16)
    return high, low


def pack_kernel(owner_ref, ids_ref, x_ref, out0_ref, out1_ref, tail_ref):
    subs = x_ref.shape[0]
    devs = out0_ref.shape[0] // ROWS
    sub = lax.broadcasted_iota(jnp.int32, (devs, subs), 0)
    here = sub == owner_ref[...]
    before = lax.broadcasted_iota(jnp.int32, (subs, subs), 0) < lax.broadcasted_iota(
        jnp.int32, (subs, subs), 1
    )
    count = jnp.dot(
        here.astype(jnp.bfloat16), before.astype(jnp.bfloat16), preferred_element_type=jnp.float32
    )
    first = jnp.where(here & (count < 0.5), 1.0, 0.0).astype(jnp.bfloat16)
    second = jnp.where(here & (count > 0.5), 1.0, 0.0).astype(jnp.bfloat16)
    pick = jnp.concatenate([first, second], axis=0)
    ids = ids_ref[...].astype(jnp.float32).T + 1.0
    ids = jnp.concatenate([ids, jnp.zeros((subs, 128 - NB), jnp.float32)], axis=1)
    pick = jnp.concatenate([pick, pick], axis=1)
    lane = lax.broadcasted_iota(jnp.int32, (subs, 128), 1)

    def flat(start):
        tile, off = divmod(start, 128)
        if off == 0:
            return x_ref[:, tile * 128 : tile * 128 + 128]
        one = pltpu.roll(x_ref[:, tile * 128 : tile * 128 + 128], 128 - off, 1)
        if (tile + 1) * 128 >= x_ref.shape[1]:
            return one
        two = pltpu.roll(x_ref[:, tile * 128 + 128 : tile * 128 + 256], 128 - off, 1)
        return jnp.where(lane < 128 - off, one, two)

    diag = jnp.zeros((subs, 128), jnp.float32)

    def wrow(i, diag):
        top = flat(NB * i)
        bottom = flat(NB * (i + HALF) + HALF)
        row = jnp.where(lane < i, bottom, jnp.where(lane == i, 0.5 * top, top))
        return row, jnp.where(lane == i, 0.5 * bottom, diag)

    for m in range(8):
        row, diag = wrow(ROWS + m, diag)
        tail_ref[m] = row
    order = [i for i in range(0, ROWS, 2) if i not in (26, 28)] + [26, 28]
    kept = {}
    for i in (26, 27, 28, 29):
        kept[i], diag = wrow(i, diag)
    for i0 in order:
        tiles = []
        for i in (i0, i0 + 1):
            if i in kept:
                row = kept[i]
            else:
                row, diag = wrow(i, diag)
            if i < 24:
                extra = pltpu.roll(tail_ref[i % 8], 96 - 32 * (i // 8), 1)
            elif i < 27:
                extra = pltpu.roll(ids, 96 - 32 * (i - 24), 1)
            elif i < 29:
                extra = pltpu.roll(diag, 96 - 32 * (i - 27), 1)
            else:
                extra = jnp.zeros_like(row)
            tiles.append(jnp.where(lane < NB, row, extra))
        high, low = split2(jnp.concatenate(tiles, axis=1))
        out = jnp.dot(
            pick, jnp.concatenate([high, low], axis=0), preferred_element_type=jnp.float32
        )
        for k in range(2):
            part = out[:, 128 * k : 128 * k + 128]
            out0_ref[pl.ds(i0 + k, devs, stride=ROWS), :] = part[:devs]
            out1_ref[pl.ds(i0 + k, devs, stride=ROWS), :] = part[devs:]


def pack(owner_map, ids, blocks, devices):
    shape = jax.ShapeDtypeStruct((devices * ROWS, 128), jnp.float32)
    return pl.pallas_call(
        pack_kernel,
        out_shape=(shape, shape),
        scratch_shapes=[pltpu.VMEM((8, blocks.shape[0], 128), jnp.float32)],
        name="pack",
    )(owner_map.reshape(1, -1), ids, blocks)


def assemble_kernel(last, base_ref, got_ref, *refs):
    place_ref, spread_ref, vec_ref, list_ref, sem = refs[-5:]
    if last:
        prev_ref, s11_ref, s12_ref, low_ref, acc_ref = refs[:5]
    else:
        acc_ref = refs[0]
    window = acc_ref.shape[0]
    half = window // 2
    slots = got_ref.shape[0] // ROWS
    lane = lax.broadcasted_iota(jnp.int32, (slots, slots), 1)
    sub = lax.broadcasted_iota(jnp.int32, (slots, slots), 0)
    filled = got_ref[pl.ds(24, slots, stride=ROWS), :][:, NB : NB + 1] > 0.5
    filled = jnp.broadcast_to(jnp.where(filled, 1.0, 0.0), (slots, slots))
    rank = jnp.dot(
        jnp.where(lane < sub, 1.0, 0.0).astype(jnp.bfloat16),
        filled.astype(jnp.bfloat16),
        preferred_element_type=jnp.float32,
    )
    subf = sub.astype(jnp.float32)
    hit = (filled > 0.5) & (rank == lane.astype(jnp.float32))
    count = jnp.sum(filled, axis=0, keepdims=True)
    spare = jnp.max(jnp.where(filled > 0.5, 0.0, subf), axis=0, keepdims=True)
    chosen = jnp.sum(jnp.where(hit, subf, 0.0), axis=0, keepdims=True)
    chosen = jnp.where(lane[:1].astype(jnp.float32) < count, chosen, spare)
    first_row = lax.broadcasted_iota(jnp.int32, (8, slots), 0) == 0
    vec_ref[...] = jnp.where(first_row, chosen, count).astype(jnp.int32)
    copy = pltpu.make_async_copy(vec_ref, list_ref, sem)
    copy.start()
    acc_ref[...] = prev_ref[...] if last else jnp.zeros_like(acc_ref)
    place_ref[1] = jnp.zeros(place_ref.shape[1:], jnp.bfloat16)
    spread_ref[1] = jnp.zeros(spread_ref.shape[1:], jnp.bfloat16)
    copy.wait()

    lane = lax.broadcasted_iota(jnp.int32, (HALF, 128), 1)
    row = lax.broadcasted_iota(jnp.int32, (HALF, 128), 0)
    lane1 = lax.broadcasted_iota(jnp.int32, (1, 128), 1)
    lane8 = lax.broadcasted_iota(jnp.int32, (8, 128), 1)
    target = lax.broadcasted_iota(jnp.int32, (window, 128), 0).astype(jnp.float32)
    start = base_ref[0].astype(jnp.float32)
    total = base_ref[1].astype(jnp.float32)

    def local(ids):
        moved = ids - 1.0 - start
        return jnp.where(ids > 0.5, jnp.where(moved < 0.0, moved + total, moved), -1.0)


    def lanes(pieces):
        out = pieces[3]
        for k in (2, 1, 0):
            out = jnp.where(lane1 < 32 * (k + 1), pieces[k], out)
        return out

    def onehot(ids):
        return jnp.where(target == local(ids), 1.0, 0.0).astype(jnp.bfloat16)

    def generate(buf, first):
        pieces = []
        for k in range(GROUP):
            slot = list_ref[0, first + k]
            base = pl.multiple_of(slot * ROWS, 8)
            got = got_ref[pl.ds(base, ROWS), :]
            rows = [got[24 + m : 25 + m] for m in range(3)]
            pieces += rows
            ids = lanes([pltpu.roll(rows[m], 32 * (m + 1), 1) for m in range(3)] + [jnp.zeros_like(rows[0])])
            half_diag = jnp.where(
                lane1 < 80, pltpu.roll(got[27:28], 80, 1), pltpu.roll(got[28:29], 112, 1)
            )
            tail = jnp.where(
                lane8 < 32,
                pltpu.roll(got[0:8], 32, 1),
                jnp.where(lane8 < 64, pltpu.roll(got[8:16], 64, 1), pltpu.roll(got[16:24], 96, 1)),
            )
            full = jnp.concatenate([got, tail], axis=0)
            top = jnp.where(lane >= row, full, 0.0)
            bottom = jnp.where(
                lane == row + HALF,
                half_diag,
                jnp.where((lane >= HALF) & (lane < row + HALF), pltpu.roll(full, HALF, 1), 0.0),
            )
            high, low = split2(jnp.concatenate([top, bottom], axis=0))
            spread = lax.dot_general(
                jnp.concatenate([high, low], axis=0),
                onehot(ids),
                (((1,), (1,)), ((), ())),
                preferred_element_type=jnp.float32,
            ).astype(jnp.bfloat16)
            spread_ref[buf, NB * k : NB * k + NB, :] = spread[:NB]
            spread_ref[buf, NB * (GROUP + k) : NB * (GROUP + k) + NB, :] = spread[NB:]
        for t in range(3):
            moved = [
                pltpu.roll(pieces[4 * t + q], (32 * (q + 1)) % 128, 1) if q < 3 else pieces[4 * t + q]
                for q in range(4)
            ]
            place = onehot(lanes(moved))
            place_ref[buf, :, 128 * t : 128 * t + 128] = place
            place_ref[buf, :, 128 * (t + 3) : 128 * (t + 3) + 128] = place

    def absorb(buf):
        acc_ref[...] += jnp.dot(
            place_ref[buf], spread_ref[buf], preferred_element_type=jnp.float32
        )

    def step(g, carry):
        generate(0, g * 2 * GROUP)
        absorb(1)
        generate(1, g * 2 * GROUP + GROUP)
        absorb(0)
        return carry

    lax.fori_loop(0, (list_ref[1, 0] + 2 * GROUP - 1) // (2 * GROUP), step, 0)
    absorb(1)
    if not last:
        return
    a11, a22 = acc_ref[:half, :half], acc_ref[half:, half:]
    s11_ref[...] = a11 + a11.T
    s12 = acc_ref[:half, half:] + acc_ref[half:, :half].T
    s12_ref[...] = s12
    low_ref[:, :half] = s12.T
    low_ref[:, half:] = a22 + a22.T


def assemble(base, got, window, prev=None):
    slots = got.shape[0] // ROWS
    half = window // 2
    last = prev is not None
    square = jax.ShapeDtypeStruct((half, half), jnp.float32)
    whole = jax.ShapeDtypeStruct((window, window), jnp.float32)
    scratch = [
        pltpu.VMEM((2, window, 2 * NB * GROUP), jnp.bfloat16),
        pltpu.VMEM((2, 2 * NB * GROUP, window), jnp.bfloat16),
        pltpu.VMEM((8, slots), jnp.int32),
        pltpu.SMEM((8, slots), jnp.int32),
        pltpu.SemaphoreType.DMA,
    ]
    if last:
        scratch = [pltpu.VMEM((window, window), jnp.float32)] + scratch
    out = (square, square, jax.ShapeDtypeStruct((half, window), jnp.float32)) if last else whole
    return pl.pallas_call(
        lambda *refs: assemble_kernel(last, *refs),
        out_shape=out,
        in_specs=[pl.BlockSpec(memory_space=pltpu.SMEM)]
        + [pl.BlockSpec(memory_space=pltpu.VMEM)] * (2 if last else 1),
        scratch_shapes=scratch,
        name="assemble_last" if last else "assemble_first",
    )(*((base, got, prev) if last else (base, got)))


def inverse_kernel(upper_ref, lower_ref, out_ref, mat_ref):
    size = upper_ref.shape[0]
    eye = jnp.where(
        lax.broadcasted_iota(jnp.int32, (size, size), 0)
        == lax.broadcasted_iota(jnp.int32, (size, size), 1),
        1.0,
        0.0,
    )
    mat = upper_ref[...] + lower_ref[:, size:] + eye
    mat_ref[...] = mat
    norm = jnp.max(jnp.sum(jnp.abs(mat), axis=0, keepdims=True))
    out_ref[...] = eye * (2.0 / (norm + 1.0))

    def cond(state):
        turn, gap = state
        return (turn < 48) & (gap > 1e-8)

    def turn(state):
        now = out_ref[...]
        miss = eye - jnp.dot(mat_ref[...], now, precision=HI, preferred_element_type=jnp.float32)
        out_ref[...] = now + jnp.dot(now, miss, precision=HI, preferred_element_type=jnp.float32)
        return state[0] + 1, jnp.sum(miss * miss)

    lax.while_loop(cond, turn, (0, jnp.float32(1.0)))


def invert(upper, lower):
    return pl.pallas_call(
        inverse_kernel,
        out_shape=jax.ShapeDtypeStruct(upper.shape, jnp.float32),
        scratch_shapes=[pltpu.VMEM(upper.shape, jnp.float32)],
        name="invert",
    )(upper, lower)


def mm(left, right, precision=MID):
    return jnp.dot(left, right, precision=precision, preferred_element_type=jnp.float32)


def column_sums(left, right):
    return jnp.sum(left * right, axis=0)


def safe(num, den):
    return jnp.where(den > 0, num / jnp.where(den > 0, den, 1.0), 0.0)


def coefficients(mu):
    m0, m1, m2, m3, m4, m5 = mu
    l1, l2 = safe(m1, m0), safe(m2, m0)
    d1 = m2 - l1 * m1
    e = m3 - l1 * m2
    l21 = safe(e, d1)
    d2 = m4 - l2 * m2 - l21 * e
    y0 = -m3
    y1 = -m4 - l1 * y0
    y2 = -m5 - l2 * y0 - l21 * y1
    b2 = safe(y2, d2)
    b1 = safe(y1, d1) - l21 * b2
    b0 = safe(y0, m0) - l1 * b1 - l2 * b2
    scale = 1.0 / (b0 - b1 + b2 - 1.0)
    c0, c1, c2, c3 = b0 * scale, b1 * scale, b2 * scale, scale
    return (1.0 - c0, c3 - c2, -c3), (c0, c1, c2, c3)


def finish_kernel(per, sums_ref, v0, w0, v1, w1, *refs):
    halves, (sol_ref, res_ref) = (refs[:3], refs[3:6]), refs[6:]
    x, c = coefficients([sums_ref[k : k + 1, :] for k in range(6)])

    def write(v2, v3, w2):
        sol_ref[...] = x[0] * w0[...] + x[1] * w1[...] + x[2] * w2[...]
        res_ref[...] = c[0] * v0[...] + c[1] * v1[...] + c[2] * v2[...] + c[3] * v3[...]

    for k in range(2):
        pl.when(pl.program_id(0) // per == k)(lambda k=k: write(*halves[k]))


def finish(sums, wholes, halves):
    rows, total = wholes[0].shape
    width = 256
    per = total // 2 // width
    whole = pl.BlockSpec((rows, width), lambda j: (0, j))
    left = pl.BlockSpec((rows, width), lambda j: (0, jnp.minimum(j, per - 1)))
    right = pl.BlockSpec((rows, width), lambda j: (0, jnp.maximum(j - per, 0)))
    return pl.pallas_call(
        lambda *refs: finish_kernel(per, *refs),
        grid=(2 * per,),
        in_specs=[pl.BlockSpec((sums.shape[0], width), lambda j: (0, j))]
        + [whole] * 4
        + [left] * 3
        + [right] * 3,
        out_specs=(whole, whole),
        out_shape=(jax.ShapeDtypeStruct((rows, total), jnp.float32),) * 2,
        name="finish",
    )(sums, *wholes, *halves[0], *halves[1])


def butterfly(x, devices, bits):
    for bit in bits:
        x = x + lax.ppermute(x, AXES, [(i, i ^ bit) for i in range(devices)])
    return x


def body(blocks, connect, owner_map, right_side):
    devices = lax.axis_size(AXES)
    own = right_side.shape[0]
    window = 2 * own
    up = [(i, (i + 1) % devices) for i in range(devices)]
    down = [(b, a) for a, b in up]

    def from_below(x):
        return lax.ppermute(x, AXES, up)

    def from_above(x):
        return lax.ppermute(x, AXES, down)

    base = jnp.stack([lax.axis_index(AXES) * own, own * devices]).astype(jnp.int32)
    v0_low = from_below(right_side)
    v0_high = from_above(right_side)
    send0, send1 = pack(owner_map, connect.T, blocks, devices)

    def exchange(send):
        got = lax.all_to_all(
            send.reshape(devices, ROWS, 128), AXES, split_axis=0, concat_axis=0, tiled=True
        )
        return got.reshape(devices * ROWS, 128)

    got0 = exchange(send0)
    got1 = exchange(send1)
    part = assemble(base, got0, window)
    center, high_band, lower = assemble(base, got1, window, part)
    lower = from_below(lower)
    low_band = lower[:, :own]
    inv = invert(center, lower)
    inv_low, inv_high = from_below(inv), from_above(inv)
    near_low, near_high = mm(low_band, inv_low, HI), mm(high_band, inv_high, HI)

    width = right_side.shape[1] // 2

    def part_of(x, h):
        return lax.slice_in_dim(x, h * width, (h + 1) * width, axis=1)

    v1 = mm(near_low, v0_low) + mm(near_high, v0_high)
    w1 = mm(inv, v1)
    w1_low, w1_high = from_below(w1), from_above(w1)
    w0 = mm(inv, right_side)
    v2, w2 = {}, {}
    for h in range(2):
        v2[h] = mm(low_band, part_of(w1_low, h)) + mm(high_band, part_of(w1_high, h))
        w2[h] = mm(inv, v2[h])
    w2_high, w2_low = {}, {}
    w2_high[0] = from_above(w2[0])
    w2_low[1] = from_below(w2[1])
    w2_high[0], w2_low[1], later0, later1 = lax.optimization_barrier(
        (w2_high[0], w2_low[1], w2[0], w2[1])
    )
    w2_low[0] = from_below(later0)
    w2_high[1] = from_above(later1)
    side = {0: mm(high_band, w2_high[0]), 1: mm(low_band, w2_low[1])}
    sums = []
    for h in range(2):
        v0h, w0h, v1h, w1h = (part_of(x, h) for x in (right_side, w0, v1, w1))
        pairs = [(v0h, w0h), (v1h, w0h), (v1h, w1h), (v2[h], w1h), (v2[h], w2[h])]
        rows = [column_sums(*pair) for pair in pairs] + [2.0 * column_sums(side[h], w2[h])]
        sums.append(jnp.stack(rows))
    sums = jnp.concatenate(sums, axis=1)
    sums = butterfly(sums, devices, (64, 32, 8, 4, 16))
    sums, low_late, high_late = lax.optimization_barrier((sums, low_band, high_band))
    v3 = {0: side[0] + mm(low_late, w2_low[0]), 1: side[1] + mm(high_late, w2_high[1])}
    sums = butterfly(sums, devices, (2, 1))
    return finish(sums, (right_side, w0, v1, w1), [(v2[h], v3[h], w2[h]) for h in range(2)])


def solution(mesh):
    both = P(AXES, None)
    return jax.shard_map(
        body,
        mesh=mesh,
        in_specs=(both, both, P(AXES), both),
        out_specs=(both, both),
        check_vma=False,
    )
```

```python
import jax
import jax.numpy as jnp
from jax import lax
from jax.experimental import pallas as pl
from jax.experimental.pallas import tpu as pltpu
from jax.sharding import PartitionSpec as P


AXES = ("row", "col")
NB = 96
HALF = 48
ROWS = 40
GROUP = 4
HI = lax.Precision.HIGHEST


def split2(x):
    high = x.astype(jnp.bfloat16)
    low = (x - high.astype(jnp.float32)).astype(jnp.bfloat16)
    return high, low


def pack_kernel(owner_ref, ids_ref, x_ref, out0_ref, out1_ref, tail_ref):
    subs = x_ref.shape[0]
    devs = out0_ref.shape[0] // ROWS
    sub = lax.broadcasted_iota(jnp.int32, (devs, subs), 0)
    here = sub == owner_ref[...]
    before = lax.broadcasted_iota(jnp.int32, (subs, subs), 0) < lax.broadcasted_iota(
        jnp.int32, (subs, subs), 1
    )
    count = jnp.dot(
        here.astype(jnp.bfloat16), before.astype(jnp.bfloat16), preferred_element_type=jnp.float32
    )
    first = jnp.where(here & (count < 0.5), 1.0, 0.0).astype(jnp.bfloat16)
    second = jnp.where(here & (count > 0.5), 1.0, 0.0).astype(jnp.bfloat16)
    pick = jnp.concatenate([first, second], axis=0)
    ids = ids_ref[...].astype(jnp.float32).T + 1.0
    ids = jnp.concatenate([ids, jnp.zeros((subs, 128 - NB), jnp.float32)], axis=1)
    pick = jnp.concatenate([pick, pick], axis=1)
    lane = lax.broadcasted_iota(jnp.int32, (subs, 128), 1)

    def flat(start):
        tile, off = divmod(start, 128)
        if off == 0:
            return x_ref[:, tile * 128 : tile * 128 + 128]
        one = pltpu.roll(x_ref[:, tile * 128 : tile * 128 + 128], 128 - off, 1)
        if (tile + 1) * 128 >= x_ref.shape[1]:
            return one
        two = pltpu.roll(x_ref[:, tile * 128 + 128 : tile * 128 + 256], 128 - off, 1)
        return jnp.where(lane < 128 - off, one, two)

    diag = jnp.zeros((subs, 128), jnp.float32)

    def wrow(i, diag):
        top = flat(NB * i)
        bottom = flat(NB * (i + HALF) + HALF)
        row = jnp.where(lane < i, bottom, jnp.where(lane == i, 0.5 * top, top))
        return row, jnp.where(lane == i, 0.5 * bottom, diag)

    for m in range(8):
        row, diag = wrow(ROWS + m, diag)
        tail_ref[m] = row
    order = [i for i in range(0, ROWS, 2) if i not in (26, 28)] + [26, 28]
    kept = {}
    for i in (26, 27, 28, 29):
        kept[i], diag = wrow(i, diag)
    for i0 in order:
        tiles = []
        for i in (i0, i0 + 1):
            if i in kept:
                row = kept[i]
            else:
                row, diag = wrow(i, diag)
            if i < 24:
                extra = pltpu.roll(tail_ref[i % 8], 96 - 32 * (i // 8), 1)
            elif i < 27:
                extra = pltpu.roll(ids, 96 - 32 * (i - 24), 1)
            elif i < 29:
                extra = pltpu.roll(diag, 96 - 32 * (i - 27), 1)
            else:
                extra = jnp.zeros_like(row)
            tiles.append(jnp.where(lane < NB, row, extra))
        high, low = split2(jnp.concatenate(tiles, axis=1))
        out = jnp.dot(
            pick, jnp.concatenate([high, low], axis=0), preferred_element_type=jnp.float32
        )
        for k in range(2):
            part = out[:, 128 * k : 128 * k + 128]
            out0_ref[pl.ds(i0 + k, devs, stride=ROWS), :] = part[:devs]
            out1_ref[pl.ds(i0 + k, devs, stride=ROWS), :] = part[devs:]


def pack(owner_map, ids, blocks, devices):
    shape = jax.ShapeDtypeStruct((devices * ROWS, 128), jnp.float32)
    return pl.pallas_call(
        pack_kernel,
        out_shape=(shape, shape),
        scratch_shapes=[pltpu.VMEM((8, blocks.shape[0], 128), jnp.float32)],
        name="pack",
    )(owner_map.reshape(1, -1), ids, blocks)


def assemble_kernel(last, base_ref, got_ref, *refs):
    place_ref, spread_ref, vec_ref, list_ref, sem = refs[-5:]
    if last:
        prev_ref, s11_ref, s12_ref, low_ref, acc_ref = refs[:5]
    else:
        acc_ref = refs[0]
    window = acc_ref.shape[0]
    half = window // 2
    slots = got_ref.shape[0] // ROWS
    lane = lax.broadcasted_iota(jnp.int32, (slots, slots), 1)
    sub = lax.broadcasted_iota(jnp.int32, (slots, slots), 0)
    filled = got_ref[pl.ds(24, slots, stride=ROWS), :][:, NB : NB + 1] > 0.5
    filled = jnp.broadcast_to(jnp.where(filled, 1.0, 0.0), (slots, slots))
    rank = jnp.dot(
        jnp.where(lane < sub, 1.0, 0.0).astype(jnp.bfloat16),
        filled.astype(jnp.bfloat16),
        preferred_element_type=jnp.float32,
    )
    subf = sub.astype(jnp.float32)
    hit = (filled > 0.5) & (rank == lane.astype(jnp.float32))
    count = jnp.sum(filled, axis=0, keepdims=True)
    spare = jnp.max(jnp.where(filled > 0.5, 0.0, subf), axis=0, keepdims=True)
    chosen = jnp.sum(jnp.where(hit, subf, 0.0), axis=0, keepdims=True)
    chosen = jnp.where(lane[:1].astype(jnp.float32) < count, chosen, spare)
    first_row = lax.broadcasted_iota(jnp.int32, (8, slots), 0) == 0
    vec_ref[...] = jnp.where(first_row, chosen, count).astype(jnp.int32)
    copy = pltpu.make_async_copy(vec_ref, list_ref, sem)
    copy.start()
    acc_ref[...] = prev_ref[...] if last else jnp.zeros_like(acc_ref)
    place_ref[1] = jnp.zeros(place_ref.shape[1:], jnp.bfloat16)
    spread_ref[1] = jnp.zeros(spread_ref.shape[1:], jnp.bfloat16)
    copy.wait()

    lane = lax.broadcasted_iota(jnp.int32, (HALF, 128), 1)
    row = lax.broadcasted_iota(jnp.int32, (HALF, 128), 0)
    lane1 = lax.broadcasted_iota(jnp.int32, (1, 128), 1)
    lane8 = lax.broadcasted_iota(jnp.int32, (8, 128), 1)
    target = lax.broadcasted_iota(jnp.int32, (window, 128), 0).astype(jnp.float32)
    start = base_ref[0].astype(jnp.float32)
    total = base_ref[1].astype(jnp.float32)

    def local(ids):
        moved = ids - 1.0 - start
        return jnp.where(ids > 0.5, jnp.where(moved < 0.0, moved + total, moved), -1.0)


    def lanes(pieces):
        out = pieces[3]
        for k in (2, 1, 0):
            out = jnp.where(lane1 < 32 * (k + 1), pieces[k], out)
        return out

    def onehot(ids):
        return jnp.where(target == local(ids), 1.0, 0.0).astype(jnp.bfloat16)

    def generate(buf, first):
        pieces = []
        for k in range(GROUP):
            slot = list_ref[0, first + k]
            base = pl.multiple_of(slot * ROWS, 8)
            got = got_ref[pl.ds(base, ROWS), :]
            rows = [got[24 + m : 25 + m] for m in range(3)]
            pieces += rows
            ids = lanes([pltpu.roll(rows[m], 32 * (m + 1), 1) for m in range(3)] + [jnp.zeros_like(rows[0])])
            half_diag = jnp.where(
                lane1 < 80, pltpu.roll(got[27:28], 80, 1), pltpu.roll(got[28:29], 112, 1)
            )
            tail = jnp.where(
                lane8 < 32,
                pltpu.roll(got[0:8], 32, 1),
                jnp.where(lane8 < 64, pltpu.roll(got[8:16], 64, 1), pltpu.roll(got[16:24], 96, 1)),
            )
            full = jnp.concatenate([got, tail], axis=0)
            top = jnp.where(lane >= row, full, 0.0)
            bottom = jnp.where(
                lane == row + HALF,
                half_diag,
                jnp.where((lane >= HALF) & (lane < row + HALF), pltpu.roll(full, HALF, 1), 0.0),
            )
            high, low = split2(jnp.concatenate([top, bottom], axis=0))
            spread = lax.dot_general(
                jnp.concatenate([high, low], axis=0),
                onehot(ids),
                (((1,), (1,)), ((), ())),
                preferred_element_type=jnp.float32,
            ).astype(jnp.bfloat16)
            spread_ref[buf, NB * k : NB * k + NB, :] = spread[:NB]
            spread_ref[buf, NB * (GROUP + k) : NB * (GROUP + k) + NB, :] = spread[NB:]
        for t in range(3):
            moved = [
                pltpu.roll(pieces[4 * t + q], (32 * (q + 1)) % 128, 1) if q < 3 else pieces[4 * t + q]
                for q in range(4)
            ]
            place = onehot(lanes(moved))
            place_ref[buf, :, 128 * t : 128 * t + 128] = place
            place_ref[buf, :, 128 * (t + 3) : 128 * (t + 3) + 128] = place

    def absorb(buf):
        acc_ref[...] += jnp.dot(
            place_ref[buf], spread_ref[buf], preferred_element_type=jnp.float32
        )

    def step(g, carry):
        generate(0, g * 2 * GROUP)
        absorb(1)
        generate(1, g * 2 * GROUP + GROUP)
        absorb(0)
        return carry

    lax.fori_loop(0, (list_ref[1, 0] + 2 * GROUP - 1) // (2 * GROUP), step, 0)
    absorb(1)
    if not last:
        return
    a11, a22 = acc_ref[:half, :half], acc_ref[half:, half:]
    s11_ref[...] = a11 + a11.T
    s12 = acc_ref[:half, half:] + acc_ref[half:, :half].T
    s12_ref[...] = s12
    low_ref[:, :half] = s12.T
    low_ref[:, half:] = a22 + a22.T


def assemble(base, got, window, prev=None):
    slots = got.shape[0] // ROWS
    half = window // 2
    last = prev is not None
    square = jax.ShapeDtypeStruct((half, half), jnp.float32)
    whole = jax.ShapeDtypeStruct((window, window), jnp.float32)
    scratch = [
        pltpu.VMEM((2, window, 2 * NB * GROUP), jnp.bfloat16),
        pltpu.VMEM((2, 2 * NB * GROUP, window), jnp.bfloat16),
        pltpu.VMEM((8, slots), jnp.int32),
        pltpu.SMEM((8, slots), jnp.int32),
        pltpu.SemaphoreType.DMA,
    ]
    if last:
        scratch = [pltpu.VMEM((window, window), jnp.float32)] + scratch
    out = (square, square, jax.ShapeDtypeStruct((half, window), jnp.float32)) if last else whole
    return pl.pallas_call(
        lambda *refs: assemble_kernel(last, *refs),
        out_shape=out,
        in_specs=[pl.BlockSpec(memory_space=pltpu.SMEM)]
        + [pl.BlockSpec(memory_space=pltpu.VMEM)] * (2 if last else 1),
        scratch_shapes=scratch,
        name="assemble_last" if last else "assemble_first",
    )(*((base, got, prev) if last else (base, got)))


def inverse_kernel(upper_ref, lower_ref, out_ref, mat_ref):
    size = upper_ref.shape[0]
    eye = jnp.where(
        lax.broadcasted_iota(jnp.int32, (size, size), 0)
        == lax.broadcasted_iota(jnp.int32, (size, size), 1),
        1.0,
        0.0,
    )
    mat = upper_ref[...] + lower_ref[:, size:] + eye
    mat_ref[...] = mat
    norm = jnp.max(jnp.sum(jnp.abs(mat), axis=0, keepdims=True))
    out_ref[...] = eye * (2.0 / (norm + 1.0))

    def cond(state):
        turn, gap = state
        return (turn < 48) & (gap > 1e-8)

    def turn(state):
        now = out_ref[...]
        miss = eye - jnp.dot(mat_ref[...], now, precision=HI, preferred_element_type=jnp.float32)
        out_ref[...] = now + jnp.dot(now, miss, precision=HI, preferred_element_type=jnp.float32)
        return state[0] + 1, jnp.sum(miss * miss)

    lax.while_loop(cond, turn, (0, jnp.float32(1.0)))


def invert(upper, lower):
    return pl.pallas_call(
        inverse_kernel,
        out_shape=jax.ShapeDtypeStruct(upper.shape, jnp.float32),
        scratch_shapes=[pltpu.VMEM(upper.shape, jnp.float32)],
        name="invert",
    )(upper, lower)


def mm(left, right):
    return jnp.dot(left, right, precision=HI, preferred_element_type=jnp.float32)


def left3(x):
    high, low = split2(x)
    return jnp.concatenate([high, high, low], axis=1)


def right3(x):
    high, low = split2(x)
    return jnp.concatenate([high, low, high], axis=0)


def dot3(left, right):
    return jnp.dot(left, right, preferred_element_type=jnp.float32)


def at_row(k, value):
    row = lax.broadcasted_iota(jnp.int32, (8, value.shape[1]), 0)
    return jnp.where(row == k, value, 0.0)


def sums_of(left, right):
    return jnp.sum(left * right, axis=0, keepdims=True)


BLOCK = 256


def in_blocks(kernel, matrices, wholes, lefts, rights, sums, outs):
    rows = matrices[0].shape[0]
    per = (lefts + rights)[0].shape[1] // BLOCK if lefts else wholes[0].shape[1] // BLOCK // 2
    square = pl.BlockSpec((rows, rows), lambda j: (0, 0))
    maps = {
        "whole": lambda j: (0, j),
        "left": lambda j: (0, jnp.minimum(j, per - 1)),
        "right": lambda j: (0, jnp.maximum(j - per, 0)),
        "sums": lambda j: (0, j),
    }

    def spec(kind):
        return pl.BlockSpec((8 if kind == "sums" else rows, BLOCK), maps[kind])

    total = 2 * per * BLOCK
    shapes = {
        "whole": (rows, total),
        "left": (rows, total // 2),
        "right": (rows, total // 2),
        "sums": (8, total),
    }
    return pl.pallas_call(
        lambda *refs: kernel(pl.program_id(0) < per, *refs),
        grid=(2 * per,),
        in_specs=[square] * len(matrices)
        + [spec("whole")] * len(wholes)
        + [spec("left")] * len(lefts)
        + [spec("right")] * len(rights)
        + [spec("sums")] * len(sums),
        out_specs=tuple(spec(kind) for kind in outs),
        out_shape=tuple(jax.ShapeDtypeStruct(shapes[kind], jnp.float32) for kind in outs),
    )(*matrices, *wholes, *lefts, *rights, *sums)


def first_kernel(is_left, low, high, inv, low0, high0, low1, high1, v_ref, w_ref, m_ref):
    def run(x_low, x_high):
        v = dot3(left3(low[...]), right3(x_low[...])) + dot3(left3(high[...]), right3(x_high[...]))
        w = dot3(left3(inv[...]), right3(v))
        v_ref[...] = v
        w_ref[...] = w
        m_ref[...] = at_row(2, sums_of(v, w))

    pl.when(is_left)(lambda: run(low0, high0))
    pl.when(jnp.logical_not(is_left))(lambda: run(low1, high1))


def start_kernel(is_left, inv, v0, v1, m_in, w_ref, m_ref):
    w = dot3(left3(inv[...]), right3(v0[...]))
    w_ref[...] = w
    m_ref[...] = m_in[...] + at_row(0, sums_of(v0[...], w)) + at_row(1, sums_of(v1[...], w))


def second_kernel(is_left, low, high, inv, x_low, x_high, w1, m_in, v_ref, left_ref, right_ref, m_ref):
    v = dot3(left3(low[...]), right3(x_low[...])) + dot3(left3(high[...]), right3(x_high[...]))
    w = dot3(left3(inv[...]), right3(v))
    v_ref[...] = v
    m_ref[...] = m_in[...] + at_row(3, sums_of(v, w1[...])) + at_row(4, sums_of(v, w))

    @pl.when(is_left)
    def _():
        left_ref[...] = w

    @pl.when(jnp.logical_not(is_left))
    def _():
        right_ref[...] = w


def side_kernel(is_left, low, high, w0_half, x_high, w1_half, x_low, m_in, t_ref, m_ref):
    def run(band, x, w):
        t = dot3(left3(band[...]), right3(x[...]))
        t_ref[...] = t
        m_ref[...] = m_in[...] + at_row(5, 2.0 * sums_of(t, w[...]))

    pl.when(is_left)(lambda: run(high, x_high, w0_half))
    pl.when(jnp.logical_not(is_left))(lambda: run(low, x_low, w1_half))


def safe(num, den):
    return jnp.where(den > 0, num / jnp.where(den > 0, den, 1.0), 0.0)


def coefficients(mu):
    m0, m1, m2, m3, m4, m5 = mu
    l1, l2 = safe(m1, m0), safe(m2, m0)
    d1 = m2 - l1 * m1
    e = m3 - l1 * m2
    l21 = safe(e, d1)
    d2 = m4 - l2 * m2 - l21 * e
    y0 = -m3
    y1 = -m4 - l1 * y0
    y2 = -m5 - l2 * y0 - l21 * y1
    b2 = safe(y2, d2)
    b1 = safe(y1, d1) - l21 * b2
    b0 = safe(y0, m0) - l1 * b1 - l2 * b2
    scale = 1.0 / (b0 - b1 + b2 - 1.0)
    c0, c1, c2, c3 = b0 * scale, b1 * scale, b2 * scale, scale
    return (1.0 - c0, c3 - c2, -c3), (c0, c1, c2, c3)


def finish_kernel(
    is_left, low, high, v0, w0, v1, w1, v2, t, w2_0, x_low, w2_1, x_high, sums, sol_ref, res_ref
):
    x, c = coefficients([sums[k : k + 1, :] for k in range(6)])

    def run(band, far, w2):
        v3 = t[...] + dot3(left3(band[...]), right3(far[...]))
        sol_ref[...] = x[0] * w0[...] + x[1] * w1[...] + x[2] * w2[...]
        res_ref[...] = c[0] * v0[...] + c[1] * v1[...] + c[2] * v2[...] + c[3] * v3

    pl.when(is_left)(lambda: run(low, x_low, w2_0))
    pl.when(jnp.logical_not(is_left))(lambda: run(high, x_high, w2_1))


def butterfly(x, devices, bits):
    for bit in bits:
        x = x + lax.ppermute(x, AXES, [(i, i ^ bit) for i in range(devices)])
    return x


def body(blocks, connect, owner_map, right_side):
    devices = lax.axis_size(AXES)
    own = right_side.shape[0]
    window = 2 * own
    up = [(i, (i + 1) % devices) for i in range(devices)]
    down = [(b, a) for a, b in up]

    def from_below(x):
        return lax.ppermute(x, AXES, up)

    def from_above(x):
        return lax.ppermute(x, AXES, down)

    base = jnp.stack([lax.axis_index(AXES) * own, own * devices]).astype(jnp.int32)
    width = right_side.shape[1] // 2
    r_low, r_high = {}, {}
    start = right_side[:, :width]
    r_low[0] = from_below(start)
    r_high[0] = from_above(start)
    send0, send1 = pack(owner_map, connect.T, blocks, devices)

    def exchange(send):
        got = lax.all_to_all(
            send.reshape(devices, ROWS, 128), AXES, split_axis=0, concat_axis=0, tiled=True
        )
        return got.reshape(devices * ROWS, 128)

    got0 = exchange(send0)
    got1 = exchange(send1)
    rest, got0 = lax.optimization_barrier((right_side, got0))
    rest = rest[:, width:]
    r_low[1], r_high[1] = from_below(rest), from_above(rest)
    part = assemble(base, got0, window)
    center, high_band, lower = assemble(base, got1, window, part)
    lower = from_below(lower)
    low_band = lower[:, :own]
    inv = invert(center, lower)
    inv_low, inv_high = from_below(inv), from_above(inv)
    near_low, near_high = mm(low_band, inv_low), mm(high_band, inv_high)

    v0 = right_side
    v1, w1, sums = in_blocks(
        first_kernel,
        (near_low, near_high, inv),
        (),
        (r_low[0], r_high[0]),
        (r_low[1], r_high[1]),
        (),
        ("whole", "whole", "sums"),
    )
    w1_low, w1_high = from_below(w1), from_above(w1)
    w0, sums = in_blocks(start_kernel, (inv,), (v0, v1), (), (), (sums,), ("whole", "sums"))
    v2, w2_0, w2_1, sums = in_blocks(
        second_kernel,
        (low_band, high_band, inv),
        (w1_low, w1_high, w1),
        (),
        (),
        (sums,),
        ("whole", "left", "right", "sums"),
    )
    near_0 = from_above(w2_0)
    near_1 = from_below(w2_1)
    near_0, near_1, later_0, later_1 = lax.optimization_barrier((near_0, near_1, w2_0, w2_1))
    far_0 = from_below(later_0)
    far_1 = from_above(later_1)
    bands = (low_band, high_band)
    t, sums = in_blocks(
        side_kernel, bands, (), (w2_0, near_0), (w2_1, near_1), (sums,), ("whole", "sums")
    )
    sums = butterfly(sums, devices, (64, 32, 8, 4, 16, 2, 1))
    return in_blocks(
        finish_kernel,
        bands,
        (v0, w0, v1, w1, v2, t),
        (w2_0, far_0),
        (w2_1, far_1),
        (sums,),
        ("whole", "whole"),
    )


def solution(mesh):
    both = P(AXES, None)
    return jax.shard_map(
        body,
        mesh=mesh,
        in_specs=(both, both, P(AXES), both),
        out_specs=(both, both),
        check_vma=False,
    )
```

```python
import jax
import jax.numpy as jnp
from jax import lax
from jax.experimental import pallas as pl
from jax.experimental.pallas import tpu as pltpu
from jax.sharding import PartitionSpec as P


AXES = ("row", "col")
NB = 96
HALF = 48
ROWS = 40
GROUP = 4
HI = lax.Precision.HIGHEST


def split2(x):
    high = x.astype(jnp.bfloat16)
    low = (x - high.astype(jnp.float32)).astype(jnp.bfloat16)
    return high, low


def pack_kernel(owner_ref, ids_ref, x_ref, out0_ref, out1_ref, tail_ref):
    subs = x_ref.shape[0]
    devs = out0_ref.shape[0] // ROWS
    sub = lax.broadcasted_iota(jnp.int32, (devs, subs), 0)
    here = sub == owner_ref[...]
    before = lax.broadcasted_iota(jnp.int32, (subs, subs), 0) < lax.broadcasted_iota(
        jnp.int32, (subs, subs), 1
    )
    count = jnp.dot(
        here.astype(jnp.bfloat16), before.astype(jnp.bfloat16), preferred_element_type=jnp.float32
    )
    first = jnp.where(here & (count < 0.5), 1.0, 0.0).astype(jnp.bfloat16)
    second = jnp.where(here & (count > 0.5), 1.0, 0.0).astype(jnp.bfloat16)
    pick = jnp.concatenate([first, second], axis=0)
    ids = ids_ref[...].astype(jnp.float32).T + 1.0
    ids = jnp.concatenate([ids, jnp.zeros((subs, 128 - NB), jnp.float32)], axis=1)
    pick = jnp.concatenate([pick, pick], axis=1)
    lane = lax.broadcasted_iota(jnp.int32, (subs, 128), 1)

    def flat(start):
        tile, off = divmod(start, 128)
        if off == 0:
            return x_ref[:, tile * 128 : tile * 128 + 128]
        one = pltpu.roll(x_ref[:, tile * 128 : tile * 128 + 128], 128 - off, 1)
        if (tile + 1) * 128 >= x_ref.shape[1]:
            return one
        two = pltpu.roll(x_ref[:, tile * 128 + 128 : tile * 128 + 256], 128 - off, 1)
        return jnp.where(lane < 128 - off, one, two)

    diag = jnp.zeros((subs, 128), jnp.float32)

    def wrow(i, diag):
        top = flat(NB * i)
        bottom = flat(NB * (i + HALF) + HALF)
        row = jnp.where(lane < i, bottom, jnp.where(lane == i, 0.5 * top, top))
        return row, jnp.where(lane == i, 0.5 * bottom, diag)

    for m in range(8):
        row, diag = wrow(ROWS + m, diag)
        tail_ref[m] = row
    order = [i for i in range(0, ROWS, 2) if i not in (26, 28)] + [26, 28]
    kept = {}
    for i in (26, 27, 28, 29):
        kept[i], diag = wrow(i, diag)
    for i0 in order:
        tiles = []
        for i in (i0, i0 + 1):
            if i in kept:
                row = kept[i]
            else:
                row, diag = wrow(i, diag)
            if i < 24:
                extra = pltpu.roll(tail_ref[i % 8], 96 - 32 * (i // 8), 1)
            elif i < 27:
                extra = pltpu.roll(ids, 96 - 32 * (i - 24), 1)
            elif i < 29:
                extra = pltpu.roll(diag, 96 - 32 * (i - 27), 1)
            else:
                extra = jnp.zeros_like(row)
            tiles.append(jnp.where(lane < NB, row, extra))
        high, low = split2(jnp.concatenate(tiles, axis=1))
        out = jnp.dot(
            pick, jnp.concatenate([high, low], axis=0), preferred_element_type=jnp.float32
        )
        for k in range(2):
            part = out[:, 128 * k : 128 * k + 128]
            out0_ref[pl.ds(i0 + k, devs, stride=ROWS), :] = part[:devs]
            out1_ref[pl.ds(i0 + k, devs, stride=ROWS), :] = part[devs:]


def pack(owner_map, ids, blocks, devices):
    shape = jax.ShapeDtypeStruct((devices * ROWS, 128), jnp.float32)
    return pl.pallas_call(
        pack_kernel,
        out_shape=(shape, shape),
        scratch_shapes=[pltpu.VMEM((8, blocks.shape[0], 128), jnp.float32)],
        name="pack",
    )(owner_map.reshape(1, -1), ids, blocks)


def assemble_kernel(last, base_ref, got_ref, *refs):
    place_ref, spread_ref, vec_ref, list_ref, sem = refs[-5:]
    if last:
        prev_ref, s11_ref, s12_ref, low_ref, acc_ref = refs[:5]
    else:
        acc_ref = refs[0]
    window = acc_ref.shape[0]
    half = window // 2
    slots = got_ref.shape[0] // ROWS
    lane = lax.broadcasted_iota(jnp.int32, (slots, slots), 1)
    sub = lax.broadcasted_iota(jnp.int32, (slots, slots), 0)
    filled = got_ref[pl.ds(24, slots, stride=ROWS), :][:, NB : NB + 1] > 0.5
    filled = jnp.broadcast_to(jnp.where(filled, 1.0, 0.0), (slots, slots))
    rank = jnp.dot(
        jnp.where(lane < sub, 1.0, 0.0).astype(jnp.bfloat16),
        filled.astype(jnp.bfloat16),
        preferred_element_type=jnp.float32,
    )
    subf = sub.astype(jnp.float32)
    hit = (filled > 0.5) & (rank == lane.astype(jnp.float32))
    count = jnp.sum(filled, axis=0, keepdims=True)
    spare = jnp.max(jnp.where(filled > 0.5, 0.0, subf), axis=0, keepdims=True)
    chosen = jnp.sum(jnp.where(hit, subf, 0.0), axis=0, keepdims=True)
    chosen = jnp.where(lane[:1].astype(jnp.float32) < count, chosen, spare)
    first_row = lax.broadcasted_iota(jnp.int32, (8, slots), 0) == 0
    vec_ref[...] = jnp.where(first_row, chosen, count).astype(jnp.int32)
    copy = pltpu.make_async_copy(vec_ref, list_ref, sem)
    copy.start()
    acc_ref[...] = prev_ref[...] if last else jnp.zeros_like(acc_ref)
    place_ref[1] = jnp.zeros(place_ref.shape[1:], jnp.bfloat16)
    spread_ref[1] = jnp.zeros(spread_ref.shape[1:], jnp.bfloat16)
    copy.wait()

    lane = lax.broadcasted_iota(jnp.int32, (HALF, 128), 1)
    row = lax.broadcasted_iota(jnp.int32, (HALF, 128), 0)
    lane1 = lax.broadcasted_iota(jnp.int32, (1, 128), 1)
    lane8 = lax.broadcasted_iota(jnp.int32, (8, 128), 1)
    target = lax.broadcasted_iota(jnp.int32, (window, 128), 0).astype(jnp.float32)
    start = base_ref[0].astype(jnp.float32)
    total = base_ref[1].astype(jnp.float32)

    def local(ids):
        moved = ids - 1.0 - start
        return jnp.where(ids > 0.5, jnp.where(moved < 0.0, moved + total, moved), -1.0)


    def lanes(pieces):
        out = pieces[3]
        for k in (2, 1, 0):
            out = jnp.where(lane1 < 32 * (k + 1), pieces[k], out)
        return out

    def onehot(ids):
        return jnp.where(target == local(ids), 1.0, 0.0).astype(jnp.bfloat16)

    def generate(buf, first):
        pieces = []
        for k in range(GROUP):
            slot = list_ref[0, first + k]
            base = pl.multiple_of(slot * ROWS, 8)
            got = got_ref[pl.ds(base, ROWS), :]
            rows = [got[24 + m : 25 + m] for m in range(3)]
            pieces += rows
            ids = lanes([pltpu.roll(rows[m], 32 * (m + 1), 1) for m in range(3)] + [jnp.zeros_like(rows[0])])
            half_diag = jnp.where(
                lane1 < 80, pltpu.roll(got[27:28], 80, 1), pltpu.roll(got[28:29], 112, 1)
            )
            tail = jnp.where(
                lane8 < 32,
                pltpu.roll(got[0:8], 32, 1),
                jnp.where(lane8 < 64, pltpu.roll(got[8:16], 64, 1), pltpu.roll(got[16:24], 96, 1)),
            )
            full = jnp.concatenate([got, tail], axis=0)
            top = jnp.where(lane >= row, full, 0.0)
            bottom = jnp.where(
                lane == row + HALF,
                half_diag,
                jnp.where((lane >= HALF) & (lane < row + HALF), pltpu.roll(full, HALF, 1), 0.0),
            )
            high, low = split2(jnp.concatenate([top, bottom], axis=0))
            spread = lax.dot_general(
                jnp.concatenate([high, low], axis=0),
                onehot(ids),
                (((1,), (1,)), ((), ())),
                preferred_element_type=jnp.float32,
            ).astype(jnp.bfloat16)
            spread_ref[buf, NB * k : NB * k + NB, :] = spread[:NB]
            spread_ref[buf, NB * (GROUP + k) : NB * (GROUP + k) + NB, :] = spread[NB:]
        for t in range(3):
            moved = [
                pltpu.roll(pieces[4 * t + q], (32 * (q + 1)) % 128, 1) if q < 3 else pieces[4 * t + q]
                for q in range(4)
            ]
            place = onehot(lanes(moved))
            place_ref[buf, :, 128 * t : 128 * t + 128] = place
            place_ref[buf, :, 128 * (t + 3) : 128 * (t + 3) + 128] = place

    def absorb(buf):
        acc_ref[...] += jnp.dot(
            place_ref[buf], spread_ref[buf], preferred_element_type=jnp.float32
        )

    def step(g, carry):
        generate(0, g * 2 * GROUP)
        absorb(1)
        generate(1, g * 2 * GROUP + GROUP)
        absorb(0)
        return carry

    lax.fori_loop(0, (list_ref[1, 0] + 2 * GROUP - 1) // (2 * GROUP), step, 0)
    absorb(1)
    if not last:
        return
    a11, a22 = acc_ref[:half, :half], acc_ref[half:, half:]
    s11_ref[...] = a11 + a11.T
    s12 = acc_ref[:half, half:] + acc_ref[half:, :half].T
    s12_ref[...] = s12
    low_ref[:, :half] = s12.T
    low_ref[:, half:] = a22 + a22.T


def assemble(base, got, window, prev=None):
    slots = got.shape[0] // ROWS
    half = window // 2
    last = prev is not None
    square = jax.ShapeDtypeStruct((half, half), jnp.float32)
    whole = jax.ShapeDtypeStruct((window, window), jnp.float32)
    scratch = [
        pltpu.VMEM((2, window, 2 * NB * GROUP), jnp.bfloat16),
        pltpu.VMEM((2, 2 * NB * GROUP, window), jnp.bfloat16),
        pltpu.VMEM((8, slots), jnp.int32),
        pltpu.SMEM((8, slots), jnp.int32),
        pltpu.SemaphoreType.DMA,
    ]
    if last:
        scratch = [pltpu.VMEM((window, window), jnp.float32)] + scratch
    out = (square, square, jax.ShapeDtypeStruct((half, window), jnp.float32)) if last else whole
    return pl.pallas_call(
        lambda *refs: assemble_kernel(last, *refs),
        out_shape=out,
        in_specs=[pl.BlockSpec(memory_space=pltpu.SMEM)]
        + [pl.BlockSpec(memory_space=pltpu.VMEM)] * (2 if last else 1),
        scratch_shapes=scratch,
        name="assemble_last" if last else "assemble_first",
    )(*((base, got, prev) if last else (base, got)))


def inverse_kernel(upper_ref, lower_ref, out_ref, mat_ref):
    size = upper_ref.shape[0]
    eye = jnp.where(
        lax.broadcasted_iota(jnp.int32, (size, size), 0)
        == lax.broadcasted_iota(jnp.int32, (size, size), 1),
        1.0,
        0.0,
    )
    mat = upper_ref[...] + lower_ref[:, size:] + eye
    mat_ref[...] = mat
    norm = jnp.max(jnp.sum(jnp.abs(mat), axis=0, keepdims=True))
    out_ref[...] = eye * (2.0 / (norm + 1.0))

    def cond(state):
        turn, gap = state
        return (turn < 48) & (gap > 1e-8)

    def turn(state):
        now = out_ref[...]
        miss = eye - jnp.dot(mat_ref[...], now, precision=HI, preferred_element_type=jnp.float32)
        out_ref[...] = now + jnp.dot(now, miss, precision=HI, preferred_element_type=jnp.float32)
        return state[0] + 1, jnp.sum(miss * miss)

    lax.while_loop(cond, turn, (0, jnp.float32(1.0)))


def invert(upper, lower):
    return pl.pallas_call(
        inverse_kernel,
        out_shape=jax.ShapeDtypeStruct(upper.shape, jnp.float32),
        scratch_shapes=[pltpu.VMEM(upper.shape, jnp.float32)],
        name="invert",
    )(upper, lower)


def mm(left, right):
    return jnp.dot(left, right, precision=HI, preferred_element_type=jnp.float32)


def left3(x):
    high, low = split2(x)
    return jnp.concatenate([high, high, low], axis=1)


def right3(x):
    high, low = split2(x)
    return jnp.concatenate([high, low, high], axis=0)


def dot3(left, right):
    return jnp.dot(left, right, preferred_element_type=jnp.float32)


def at_row(k, value):
    row = lax.broadcasted_iota(jnp.int32, (8, value.shape[1]), 0)
    return jnp.where(row == k, value, 0.0)


def sums_of(left, right):
    return jnp.sum(left * right, axis=0, keepdims=True)


BLOCK = 512


def in_blocks(kernel, matrices, wholes, lefts, rights, sums, outs, kept):
    rows = matrices[0].shape[0]
    total = wholes[0].shape[1] if wholes else 2 * lefts[0].shape[1]
    per = total // 2 // BLOCK
    maps = {
        "whole": lambda j: (0, j),
        "left": lambda j: (0, jnp.minimum(j, per - 1)),
        "right": lambda j: (0, jnp.maximum(j - per, 0)),
        "sums": lambda j: (0, j),
    }
    shapes = {
        "whole": (rows, total),
        "left": (rows, total // 2),
        "right": (rows, total // 2),
        "sums": (8, total),
    }

    def spec(kind, height):
        return pl.BlockSpec((height, BLOCK), maps[kind])

    ins = [("whole", x) for x in wholes] + [("left", x) for x in lefts]
    ins += [("right", x) for x in rights] + [("sums", x) for x in sums]

    def run(*refs):
        mats, mid, three = refs[: len(matrices)], refs[len(matrices) : -1], refs[-1]
        kernel(pl.program_id(0), per, mats, three, *mid)

    return pl.pallas_call(
        run,
        grid=(2 * per,),
        in_specs=[pl.BlockSpec(x.shape, lambda j: (0, 0)) for x in matrices]
        + [spec(kind, x.shape[0]) for kind, x in ins],
        out_specs=tuple(spec(kind, shapes[kind][0]) for kind in outs),
        out_shape=tuple(jax.ShapeDtypeStruct(shapes[kind], jnp.float32) for kind in outs),
        scratch_shapes=[pltpu.VMEM((kept, rows, 3 * rows), jnp.bfloat16)],
    )(*matrices, *(x for _, x in ins))


def keep(step, mats, three):
    @pl.when(step == 0)
    def _():
        for k, mat in enumerate(mats):
            three[k] = left3(mat[...])


def first_kernel(step, per, mats, three, low0, high0, low1, high1, v_ref, w_ref, m_ref):
    low, high, inv, inv_low, inv_high = mats

    @pl.when(step == 0)
    def _():
        three[0] = left3(mm(low[...], inv_low[...]))
        three[1] = left3(mm(high[...], inv_high[...]))
        three[2] = left3(inv[...])

    x_low = jnp.concatenate([low0[...], low1[...]], axis=0)
    x_high = jnp.concatenate([high0[...], high1[...]], axis=0)
    v = dot3(three[0], right3(x_low)) + dot3(three[1], right3(x_high))
    w = dot3(three[2], right3(v))
    v_ref[...] = v
    w_ref[...] = w
    m_ref[...] = at_row(2, sums_of(v, w))


def start_kernel(step, per, mats, three, v0, v1, m_in, w_ref, m_ref):
    keep(step, mats, three)
    w = dot3(three[0], right3(v0[...]))
    w_ref[...] = w
    m_ref[...] = m_in[...] + at_row(0, sums_of(v0[...], w)) + at_row(1, sums_of(v1[...], w))


def second_kernel(step, per, mats, three, x_low, x_high, w1, m_in, v_ref, left_ref, right_ref, m_ref):
    keep(step, mats, three)
    v = dot3(three[0], right3(x_low[...])) + dot3(three[1], right3(x_high[...]))
    w = dot3(three[2], right3(v))
    v_ref[...] = v
    m_ref[...] = m_in[...] + at_row(3, sums_of(v, w1[...])) + at_row(4, sums_of(v, w))

    @pl.when(step < per)
    def _():
        left_ref[...] = w

    @pl.when(step >= per)
    def _():
        right_ref[...] = w


def side_kernel(step, per, mats, three, w_left, x_high, w_right, x_low, m_in, t_ref, m_ref):
    keep(step, mats, three)
    left = step < per
    x = jnp.where(left, x_high[...], x_low[...])
    w = jnp.where(left, w_left[...], w_right[...])
    t = dot3(three[jnp.where(left, 1, 0)], right3(x))
    t_ref[...] = t
    m_ref[...] = m_in[...] + at_row(5, 2.0 * sums_of(t, w))


def safe(num, den):
    return jnp.where(den > 0, num / jnp.where(den > 0, den, 1.0), 0.0)


def coefficients(mu):
    m0, m1, m2, m3, m4, m5 = mu
    l1, l2 = safe(m1, m0), safe(m2, m0)
    d1 = m2 - l1 * m1
    e = m3 - l1 * m2
    l21 = safe(e, d1)
    d2 = m4 - l2 * m2 - l21 * e
    y0 = -m3
    y1 = -m4 - l1 * y0
    y2 = -m5 - l2 * y0 - l21 * y1
    b2 = safe(y2, d2)
    b1 = safe(y1, d1) - l21 * b2
    b0 = safe(y0, m0) - l1 * b1 - l2 * b2
    scale = 1.0 / (b0 - b1 + b2 - 1.0)
    c0, c1, c2, c3 = b0 * scale, b1 * scale, b2 * scale, scale
    return (1.0 - c0, c3 - c2, -c3), (c0, c1, c2, c3)


def finish_kernel(
    step, per, mats, three, v0, w0, v1, w1, v2, t, w_left, x_low, w_right, x_high, sums, sol, res
):
    keep(step, mats, three)
    left = step < per
    far = jnp.where(left, x_low[...], x_high[...])
    w2 = jnp.where(left, w_left[...], w_right[...])
    v3 = t[...] + dot3(three[jnp.where(left, 0, 1)], right3(far))
    x, c = coefficients([sums[k : k + 1, :] for k in range(6)])
    sol[...] = x[0] * w0[...] + x[1] * w1[...] + x[2] * w2
    res[...] = c[0] * v0[...] + c[1] * v1[...] + c[2] * v2[...] + c[3] * v3


def butterfly(x, devices, bits):
    for bit in bits:
        x = x + lax.ppermute(x, AXES, [(i, i ^ bit) for i in range(devices)])
    return x


def body(blocks, connect, owner_map, right_side):
    devices = lax.axis_size(AXES)
    own = right_side.shape[0]
    window = 2 * own
    up = [(i, (i + 1) % devices) for i in range(devices)]
    down = [(b, a) for a, b in up]

    def from_below(x):
        return lax.ppermute(x, AXES, up)

    def from_above(x):
        return lax.ppermute(x, AXES, down)

    base = jnp.stack([lax.axis_index(AXES) * own, own * devices]).astype(jnp.int32)
    r_low, r_high = {}, {}
    start = right_side[: own // 2]
    r_low[0] = from_below(start)
    r_high[0] = from_above(start)
    send0, send1 = pack(owner_map, connect.T, blocks, devices)

    def exchange(send):
        got = lax.all_to_all(
            send.reshape(devices, ROWS, 128), AXES, split_axis=0, concat_axis=0, tiled=True
        )
        return got.reshape(devices * ROWS, 128)

    got0 = exchange(send0)
    got1 = exchange(send1)
    rest, got0 = lax.optimization_barrier((right_side, got0))
    rest = rest[own // 2 :]
    r_low[1], r_high[1] = from_below(rest), from_above(rest)
    part = assemble(base, got0, window)
    center, high_band, lower = assemble(base, got1, window, part)
    lower = from_below(lower)
    low_band = lower[:, :own]
    inv = invert(center, lower)
    inv_low, inv_high = from_below(inv), from_above(inv)
    v0 = right_side
    v1, w1, sums = in_blocks(
        first_kernel,
        (low_band, high_band, inv, inv_low, inv_high),
        (r_low[0], r_high[0], r_low[1], r_high[1]),
        (),
        (),
        (),
        ("whole", "whole", "sums"),
        3,
    )
    w1_low, w1_high = from_below(w1), from_above(w1)
    w0, sums = in_blocks(start_kernel, (inv,), (v0, v1), (), (), (sums,), ("whole", "sums"), 1)
    v2, w2_0, w2_1, sums = in_blocks(
        second_kernel,
        (low_band, high_band, inv),
        (w1_low, w1_high, w1),
        (),
        (),
        (sums,),
        ("whole", "left", "right", "sums"),
        3,
    )
    near_0 = from_above(w2_0)
    near_1 = from_below(w2_1)
    near_0, near_1, later_0, later_1 = lax.optimization_barrier((near_0, near_1, w2_0, w2_1))
    far_0 = from_below(later_0)
    far_1 = from_above(later_1)
    bands = (low_band, high_band)
    t, sums = in_blocks(
        side_kernel, bands, (), (w2_0, near_0), (w2_1, near_1), (sums,), ("whole", "sums"), 2
    )
    sums = butterfly(sums, devices, (64, 32, 8, 4, 16, 2, 1))
    return in_blocks(
        finish_kernel,
        bands,
        (v0, w0, v1, w1, v2, t),
        (w2_0, far_0),
        (w2_1, far_1),
        (sums,),
        ("whole", "whole"),
        2,
    )


def solution(mesh):
    both = P(AXES, None)
    return jax.shard_map(
        body,
        mesh=mesh,
        in_specs=(both, both, P(AXES), both),
        out_specs=(both, both),
        check_vma=False,
    )
```

```python
import jax
import jax.numpy as jnp
from jax import lax
from jax.experimental import pallas as pl
from jax.experimental.pallas import tpu as pltpu
from jax.sharding import PartitionSpec as P


AXES = ("row", "col")
NB = 96
HALF = 48
ROWS = 40
GROUP = 4
HI = lax.Precision.HIGHEST


def split2(x):
    high = x.astype(jnp.bfloat16)
    low = (x - high.astype(jnp.float32)).astype(jnp.bfloat16)
    return high, low


def pack_kernel(owner_ref, ids_ref, blocks_ref, out0_ref, out1_ref, tail_ref, x_ref, sem):
    subs = x_ref.shape[0]
    devs = out0_ref.shape[0] // ROWS
    sub = lax.broadcasted_iota(jnp.int32, (devs, subs), 0)
    here = sub == owner_ref[...]
    before = lax.broadcasted_iota(jnp.int32, (subs, subs), 0) < lax.broadcasted_iota(
        jnp.int32, (subs, subs), 1
    )
    count = jnp.dot(
        here.astype(jnp.bfloat16), before.astype(jnp.bfloat16), preferred_element_type=jnp.float32
    )
    first = jnp.where(here & (count < 0.5), 1.0, 0.0).astype(jnp.bfloat16)
    second = jnp.where(here & (count > 0.5), 1.0, 0.0).astype(jnp.bfloat16)
    pick = jnp.concatenate([first, second], axis=0)
    ids = ids_ref[...].astype(jnp.float32).T + 1.0
    ids = jnp.concatenate([ids, jnp.zeros((subs, 128 - NB), jnp.float32)], axis=1)
    pick = jnp.concatenate([pick, pick], axis=1)
    lane = lax.broadcasted_iota(jnp.int32, (subs, 128), 1)

    part = 12 * NB
    upper = HALF * NB
    copies = []
    for q in range(8):
        begin = (3 - q // 2) * part + (q % 2) * upper
        there = pl.ds(begin, part)
        copies.append(pltpu.make_async_copy(blocks_ref.at[:, there], x_ref.at[:, there], sem.at[q]))
        copies[-1].start()
    waited = [0]

    def arrive(i):
        needed = 2 * (4 - i // 12)
        while waited[0] < needed:
            copies[waited[0]].wait()
            waited[0] += 1

    def flat(start, need):
        tile, off = divmod(start, 128)
        if off == 0:
            return x_ref[:, tile * 128 : tile * 128 + 128]
        one = pltpu.roll(x_ref[:, tile * 128 : tile * 128 + 128], 128 - off, 1)
        if off + need <= 128:
            return one
        two = pltpu.roll(x_ref[:, tile * 128 + 128 : tile * 128 + 256], 128 - off, 1)
        return jnp.where(lane < 128 - off, one, two)

    diag = jnp.zeros((subs, 128), jnp.float32)

    def wrow(i, diag):
        arrive(i)
        top = flat(NB * i, NB)
        bottom = flat(NB * (i + HALF) + HALF, HALF)
        row = jnp.where(lane < i, bottom, jnp.where(lane == i, 0.5 * top, top))
        return row, jnp.where(lane == i, 0.5 * bottom, diag)

    for m in range(8):
        row, diag = wrow(ROWS + m, diag)
        tail_ref[m] = row
    order = [i for i in range(ROWS - 2, -2, -2) if i not in (26, 28)] + [26, 28]
    kept = {}
    for i0 in order:
        tiles = []
        if i0 == 26:
            for i in (26, 27, 28, 29):
                kept[i], diag = wrow(i, diag)
        for i in (i0, i0 + 1):
            if i in kept:
                row = kept[i]
            else:
                row, diag = wrow(i, diag)
            if i < 24:
                extra = pltpu.roll(tail_ref[i % 8], 96 - 32 * (i // 8), 1)
            elif i < 27:
                extra = pltpu.roll(ids, 96 - 32 * (i - 24), 1)
            elif i < 29:
                extra = pltpu.roll(diag, 96 - 32 * (i - 27), 1)
            else:
                extra = jnp.zeros_like(row)
            tiles.append(jnp.where(lane < NB, row, extra))
        high, low = split2(jnp.concatenate(tiles, axis=1))
        out = jnp.dot(
            pick, jnp.concatenate([high, low], axis=0), preferred_element_type=jnp.float32
        )
        for k in range(2):
            part = out[:, 128 * k : 128 * k + 128]
            out0_ref[pl.ds(i0 + k, devs, stride=ROWS), :] = part[:devs]
            out1_ref[pl.ds(i0 + k, devs, stride=ROWS), :] = part[devs:]


def pack(owner_map, ids, blocks, devices):
    shape = jax.ShapeDtypeStruct((devices * ROWS, 128), jnp.float32)
    return pl.pallas_call(
        pack_kernel,
        out_shape=(shape, shape),
        in_specs=[
            pl.BlockSpec(memory_space=pltpu.VMEM),
            pl.BlockSpec(memory_space=pltpu.VMEM),
            pl.BlockSpec(memory_space=pl.ANY),
        ],
        scratch_shapes=[
            pltpu.VMEM((8, blocks.shape[0], 128), jnp.float32),
            pltpu.VMEM(blocks.shape, jnp.float32),
            pltpu.SemaphoreType.DMA((8,)),
        ],
        name="pack",
    )(owner_map.reshape(1, -1), ids, blocks)


def assemble_kernel(last, base_ref, got_ref, *refs):
    place_ref, spread_ref, vec_ref, list_ref, sem = refs[-5:]
    if last:
        prev_ref, s11_ref, s12_ref, low_ref, acc_ref = refs[:5]
    else:
        acc_ref = refs[0]
    window = acc_ref.shape[0]
    half = window // 2
    slots = got_ref.shape[0] // ROWS
    lane = lax.broadcasted_iota(jnp.int32, (slots, slots), 1)
    sub = lax.broadcasted_iota(jnp.int32, (slots, slots), 0)
    filled = got_ref[pl.ds(24, slots, stride=ROWS), :][:, NB : NB + 1] > 0.5
    filled = jnp.broadcast_to(jnp.where(filled, 1.0, 0.0), (slots, slots))
    rank = jnp.dot(
        jnp.where(lane < sub, 1.0, 0.0).astype(jnp.bfloat16),
        filled.astype(jnp.bfloat16),
        preferred_element_type=jnp.float32,
    )
    subf = sub.astype(jnp.float32)
    hit = (filled > 0.5) & (rank == lane.astype(jnp.float32))
    count = jnp.sum(filled, axis=0, keepdims=True)
    spare = jnp.max(jnp.where(filled > 0.5, 0.0, subf), axis=0, keepdims=True)
    chosen = jnp.sum(jnp.where(hit, subf, 0.0), axis=0, keepdims=True)
    chosen = jnp.where(lane[:1].astype(jnp.float32) < count, chosen, spare)
    first_row = lax.broadcasted_iota(jnp.int32, (8, slots), 0) == 0
    vec_ref[...] = jnp.where(first_row, chosen, count).astype(jnp.int32)
    copy = pltpu.make_async_copy(vec_ref, list_ref, sem)
    copy.start()
    acc_ref[...] = prev_ref[...] if last else jnp.zeros_like(acc_ref)
    place_ref[1] = jnp.zeros(place_ref.shape[1:], jnp.bfloat16)
    spread_ref[1] = jnp.zeros(spread_ref.shape[1:], jnp.bfloat16)
    copy.wait()

    lane = lax.broadcasted_iota(jnp.int32, (HALF, 128), 1)
    row = lax.broadcasted_iota(jnp.int32, (HALF, 128), 0)
    lane1 = lax.broadcasted_iota(jnp.int32, (1, 128), 1)
    lane8 = lax.broadcasted_iota(jnp.int32, (8, 128), 1)
    target = lax.broadcasted_iota(jnp.int32, (window, 128), 0).astype(jnp.float32)
    start = base_ref[0].astype(jnp.float32)
    total = base_ref[1].astype(jnp.float32)

    def local(ids):
        moved = ids - 1.0 - start
        return jnp.where(ids > 0.5, jnp.where(moved < 0.0, moved + total, moved), -1.0)


    def lanes(pieces):
        out = pieces[3]
        for k in (2, 1, 0):
            out = jnp.where(lane1 < 32 * (k + 1), pieces[k], out)
        return out

    def onehot(ids):
        return jnp.where(target == local(ids), 1.0, 0.0).astype(jnp.bfloat16)

    def generate(buf, first):
        pieces = []
        for k in range(GROUP):
            slot = list_ref[0, first + k]
            base = pl.multiple_of(slot * ROWS, 8)
            got = got_ref[pl.ds(base, ROWS), :]
            rows = [got[24 + m : 25 + m] for m in range(3)]
            pieces += rows
            ids = lanes([pltpu.roll(rows[m], 32 * (m + 1), 1) for m in range(3)] + [jnp.zeros_like(rows[0])])
            half_diag = jnp.where(
                lane1 < 80, pltpu.roll(got[27:28], 80, 1), pltpu.roll(got[28:29], 112, 1)
            )
            tail = jnp.where(
                lane8 < 32,
                pltpu.roll(got[0:8], 32, 1),
                jnp.where(lane8 < 64, pltpu.roll(got[8:16], 64, 1), pltpu.roll(got[16:24], 96, 1)),
            )
            full = jnp.concatenate([got, tail], axis=0)
            top = jnp.where(lane >= row, full, 0.0)
            bottom = jnp.where(
                lane == row + HALF,
                half_diag,
                jnp.where((lane >= HALF) & (lane < row + HALF), pltpu.roll(full, HALF, 1), 0.0),
            )
            high, low = split2(jnp.concatenate([top, bottom], axis=0))
            spread = lax.dot_general(
                jnp.concatenate([high, low], axis=0),
                onehot(ids),
                (((1,), (1,)), ((), ())),
                preferred_element_type=jnp.float32,
            ).astype(jnp.bfloat16)
            spread_ref[buf, NB * k : NB * k + NB, :] = spread[:NB]
            spread_ref[buf, NB * (GROUP + k) : NB * (GROUP + k) + NB, :] = spread[NB:]
        for t in range(3):
            moved = [
                pltpu.roll(pieces[4 * t + q], (32 * (q + 1)) % 128, 1) if q < 3 else pieces[4 * t + q]
                for q in range(4)
            ]
            place = onehot(lanes(moved))
            place_ref[buf, :, 128 * t : 128 * t + 128] = place
            place_ref[buf, :, 128 * (t + 3) : 128 * (t + 3) + 128] = place

    def absorb(buf):
        acc_ref[...] += jnp.dot(
            place_ref[buf], spread_ref[buf], preferred_element_type=jnp.float32
        )

    def step(g, carry):
        generate(0, g * 2 * GROUP)
        absorb(1)
        generate(1, g * 2 * GROUP + GROUP)
        absorb(0)
        return carry

    lax.fori_loop(0, (list_ref[1, 0] + 2 * GROUP - 1) // (2 * GROUP), step, 0)
    absorb(1)
    if not last:
        return
    a11, a22 = acc_ref[:half, :half], acc_ref[half:, half:]
    s11_ref[...] = a11 + a11.T
    s12 = acc_ref[:half, half:] + acc_ref[half:, :half].T
    s12_ref[...] = s12
    low_ref[:, :half] = s12.T
    low_ref[:, half:] = a22 + a22.T


def assemble(base, got, window, prev=None):
    slots = got.shape[0] // ROWS
    half = window // 2
    last = prev is not None
    square = jax.ShapeDtypeStruct((half, half), jnp.float32)
    whole = jax.ShapeDtypeStruct((window, window), jnp.float32)
    scratch = [
        pltpu.VMEM((2, window, 2 * NB * GROUP), jnp.bfloat16),
        pltpu.VMEM((2, 2 * NB * GROUP, window), jnp.bfloat16),
        pltpu.VMEM((8, slots), jnp.int32),
        pltpu.SMEM((8, slots), jnp.int32),
        pltpu.SemaphoreType.DMA,
    ]
    if last:
        scratch = [pltpu.VMEM((window, window), jnp.float32)] + scratch
    out = (square, square, jax.ShapeDtypeStruct((half, window), jnp.float32)) if last else whole
    return pl.pallas_call(
        lambda *refs: assemble_kernel(last, *refs),
        out_shape=out,
        in_specs=[pl.BlockSpec(memory_space=pltpu.SMEM)]
        + [pl.BlockSpec(memory_space=pltpu.VMEM)] * (2 if last else 1),
        scratch_shapes=scratch,
        name="assemble_last" if last else "assemble_first",
    )(*((base, got, prev) if last else (base, got)))


def inverse_kernel(upper_ref, lower_ref, out_ref, mat_ref):
    size = upper_ref.shape[0]
    eye = jnp.where(
        lax.broadcasted_iota(jnp.int32, (size, size), 0)
        == lax.broadcasted_iota(jnp.int32, (size, size), 1),
        1.0,
        0.0,
    )
    mat = upper_ref[...] + lower_ref[:, size:] + eye
    mat_ref[...] = mat
    norm = jnp.max(jnp.sum(jnp.abs(mat), axis=0, keepdims=True))
    out_ref[...] = eye * (2.0 / (norm + 1.0))

    def cond(state):
        turn, gap = state
        return (turn < 48) & (gap > 1e-8)

    def turn(state):
        now = out_ref[...]
        miss = eye - jnp.dot(mat_ref[...], now, precision=HI, preferred_element_type=jnp.float32)
        out_ref[...] = now + jnp.dot(now, miss, precision=HI, preferred_element_type=jnp.float32)
        return state[0] + 1, jnp.sum(miss * miss)

    lax.while_loop(cond, turn, (0, jnp.float32(1.0)))


def invert(upper, lower):
    return pl.pallas_call(
        inverse_kernel,
        out_shape=jax.ShapeDtypeStruct(upper.shape, jnp.float32),
        scratch_shapes=[pltpu.VMEM(upper.shape, jnp.float32)],
        name="invert",
    )(upper, lower)


def mm(left, right):
    return jnp.dot(left, right, precision=HI, preferred_element_type=jnp.float32)


def left3(x):
    high, low = split2(x)
    return jnp.concatenate([high, high, low], axis=1)


def right3(x):
    high, low = split2(x)
    return jnp.concatenate([high, low, high], axis=0)


def dot3(left, right):
    return jnp.dot(left, right, preferred_element_type=jnp.float32)


def at_row(k, value):
    row = lax.broadcasted_iota(jnp.int32, (4, value.shape[1]), 0)
    return jnp.where(row == k, value, 0.0)


def sums_of(left, right):
    return jnp.sum(left * right, axis=0, keepdims=True)


BLOCK = 512


def in_blocks(kernel, matrices, wholes, lefts, rights, sums, outs, kept):
    rows = matrices[0].shape[0]
    total = wholes[0].shape[1] if wholes else 2 * lefts[0].shape[1]
    per = total // 2 // BLOCK
    maps = {
        "whole": lambda j: (0, j),
        "left": lambda j: (0, jnp.minimum(j, per - 1)),
        "right": lambda j: (0, jnp.maximum(j - per, 0)),
        "sums": lambda j: (0, j),
    }
    shapes = {
        "whole": (rows, total),
        "left": (rows, total // 2),
        "right": (rows, total // 2),
        "sums": (4, total),
    }

    def spec(kind, height):
        return pl.BlockSpec((height, BLOCK), maps[kind])

    ins = [("whole", x) for x in wholes] + [("left", x) for x in lefts]
    ins += [("right", x) for x in rights] + [("sums", x) for x in sums]

    def run(*refs):
        mats, mid, three = refs[: len(matrices)], refs[len(matrices) : -1], refs[-1]
        kernel(pl.program_id(0), per, mats, three, *mid)

    return pl.pallas_call(
        run,
        grid=(2 * per,),
        in_specs=[pl.BlockSpec((rows, rows), lambda j: (0, 0)) for x in matrices]
        + [spec(kind, x.shape[0]) for kind, x in ins],
        out_specs=tuple(spec(kind, shapes[kind][0]) for kind in outs),
        out_shape=tuple(jax.ShapeDtypeStruct(shapes[kind], jnp.float32) for kind in outs),
        scratch_shapes=[pltpu.VMEM((kept, rows, 3 * rows), jnp.bfloat16)],
    )(*matrices, *(x for _, x in ins))


def keep(step, mats, three):
    @pl.when(step == 0)
    def _():
        for k, mat in enumerate(mats):
            three[k] = left3(mat[...])


def first_kernel(step, per, mats, three, low0, high0, low1, high1, v_ref, w_ref, m_ref):
    low, high, inv, inv_low, inv_high = mats

    @pl.when(step == 0)
    def _():
        three[0] = left3(mm(low[...], inv_low[...]))
        three[1] = left3(mm(high[...], inv_high[...]))
        three[2] = left3(inv[...])

    x_low = jnp.concatenate([low0[...], low1[...]], axis=0)
    x_high = jnp.concatenate([high0[...], high1[...]], axis=0)
    v = dot3(three[0], right3(x_low)) + dot3(three[1], right3(x_high))
    w = dot3(three[2], right3(v))
    v_ref[...] = v
    w_ref[...] = w
    m_ref[...] = at_row(2, sums_of(v, w))


def start_kernel(step, per, mats, three, v0, v1, m_in, w_ref, m_ref):
    keep(step, mats, three)
    w = dot3(three[0], right3(v0[...]))
    w_ref[...] = w
    m_ref[...] = m_in[...] + at_row(0, sums_of(v0[...], w)) + at_row(1, sums_of(v1[...], w))


def second_kernel(step, per, mats, three, x_low, x_high, w1, v_ref, left_ref, right_ref, m_ref):
    keep(step, mats, three)
    v = dot3(three[0], right3(x_low[...])) + dot3(three[1], right3(x_high[...]))
    w = dot3(three[2], right3(v))
    v_ref[...] = v
    m_ref[...] = at_row(0, sums_of(v, w1[...])) + at_row(1, sums_of(v, w))

    @pl.when(step < per)
    def _():
        left_ref[...] = w

    @pl.when(step >= per)
    def _():
        right_ref[...] = w


def side_kernel(step, per, mats, three, w_left, x_high, w_right, x_low, m_in, t_ref, m_ref):
    keep(step, mats, three)
    left = step < per
    x = jnp.where(left, x_high[...], x_low[...])
    w = jnp.where(left, w_left[...], w_right[...])
    t = dot3(three[jnp.where(left, 1, 0)], right3(x))
    t_ref[...] = t
    m_ref[...] = m_in[...] + at_row(2, 2.0 * sums_of(t, w))


def safe(num, den):
    return jnp.where(den > 0, num / jnp.where(den > 0, den, 1.0), 0.0)


def coefficients(mu):
    m0, m1, m2, m3, m4, m5 = mu
    l1, l2 = safe(m1, m0), safe(m2, m0)
    d1 = m2 - l1 * m1
    e = m3 - l1 * m2
    l21 = safe(e, d1)
    d2 = m4 - l2 * m2 - l21 * e
    y0 = -m3
    y1 = -m4 - l1 * y0
    y2 = -m5 - l2 * y0 - l21 * y1
    b2 = safe(y2, d2)
    b1 = safe(y1, d1) - l21 * b2
    b0 = safe(y0, m0) - l1 * b1 - l2 * b2
    scale = 1.0 / (b0 - b1 + b2 - 1.0)
    c0, c1, c2, c3 = b0 * scale, b1 * scale, b2 * scale, scale
    return (1.0 - c0, c3 - c2, -c3), (c0, c1, c2, c3)


def finish_kernel(
    step, per, mats, three, v0, w0, v1, w1, v2, t, w_left, x_low, w_right, x_high, early, late, sol, res
):
    keep(step, mats, three)
    left = step < per
    far = jnp.where(left, x_low[...], x_high[...])
    w2 = jnp.where(left, w_left[...], w_right[...])
    v3 = t[...] + dot3(three[jnp.where(left, 0, 1)], right3(far))
    x, c = coefficients([m[k : k + 1, :] for m in (early, late) for k in range(3)])
    sol[...] = x[0] * w0[...] + x[1] * w1[...] + x[2] * w2
    res[...] = c[0] * v0[...] + c[1] * v1[...] + c[2] * v2[...] + c[3] * v3


def butterfly(x, devices):
    for bit in (64, 32, 8, 4, 16, 2, 1):
        x = x + lax.ppermute(x, AXES, [(i, i ^ bit) for i in range(devices)])
    return x


def body(blocks, connect, owner_map, right_side):
    devices = lax.axis_size(AXES)
    own = right_side.shape[0]
    window = 2 * own
    up = [(i, (i + 1) % devices) for i in range(devices)]
    down = [(b, a) for a, b in up]

    def from_below(x):
        return lax.ppermute(x, AXES, up)

    def from_above(x):
        return lax.ppermute(x, AXES, down)

    base = jnp.stack([lax.axis_index(AXES) * own, own * devices]).astype(jnp.int32)
    r_low, r_high = {}, {}
    start = right_side[: own // 2]
    r_low[0] = from_below(start)
    r_high[0] = from_above(start)
    send0, send1 = pack(owner_map, connect.T, blocks, devices)

    def exchange(send):
        got = lax.all_to_all(
            send.reshape(devices, ROWS, 128), AXES, split_axis=0, concat_axis=0, tiled=True
        )
        return got.reshape(devices * ROWS, 128)

    got0 = exchange(send0)
    got1 = exchange(send1)
    rest, got0 = lax.optimization_barrier((right_side, got0))
    rest = rest[own // 2 :]
    r_low[1], r_high[1] = from_below(rest), from_above(rest)
    part = assemble(base, got0, window)
    center, high_band, lower = assemble(base, got1, window, part)
    lower = from_below(lower)
    inv = invert(center, lower)
    inv_low, inv_high = from_below(inv), from_above(inv)
    v0 = right_side
    v1, w1, sums = in_blocks(
        first_kernel,
        (lower, high_band, inv, inv_low, inv_high),
        (r_low[0], r_high[0], r_low[1], r_high[1]),
        (),
        (),
        (),
        ("whole", "whole", "sums"),
        3,
    )
    w1_low, w1_high = from_below(w1), from_above(w1)
    w0, early = in_blocks(start_kernel, (inv,), (v0, v1), (), (), (sums,), ("whole", "sums"), 1)
    early = butterfly(early, devices)
    v2, w2_0, w2_1, sums = in_blocks(
        second_kernel,
        (lower, high_band, inv),
        (w1_low, w1_high, w1),
        (),
        (),
        (),
        ("whole", "left", "right", "sums"),
        3,
    )
    near_0 = from_above(w2_0)
    near_1 = from_below(w2_1)
    near_0, near_1, later_0, later_1 = lax.optimization_barrier((near_0, near_1, w2_0, w2_1))
    far_0 = from_below(later_0)
    far_1 = from_above(later_1)
    bands = (lower, high_band)
    t, late = in_blocks(
        side_kernel, bands, (), (w2_0, near_0), (w2_1, near_1), (sums,), ("whole", "sums"), 2
    )
    late = butterfly(late, devices)
    return in_blocks(
        finish_kernel,
        bands,
        (v0, w0, v1, w1, v2, t),
        (w2_0, far_0),
        (w2_1, far_1),
        (early, late),
        ("whole", "whole"),
        2,
    )


def solution(mesh):
    both = P(AXES, None)
    return jax.shard_map(
        body,
        mesh=mesh,
        in_specs=(both, both, P(AXES), both),
        out_specs=(both, both),
        check_vma=False,
    )
```

```python
import jax
import jax.numpy as jnp
from jax import lax
from jax.experimental import pallas as pl
from jax.experimental.pallas import tpu as pltpu
from jax.sharding import PartitionSpec as P


AXES = ("row", "col")
NB = 96
HALF = 48
ROWS = 40
GROUP = 4
HI = lax.Precision.HIGHEST


def split2(x):
    high = x.astype(jnp.bfloat16)
    low = (x - high.astype(jnp.float32)).astype(jnp.bfloat16)
    return high, low


def pack_kernel(owner_ref, ids_ref, blocks_ref, out0_ref, out1_ref, tail_ref, x_ref, sem):
    subs = x_ref.shape[0]
    devs = out0_ref.shape[0] // ROWS
    sub = lax.broadcasted_iota(jnp.int32, (devs, subs), 0)
    here = sub == owner_ref[...]
    before = lax.broadcasted_iota(jnp.int32, (subs, subs), 0) < lax.broadcasted_iota(
        jnp.int32, (subs, subs), 1
    )
    count = jnp.dot(
        here.astype(jnp.bfloat16), before.astype(jnp.bfloat16), preferred_element_type=jnp.float32
    )
    first = jnp.where(here & (count < 0.5), 1.0, 0.0).astype(jnp.bfloat16)
    second = jnp.where(here & (count > 0.5), 1.0, 0.0).astype(jnp.bfloat16)
    pick = jnp.concatenate([first, second], axis=0)
    ids = ids_ref[...].astype(jnp.float32).T + 1.0
    ids = jnp.concatenate([ids, jnp.zeros((subs, 128 - NB), jnp.float32)], axis=1)
    pick = jnp.concatenate([pick, pick], axis=1)
    lane = lax.broadcasted_iota(jnp.int32, (subs, 128), 1)

    part = 12 * NB
    upper = HALF * NB
    copies = []
    for q in range(8):
        begin = (3 - q // 2) * part + (q % 2) * upper
        there = pl.ds(begin, part)
        copies.append(pltpu.make_async_copy(blocks_ref.at[:, there], x_ref.at[:, there], sem.at[q]))
        copies[-1].start()
    waited = [0]

    def arrive(i):
        needed = 2 * (4 - i // 12)
        while waited[0] < needed:
            copies[waited[0]].wait()
            waited[0] += 1

    def flat(start, need):
        tile, off = divmod(start, 128)
        if off == 0:
            return x_ref[:, tile * 128 : tile * 128 + 128]
        one = pltpu.roll(x_ref[:, tile * 128 : tile * 128 + 128], 128 - off, 1)
        if off + need <= 128:
            return one
        two = pltpu.roll(x_ref[:, tile * 128 + 128 : tile * 128 + 256], 128 - off, 1)
        return jnp.where(lane < 128 - off, one, two)

    diag = jnp.zeros((subs, 128), jnp.float32)

    def wrow(i, diag):
        arrive(i)
        top = flat(NB * i, NB)
        bottom = flat(NB * (i + HALF) + HALF, HALF)
        row = jnp.where(lane < i, bottom, jnp.where(lane == i, 0.5 * top, top))
        return row, jnp.where(lane == i, 0.5 * bottom, diag)

    for m in range(8):
        row, diag = wrow(ROWS + m, diag)
        tail_ref[m] = row
    order = [i for i in range(ROWS - 2, -2, -2) if i not in (26, 28)] + [26, 28]
    kept = {}
    for i0 in order:
        tiles = []
        if i0 == 26:
            for i in (26, 27, 28, 29):
                kept[i], diag = wrow(i, diag)
        for i in (i0, i0 + 1):
            if i in kept:
                row = kept[i]
            else:
                row, diag = wrow(i, diag)
            if i < 24:
                extra = pltpu.roll(tail_ref[i % 8], 96 - 32 * (i // 8), 1)
            elif i < 27:
                extra = pltpu.roll(ids, 96 - 32 * (i - 24), 1)
            elif i < 29:
                extra = pltpu.roll(diag, 96 - 32 * (i - 27), 1)
            else:
                extra = jnp.zeros_like(row)
            tiles.append(jnp.where(lane < NB, row, extra))
        high, low = split2(jnp.concatenate(tiles, axis=1))
        out = jnp.dot(
            pick, jnp.concatenate([high, low], axis=0), preferred_element_type=jnp.float32
        )
        for k in range(2):
            part = out[:, 128 * k : 128 * k + 128]
            out0_ref[pl.ds(i0 + k, devs, stride=ROWS), :] = part[:devs]
            out1_ref[pl.ds(i0 + k, devs, stride=ROWS), :] = part[devs:]


def pack(owner_map, ids, blocks, devices):
    shape = jax.ShapeDtypeStruct((devices * ROWS, 128), jnp.float32)
    return pl.pallas_call(
        pack_kernel,
        out_shape=(shape, shape),
        in_specs=[
            pl.BlockSpec(memory_space=pltpu.VMEM),
            pl.BlockSpec(memory_space=pltpu.VMEM),
            pl.BlockSpec(memory_space=pl.ANY),
        ],
        scratch_shapes=[
            pltpu.VMEM((8, blocks.shape[0], 128), jnp.float32),
            pltpu.VMEM(blocks.shape, jnp.float32),
            pltpu.SemaphoreType.DMA((8,)),
        ],
        name="pack",
    )(owner_map.reshape(1, -1), ids, blocks)


def assemble_kernel(last, base_ref, got_ref, *refs):
    place_ref, spread_ref, vec_ref, list_ref, sem = refs[-5:]
    if last:
        prev_ref, s11_ref, s12_ref, low_ref, acc_ref = refs[:5]
    else:
        acc_ref = refs[0]
    window = acc_ref.shape[0]
    half = window // 2
    slots = got_ref.shape[0] // ROWS
    lane = lax.broadcasted_iota(jnp.int32, (slots, slots), 1)
    sub = lax.broadcasted_iota(jnp.int32, (slots, slots), 0)
    filled = got_ref[pl.ds(24, slots, stride=ROWS), :][:, NB : NB + 1] > 0.5
    filled = jnp.broadcast_to(jnp.where(filled, 1.0, 0.0), (slots, slots))
    rank = jnp.dot(
        jnp.where(lane < sub, 1.0, 0.0).astype(jnp.bfloat16),
        filled.astype(jnp.bfloat16),
        preferred_element_type=jnp.float32,
    )
    subf = sub.astype(jnp.float32)
    hit = (filled > 0.5) & (rank == lane.astype(jnp.float32))
    count = jnp.sum(filled, axis=0, keepdims=True)
    spare = jnp.max(jnp.where(filled > 0.5, 0.0, subf), axis=0, keepdims=True)
    chosen = jnp.sum(jnp.where(hit, subf, 0.0), axis=0, keepdims=True)
    chosen = jnp.where(lane[:1].astype(jnp.float32) < count, chosen, spare)
    first_row = lax.broadcasted_iota(jnp.int32, (8, slots), 0) == 0
    vec_ref[...] = jnp.where(first_row, chosen, count).astype(jnp.int32)
    copy = pltpu.make_async_copy(vec_ref, list_ref, sem)
    copy.start()
    acc_ref[...] = prev_ref[...] if last else jnp.zeros_like(acc_ref)
    place_ref[1] = jnp.zeros(place_ref.shape[1:], jnp.bfloat16)
    spread_ref[1] = jnp.zeros(spread_ref.shape[1:], jnp.bfloat16)
    copy.wait()

    lane = lax.broadcasted_iota(jnp.int32, (HALF, 128), 1)
    row = lax.broadcasted_iota(jnp.int32, (HALF, 128), 0)
    lane1 = lax.broadcasted_iota(jnp.int32, (1, 128), 1)
    lane8 = lax.broadcasted_iota(jnp.int32, (8, 128), 1)
    target = lax.broadcasted_iota(jnp.int32, (window, 128), 0).astype(jnp.float32)
    start = base_ref[0].astype(jnp.float32)
    total = base_ref[1].astype(jnp.float32)

    def local(ids):
        moved = ids - 1.0 - start
        return jnp.where(ids > 0.5, jnp.where(moved < 0.0, moved + total, moved), -1.0)


    def lanes(pieces):
        out = pieces[3]
        for k in (2, 1, 0):
            out = jnp.where(lane1 < 32 * (k + 1), pieces[k], out)
        return out

    def onehot(ids):
        return jnp.where(target == local(ids), 1.0, 0.0).astype(jnp.bfloat16)

    def generate(buf, first):
        pieces = []
        for k in range(GROUP):
            slot = list_ref[0, first + k]
            base = pl.multiple_of(slot * ROWS, 8)
            got = got_ref[pl.ds(base, ROWS), :]
            rows = [got[24 + m : 25 + m] for m in range(3)]
            pieces += rows
            ids = lanes([pltpu.roll(rows[m], 32 * (m + 1), 1) for m in range(3)] + [jnp.zeros_like(rows[0])])
            half_diag = jnp.where(
                lane1 < 80, pltpu.roll(got[27:28], 80, 1), pltpu.roll(got[28:29], 112, 1)
            )
            tail = jnp.where(
                lane8 < 32,
                pltpu.roll(got[0:8], 32, 1),
                jnp.where(lane8 < 64, pltpu.roll(got[8:16], 64, 1), pltpu.roll(got[16:24], 96, 1)),
            )
            full = jnp.concatenate([got, tail], axis=0)
            top = jnp.where(lane >= row, full, 0.0)
            bottom = jnp.where(
                lane == row + HALF,
                half_diag,
                jnp.where((lane >= HALF) & (lane < row + HALF), pltpu.roll(full, HALF, 1), 0.0),
            )
            high, low = split2(jnp.concatenate([top, bottom], axis=0))
            spread = lax.dot_general(
                jnp.concatenate([high, low], axis=0),
                onehot(ids),
                (((1,), (1,)), ((), ())),
                preferred_element_type=jnp.float32,
            ).astype(jnp.bfloat16)
            spread_ref[buf, NB * k : NB * k + NB, :] = spread[:NB]
            spread_ref[buf, NB * (GROUP + k) : NB * (GROUP + k) + NB, :] = spread[NB:]
        for t in range(3):
            moved = [
                pltpu.roll(pieces[4 * t + q], (32 * (q + 1)) % 128, 1) if q < 3 else pieces[4 * t + q]
                for q in range(4)
            ]
            place = onehot(lanes(moved))
            place_ref[buf, :, 128 * t : 128 * t + 128] = place
            place_ref[buf, :, 128 * (t + 3) : 128 * (t + 3) + 128] = place

    def absorb(buf):
        acc_ref[...] += jnp.dot(
            place_ref[buf], spread_ref[buf], preferred_element_type=jnp.float32
        )

    def step(g, carry):
        generate(0, g * 2 * GROUP)
        absorb(1)
        generate(1, g * 2 * GROUP + GROUP)
        absorb(0)
        return carry

    lax.fori_loop(0, (list_ref[1, 0] + 2 * GROUP - 1) // (2 * GROUP), step, 0)
    absorb(1)
    if not last:
        return
    a11, a22 = acc_ref[:half, :half], acc_ref[half:, half:]
    s11_ref[...] = a11 + a11.T
    s12 = acc_ref[:half, half:] + acc_ref[half:, :half].T
    s12_ref[...] = s12
    low_ref[:, :half] = s12.T
    low_ref[:, half:] = a22 + a22.T


def assemble(base, got, window, prev=None):
    slots = got.shape[0] // ROWS
    half = window // 2
    last = prev is not None
    square = jax.ShapeDtypeStruct((half, half), jnp.float32)
    whole = jax.ShapeDtypeStruct((window, window), jnp.float32)
    scratch = [
        pltpu.VMEM((2, window, 2 * NB * GROUP), jnp.bfloat16),
        pltpu.VMEM((2, 2 * NB * GROUP, window), jnp.bfloat16),
        pltpu.VMEM((8, slots), jnp.int32),
        pltpu.SMEM((8, slots), jnp.int32),
        pltpu.SemaphoreType.DMA,
    ]
    if last:
        scratch = [pltpu.VMEM((window, window), jnp.float32)] + scratch
    out = (square, square, jax.ShapeDtypeStruct((half, window), jnp.float32)) if last else whole
    return pl.pallas_call(
        lambda *refs: assemble_kernel(last, *refs),
        out_shape=out,
        in_specs=[pl.BlockSpec(memory_space=pltpu.SMEM)]
        + [pl.BlockSpec(memory_space=pltpu.VMEM)] * (2 if last else 1),
        scratch_shapes=scratch,
        name="assemble_last" if last else "assemble_first",
    )(*((base, got, prev) if last else (base, got)))


def inverse_kernel(upper_ref, lower_ref, out_ref, mat_ref):
    size = upper_ref.shape[0]
    eye = jnp.where(
        lax.broadcasted_iota(jnp.int32, (size, size), 0)
        == lax.broadcasted_iota(jnp.int32, (size, size), 1),
        1.0,
        0.0,
    )
    mat = upper_ref[...] + lower_ref[:, size:] + eye
    mat_ref[...] = mat
    norm = jnp.max(jnp.sum(jnp.abs(mat), axis=0, keepdims=True))
    out_ref[...] = eye * (2.0 / (norm + 1.0))

    def cond(state):
        turn, gap = state
        return (turn < 48) & (gap > 1e-8)

    def turn(state):
        now = out_ref[...]
        miss = eye - jnp.dot(mat_ref[...], now, precision=HI, preferred_element_type=jnp.float32)
        out_ref[...] = now + jnp.dot(now, miss, precision=HI, preferred_element_type=jnp.float32)
        return state[0] + 1, jnp.sum(miss * miss)

    lax.while_loop(cond, turn, (0, jnp.float32(1.0)))


def invert(upper, lower):
    return pl.pallas_call(
        inverse_kernel,
        out_shape=jax.ShapeDtypeStruct(upper.shape, jnp.float32),
        scratch_shapes=[pltpu.VMEM(upper.shape, jnp.float32)],
        name="invert",
    )(upper, lower)


def mm(left, right):
    return jnp.dot(left, right, precision=HI, preferred_element_type=jnp.float32)


def left3(x):
    high, low = split2(x)
    return jnp.concatenate([high, high, low], axis=1)


def right3(x):
    high, low = split2(x)
    return jnp.concatenate([high, low, high], axis=0)


def dot3(left, right):
    return jnp.dot(left, right, preferred_element_type=jnp.float32)


def at_row(k, value):
    row = lax.broadcasted_iota(jnp.int32, (8, value.shape[1]), 0)
    return jnp.where(row == k, value, 0.0)


def sums_of(left, right):
    return jnp.sum(left * right, axis=0, keepdims=True)


BLOCK = 512


def in_blocks(kernel, matrices, wholes, lefts, rights, sums, outs, kept):
    rows = matrices[0].shape[0]
    total = wholes[0].shape[1] if wholes else 2 * lefts[0].shape[1]
    per = total // 2 // BLOCK
    maps = {
        "whole": lambda j: (0, j),
        "left": lambda j: (0, jnp.minimum(j, per - 1)),
        "right": lambda j: (0, jnp.maximum(j - per, 0)),
        "sums": lambda j: (0, j),
    }
    shapes = {
        "whole": (rows, total),
        "left": (rows, total // 2),
        "right": (rows, total // 2),
        "sums": (8, total),
    }

    def spec(kind, height):
        return pl.BlockSpec((height, BLOCK), maps[kind])

    ins = [("whole", x) for x in wholes] + [("left", x) for x in lefts]
    ins += [("right", x) for x in rights] + [("sums", x) for x in sums]

    def run(*refs):
        mats, mid, three = refs[: len(matrices)], refs[len(matrices) : -1], refs[-1]
        kernel(pl.program_id(0), per, mats, three, *mid)

    return pl.pallas_call(
        run,
        grid=(2 * per,),
        in_specs=[pl.BlockSpec((rows, rows), lambda j: (0, 0)) for x in matrices]
        + [spec(kind, x.shape[0]) for kind, x in ins],
        out_specs=tuple(spec(kind, shapes[kind][0]) for kind in outs),
        out_shape=tuple(jax.ShapeDtypeStruct(shapes[kind], jnp.float32) for kind in outs),
        scratch_shapes=[pltpu.VMEM((kept, rows, 3 * rows), jnp.bfloat16)],
    )(*matrices, *(x for _, x in ins))


def keep(step, mats, three):
    @pl.when(step == 0)
    def _():
        for k, mat in enumerate(mats):
            three[k] = left3(mat[...])


def first_kernel(step, per, mats, three, low0, high0, low1, high1, v_ref, w_ref, m_ref):
    low, high, inv, inv_low, inv_high = mats

    @pl.when(step == 0)
    def _():
        three[0] = left3(mm(low[...], inv_low[...]))
        three[1] = left3(mm(high[...], inv_high[...]))
        three[2] = left3(inv[...])

    x_low = jnp.concatenate([low0[...], low1[...]], axis=0)
    x_high = jnp.concatenate([high0[...], high1[...]], axis=0)
    v = dot3(three[0], right3(x_low)) + dot3(three[1], right3(x_high))
    w = dot3(three[2], right3(v))
    v_ref[...] = v
    w_ref[...] = w
    m_ref[...] = at_row(2, sums_of(v, w))


def start_kernel(step, per, mats, three, v0, v1, m_in, w_ref, m_ref):
    keep(step, mats, three)
    w = dot3(three[0], right3(v0[...]))
    w_ref[...] = w
    m_ref[...] = m_in[...] + at_row(0, sums_of(v0[...], w)) + at_row(1, sums_of(v1[...], w))


def second_kernel(
    step, per, mats, three, x_low, x_high, w1, m_in, v_ref, left_ref, right_ref, m_ref
):
    keep(step, mats, three)
    v = dot3(three[0], right3(x_low[...])) + dot3(three[1], right3(x_high[...]))
    w = dot3(three[2], right3(v))
    v_ref[...] = v
    m_ref[...] = m_in[...] + at_row(3, sums_of(v, w1[...])) + at_row(4, sums_of(v, w))

    @pl.when(step < per)
    def _():
        left_ref[...] = w

    @pl.when(step >= per)
    def _():
        right_ref[...] = w


def side_kernel(step, per, mats, three, w_left, x_high, w_right, x_low, m_in, t_ref, m_ref):
    keep(step, mats, three)
    left = step < per
    x = jnp.where(left, x_high[...], x_low[...])
    w = jnp.where(left, w_left[...], w_right[...])
    t = dot3(three[jnp.where(left, 1, 0)], right3(x))
    t_ref[...] = t
    m_ref[...] = m_in[...] + at_row(5, 2.0 * sums_of(t, w))


def safe(num, den):
    return jnp.where(den > 0, num / jnp.where(den > 0, den, 1.0), 0.0)


def coefficients(mu):
    m0, m1, m2, m3, m4, m5 = mu
    l1, l2 = safe(m1, m0), safe(m2, m0)
    d1 = m2 - l1 * m1
    e = m3 - l1 * m2
    l21 = safe(e, d1)
    d2 = m4 - l2 * m2 - l21 * e
    y0 = -m3
    y1 = -m4 - l1 * y0
    y2 = -m5 - l2 * y0 - l21 * y1
    b2 = safe(y2, d2)
    b1 = safe(y1, d1) - l21 * b2
    b0 = safe(y0, m0) - l1 * b1 - l2 * b2
    scale = 1.0 / (b0 - b1 + b2 - 1.0)
    c0, c1, c2, c3 = b0 * scale, b1 * scale, b2 * scale, scale
    return (1.0 - c0, c3 - c2, -c3), (c0, c1, c2, c3)


def finish_kernel(
    step, per, mats, three, v0, w0, v1, w1, v2, t, w_left, x_low, w_right, x_high, sums, sol, res
):
    keep(step, mats, three)
    left = step < per
    far = jnp.where(left, x_low[...], x_high[...])
    w2 = jnp.where(left, w_left[...], w_right[...])
    v3 = t[...] + dot3(three[jnp.where(left, 0, 1)], right3(far))
    x, c = coefficients([sums[k : k + 1, :] for k in range(6)])
    sol[...] = x[0] * w0[...] + x[1] * w1[...] + x[2] * w2
    res[...] = c[0] * v0[...] + c[1] * v1[...] + c[2] * v2[...] + c[3] * v3


def butterfly(x, devices):
    for bit in (16, 64, 32, 8, 4, 2, 1):
        x = x + lax.ppermute(x, AXES, [(i, i ^ bit) for i in range(devices)])
    return x


def body(blocks, connect, owner_map, right_side):
    devices = lax.axis_size(AXES)
    own = right_side.shape[0]
    window = 2 * own
    up = [(i, (i + 1) % devices) for i in range(devices)]
    down = [(b, a) for a, b in up]

    def from_below(x):
        return lax.ppermute(x, AXES, up)

    def from_above(x):
        return lax.ppermute(x, AXES, down)

    base = jnp.stack([lax.axis_index(AXES) * own, own * devices]).astype(jnp.int32)
    r_low, r_high = {}, {}
    start = right_side[: own // 2]
    r_low[0] = from_below(start)
    r_high[0] = from_above(start)
    send0, send1 = pack(owner_map, connect.T, blocks, devices)

    def exchange(send):
        got = lax.all_to_all(
            send.reshape(devices, ROWS, 128), AXES, split_axis=0, concat_axis=0, tiled=True
        )
        return got.reshape(devices * ROWS, 128)

    got0 = exchange(send0)
    got1 = exchange(send1)
    rest, got0 = lax.optimization_barrier((right_side, got0))
    rest = rest[own // 2 :]
    r_low[1], r_high[1] = from_below(rest), from_above(rest)
    part = assemble(base, got0, window)
    center, high_band, lower = assemble(base, got1, window, part)
    lower = from_below(lower)
    inv = invert(center, lower)
    inv_low, inv_high = from_below(inv), from_above(inv)
    v0 = right_side
    v1, w1, sums = in_blocks(
        first_kernel,
        (lower, high_band, inv, inv_low, inv_high),
        (r_low[0], r_high[0], r_low[1], r_high[1]),
        (),
        (),
        (),
        ("whole", "whole", "sums"),
        3,
    )
    w1_low, w1_high = from_below(w1), from_above(w1)
    w0, sums = in_blocks(start_kernel, (inv,), (v0, v1), (), (), (sums,), ("whole", "sums"), 1)
    v2, w2_0, w2_1, sums = in_blocks(
        second_kernel,
        (lower, high_band, inv),
        (w1_low, w1_high, w1),
        (),
        (),
        (sums,),
        ("whole", "left", "right", "sums"),
        3,
    )
    near_0 = from_above(w2_0)
    near_1 = from_below(w2_1)
    far_0 = from_below(w2_0)
    far_1 = from_above(w2_1)
    bands = (lower, high_band)
    t, sums = in_blocks(
        side_kernel, bands, (), (w2_0, near_0), (w2_1, near_1), (sums,), ("whole", "sums"), 2
    )
    sums = butterfly(sums, devices)
    return in_blocks(
        finish_kernel,
        bands,
        (v0, w0, v1, w1, v2, t),
        (w2_0, far_0),
        (w2_1, far_1),
        (sums,),
        ("whole", "whole"),
        2,
    )


def solution(mesh):
    both = P(AXES, None)
    return jax.shard_map(
        body,
        mesh=mesh,
        in_specs=(both, both, P(AXES), both),
        out_specs=(both, both),
        check_vma=False,
    )
```

```python
import jax
import jax.numpy as jnp
from jax import lax
from jax.experimental import pallas as pl
from jax.experimental.pallas import tpu as pltpu
from jax.sharding import PartitionSpec as P


AXES = ("row", "col")
NB = 96
HALF = 48
ROWS = 40
GROUP = 4
HI = lax.Precision.HIGHEST


def vmem(mib):
    return pltpu.CompilerParams(vmem_limit_bytes=mib * 1024 * 1024)


def split2(x):
    high = x.astype(jnp.bfloat16)
    low = (x - high.astype(jnp.float32)).astype(jnp.bfloat16)
    return high, low


def pack_kernel(owner_ref, ids_ref, blocks_ref, out0_ref, out1_ref, tail_ref, x_ref, sem):
    subs = x_ref.shape[0]
    devs = out0_ref.shape[0] // ROWS
    sub = lax.broadcasted_iota(jnp.int32, (devs, subs), 0)
    here = sub == owner_ref[...]
    before = lax.broadcasted_iota(jnp.int32, (subs, subs), 0) < lax.broadcasted_iota(
        jnp.int32, (subs, subs), 1
    )
    count = jnp.dot(
        here.astype(jnp.bfloat16), before.astype(jnp.bfloat16), preferred_element_type=jnp.float32
    )
    first = jnp.where(here & (count < 0.5), 1.0, 0.0).astype(jnp.bfloat16)
    second = jnp.where(here & (count > 0.5), 1.0, 0.0).astype(jnp.bfloat16)
    pick = jnp.concatenate([first, second], axis=0)
    ids = ids_ref[...].astype(jnp.float32).T + 1.0
    ids = jnp.concatenate([ids, jnp.zeros((subs, 128 - NB), jnp.float32)], axis=1)
    pick = jnp.concatenate([pick, pick], axis=1)
    lane = lax.broadcasted_iota(jnp.int32, (subs, 128), 1)

    part = 12 * NB
    upper = HALF * NB
    copies = []
    for q in range(8):
        begin = (3 - q // 2) * part + (q % 2) * upper
        there = pl.ds(begin, part)
        copies.append(pltpu.make_async_copy(blocks_ref.at[:, there], x_ref.at[:, there], sem.at[q]))
        copies[-1].start()
    waited = [0]

    def arrive(i):
        needed = 2 * (4 - i // 12)
        while waited[0] < needed:
            copies[waited[0]].wait()
            waited[0] += 1

    def flat(start, need):
        tile, off = divmod(start, 128)
        if off == 0:
            return x_ref[:, tile * 128 : tile * 128 + 128]
        one = pltpu.roll(x_ref[:, tile * 128 : tile * 128 + 128], 128 - off, 1)
        if off + need <= 128:
            return one
        two = pltpu.roll(x_ref[:, tile * 128 + 128 : tile * 128 + 256], 128 - off, 1)
        return jnp.where(lane < 128 - off, one, two)

    diag = jnp.zeros((subs, 128), jnp.float32)

    def wrow(i, diag):
        arrive(i)
        top = flat(NB * i, NB)
        bottom = flat(NB * (i + HALF) + HALF, HALF)
        row = jnp.where(lane < i, bottom, jnp.where(lane == i, 0.5 * top, top))
        return row, jnp.where(lane == i, 0.5 * bottom, diag)

    for m in range(8):
        row, diag = wrow(ROWS + m, diag)
        tail_ref[m] = row
    order = [i for i in range(ROWS - 2, -2, -2) if i not in (26, 28)] + [26, 28]
    kept = {}
    for i0 in order:
        tiles = []
        if i0 == 26:
            for i in (26, 27, 28, 29):
                kept[i], diag = wrow(i, diag)
        for i in (i0, i0 + 1):
            if i in kept:
                row = kept[i]
            else:
                row, diag = wrow(i, diag)
            if i < 24:
                extra = pltpu.roll(tail_ref[i % 8], 96 - 32 * (i // 8), 1)
            elif i < 27:
                extra = pltpu.roll(ids, 96 - 32 * (i - 24), 1)
            elif i < 29:
                extra = pltpu.roll(diag, 96 - 32 * (i - 27), 1)
            else:
                extra = jnp.zeros_like(row)
            tiles.append(jnp.where(lane < NB, row, extra))
        high, low = split2(jnp.concatenate(tiles, axis=1))
        out = jnp.dot(
            pick, jnp.concatenate([high, low], axis=0), preferred_element_type=jnp.float32
        )
        for k in range(2):
            part = out[:, 128 * k : 128 * k + 128]
            out0_ref[pl.ds(i0 + k, devs, stride=ROWS), :] = part[:devs]
            out1_ref[pl.ds(i0 + k, devs, stride=ROWS), :] = part[devs:]


def pack(owner_map, ids, blocks, devices):
    shape = jax.ShapeDtypeStruct((devices * ROWS, 128), jnp.float32)
    return pl.pallas_call(
        pack_kernel,
        out_shape=(shape, shape),
        in_specs=[
            pl.BlockSpec(memory_space=pltpu.VMEM),
            pl.BlockSpec(memory_space=pltpu.VMEM),
            pl.BlockSpec(memory_space=pl.ANY),
        ],
        scratch_shapes=[
            pltpu.VMEM((8, blocks.shape[0], 128), jnp.float32),
            pltpu.VMEM(blocks.shape, jnp.float32),
            pltpu.SemaphoreType.DMA((8,)),
        ],
        compiler_params=vmem(24),
        name="pack",
    )(owner_map.reshape(1, -1), ids, blocks)


def assemble_kernel(last, base_ref, got_ref, *refs):
    place_ref, spread_ref, vec_ref, list_ref, sem = refs[-5:]
    if last:
        prev_ref, s11_ref, s12_ref, low_ref, acc_ref = refs[:5]
    else:
        acc_ref = refs[0]
    window = acc_ref.shape[0]
    half = window // 2
    slots = got_ref.shape[0] // ROWS
    lane = lax.broadcasted_iota(jnp.int32, (slots, slots), 1)
    sub = lax.broadcasted_iota(jnp.int32, (slots, slots), 0)
    filled = got_ref[pl.ds(24, slots, stride=ROWS), :][:, NB : NB + 1] > 0.5
    filled = jnp.broadcast_to(jnp.where(filled, 1.0, 0.0), (slots, slots))
    rank = jnp.dot(
        jnp.where(lane < sub, 1.0, 0.0).astype(jnp.bfloat16),
        filled.astype(jnp.bfloat16),
        preferred_element_type=jnp.float32,
    )
    subf = sub.astype(jnp.float32)
    hit = (filled > 0.5) & (rank == lane.astype(jnp.float32))
    count = jnp.sum(filled, axis=0, keepdims=True)
    spare = jnp.max(jnp.where(filled > 0.5, 0.0, subf), axis=0, keepdims=True)
    chosen = jnp.sum(jnp.where(hit, subf, 0.0), axis=0, keepdims=True)
    chosen = jnp.where(lane[:1].astype(jnp.float32) < count, chosen, spare)
    first_row = lax.broadcasted_iota(jnp.int32, (8, slots), 0) == 0
    vec_ref[...] = jnp.where(first_row, chosen, count).astype(jnp.int32)
    copy = pltpu.make_async_copy(vec_ref, list_ref, sem)
    copy.start()
    acc_ref[...] = prev_ref[...] if last else jnp.zeros_like(acc_ref)
    place_ref[1] = jnp.zeros(place_ref.shape[1:], jnp.bfloat16)
    spread_ref[1] = jnp.zeros(spread_ref.shape[1:], jnp.bfloat16)
    copy.wait()

    lane = lax.broadcasted_iota(jnp.int32, (HALF, 128), 1)
    row = lax.broadcasted_iota(jnp.int32, (HALF, 128), 0)
    lane1 = lax.broadcasted_iota(jnp.int32, (1, 128), 1)
    lane8 = lax.broadcasted_iota(jnp.int32, (8, 128), 1)
    target = lax.broadcasted_iota(jnp.int32, (window, 128), 0).astype(jnp.float32)
    start = base_ref[0].astype(jnp.float32)
    total = base_ref[1].astype(jnp.float32)

    def local(ids):
        moved = ids - 1.0 - start
        return jnp.where(ids > 0.5, jnp.where(moved < 0.0, moved + total, moved), -1.0)


    def lanes(pieces):
        out = pieces[3]
        for k in (2, 1, 0):
            out = jnp.where(lane1 < 32 * (k + 1), pieces[k], out)
        return out

    def onehot(ids):
        return jnp.where(target == local(ids), 1.0, 0.0).astype(jnp.bfloat16)

    def generate(buf, first):
        pieces = []
        for k in range(GROUP):
            slot = list_ref[0, first + k]
            base = pl.multiple_of(slot * ROWS, 8)
            got = got_ref[pl.ds(base, ROWS), :]
            rows = [got[24 + m : 25 + m] for m in range(3)]
            pieces += rows
            ids = lanes([pltpu.roll(rows[m], 32 * (m + 1), 1) for m in range(3)] + [jnp.zeros_like(rows[0])])
            half_diag = jnp.where(
                lane1 < 80, pltpu.roll(got[27:28], 80, 1), pltpu.roll(got[28:29], 112, 1)
            )
            tail = jnp.where(
                lane8 < 32,
                pltpu.roll(got[0:8], 32, 1),
                jnp.where(lane8 < 64, pltpu.roll(got[8:16], 64, 1), pltpu.roll(got[16:24], 96, 1)),
            )
            full = jnp.concatenate([got, tail], axis=0)
            top = jnp.where(lane >= row, full, 0.0)
            bottom = jnp.where(
                lane == row + HALF,
                half_diag,
                jnp.where((lane >= HALF) & (lane < row + HALF), pltpu.roll(full, HALF, 1), 0.0),
            )
            high, low = split2(jnp.concatenate([top, bottom], axis=0))
            spread = lax.dot_general(
                jnp.concatenate([high, low], axis=0),
                onehot(ids),
                (((1,), (1,)), ((), ())),
                preferred_element_type=jnp.float32,
            ).astype(jnp.bfloat16)
            spread_ref[buf, NB * k : NB * k + NB, :] = spread[:NB]
            spread_ref[buf, NB * (GROUP + k) : NB * (GROUP + k) + NB, :] = spread[NB:]
        for t in range(3):
            moved = [
                pltpu.roll(pieces[4 * t + q], (32 * (q + 1)) % 128, 1) if q < 3 else pieces[4 * t + q]
                for q in range(4)
            ]
            place = onehot(lanes(moved))
            place_ref[buf, :, 128 * t : 128 * t + 128] = place
            place_ref[buf, :, 128 * (t + 3) : 128 * (t + 3) + 128] = place

    def absorb(buf):
        acc_ref[...] += jnp.dot(
            place_ref[buf], spread_ref[buf], preferred_element_type=jnp.float32
        )

    def step(g, carry):
        generate(0, g * 2 * GROUP)
        absorb(1)
        generate(1, g * 2 * GROUP + GROUP)
        absorb(0)
        return carry

    lax.fori_loop(0, (list_ref[1, 0] + 2 * GROUP - 1) // (2 * GROUP), step, 0)
    absorb(1)
    if not last:
        return
    a11, a22 = acc_ref[:half, :half], acc_ref[half:, half:]
    s11_ref[...] = a11 + a11.T
    s12 = acc_ref[:half, half:] + acc_ref[half:, :half].T
    s12_ref[...] = s12
    low_ref[:, :half] = s12.T
    low_ref[:, half:] = a22 + a22.T


def assemble(base, got, window, prev=None):
    slots = got.shape[0] // ROWS
    half = window // 2
    last = prev is not None
    square = jax.ShapeDtypeStruct((half, half), jnp.float32)
    whole = jax.ShapeDtypeStruct((window, window), jnp.float32)
    scratch = [
        pltpu.VMEM((2, window, 2 * NB * GROUP), jnp.bfloat16),
        pltpu.VMEM((2, 2 * NB * GROUP, window), jnp.bfloat16),
        pltpu.VMEM((8, slots), jnp.int32),
        pltpu.SMEM((8, slots), jnp.int32),
        pltpu.SemaphoreType.DMA,
    ]
    if last:
        scratch = [pltpu.VMEM((window, window), jnp.float32)] + scratch
    out = (square, square, jax.ShapeDtypeStruct((half, window), jnp.float32)) if last else whole
    return pl.pallas_call(
        lambda *refs: assemble_kernel(last, *refs),
        out_shape=out,
        in_specs=[pl.BlockSpec(memory_space=pltpu.SMEM)]
        + [pl.BlockSpec(memory_space=pltpu.VMEM)] * (2 if last else 1),
        scratch_shapes=scratch,
        compiler_params=vmem(20),
        name="assemble_last" if last else "assemble_first",
    )(*((base, got, prev) if last else (base, got)))


def inverse_kernel(upper_ref, lower_ref, out_ref, mat_ref):
    size = upper_ref.shape[0]
    eye = jnp.where(
        lax.broadcasted_iota(jnp.int32, (size, size), 0)
        == lax.broadcasted_iota(jnp.int32, (size, size), 1),
        1.0,
        0.0,
    )
    mat = upper_ref[...] + lower_ref[:, size:] + eye
    mat_ref[...] = mat
    norm = jnp.max(jnp.sum(jnp.abs(mat), axis=0, keepdims=True))
    out_ref[...] = eye * (2.0 / (norm + 1.0))

    def cond(state):
        turn, gap = state
        return (turn < 48) & (gap > 1e-8)

    def turn(state):
        now = out_ref[...]
        miss = eye - jnp.dot(mat_ref[...], now, precision=HI, preferred_element_type=jnp.float32)
        out_ref[...] = now + jnp.dot(now, miss, precision=HI, preferred_element_type=jnp.float32)
        return state[0] + 1, jnp.sum(miss * miss)

    lax.while_loop(cond, turn, (0, jnp.float32(1.0)))


def invert(upper, lower):
    return pl.pallas_call(
        inverse_kernel,
        out_shape=jax.ShapeDtypeStruct(upper.shape, jnp.float32),
        scratch_shapes=[pltpu.VMEM(upper.shape, jnp.float32)],
        compiler_params=vmem(8),
        name="invert",
    )(upper, lower)


def mm(left, right):
    return jnp.dot(left, right, precision=HI, preferred_element_type=jnp.float32)


def left3(x):
    high, low = split2(x)
    return jnp.concatenate([high, high, low], axis=1)


def right3(x):
    high, low = split2(x)
    return jnp.concatenate([high, low, high], axis=0)


def dot3(left, right):
    return jnp.dot(left, right, preferred_element_type=jnp.float32)


def at_row(k, value):
    row = lax.broadcasted_iota(jnp.int32, (8, value.shape[1]), 0)
    return jnp.where(row == k, value, 0.0)


def sums_of(left, right):
    return jnp.sum(left * right, axis=0, keepdims=True)


BLOCK = 512


def in_blocks(kernel, matrices, wholes, lefts, rights, sums, outs, kept):
    rows = matrices[0].shape[0]
    total = wholes[0].shape[1] if wholes else 2 * lefts[0].shape[1]
    per = total // 2 // BLOCK
    maps = {
        "whole": lambda j: (0, j),
        "left": lambda j: (0, jnp.minimum(j, per - 1)),
        "right": lambda j: (0, jnp.maximum(j - per, 0)),
        "sums": lambda j: (0, j),
    }
    shapes = {
        "whole": (rows, total),
        "left": (rows, total // 2),
        "right": (rows, total // 2),
        "sums": (8, total),
    }

    def spec(kind, height):
        return pl.BlockSpec((height, BLOCK), maps[kind])

    ins = [("whole", x) for x in wholes] + [("left", x) for x in lefts]
    ins += [("right", x) for x in rights] + [("sums", x) for x in sums]

    def run(*refs):
        mats, mid, three = refs[: len(matrices)], refs[len(matrices) : -1], refs[-1]
        kernel(pl.program_id(0), per, mats, three, *mid)

    return pl.pallas_call(
        run,
        grid=(2 * per,),
        in_specs=[pl.BlockSpec((rows, rows), lambda j: (0, 0)) for x in matrices]
        + [spec(kind, x.shape[0]) for kind, x in ins],
        out_specs=tuple(spec(kind, shapes[kind][0]) for kind in outs),
        out_shape=tuple(jax.ShapeDtypeStruct(shapes[kind], jnp.float32) for kind in outs),
        scratch_shapes=[pltpu.VMEM((kept, rows, 3 * rows), jnp.bfloat16)],
        compiler_params=vmem(24),
    )(*matrices, *(x for _, x in ins))


def keep(step, mats, three):
    @pl.when(step == 0)
    def _():
        for k, mat in enumerate(mats):
            three[k] = left3(mat[...])


def first_kernel(step, per, mats, three, low0, high0, low1, high1, v_ref, w_ref, m_ref):
    low, high, inv, inv_low, inv_high = mats

    @pl.when(step == 0)
    def _():
        three[0] = left3(mm(low[...], inv_low[...]))
        three[1] = left3(mm(high[...], inv_high[...]))
        three[2] = left3(inv[...])

    x_low = jnp.concatenate([low0[...], low1[...]], axis=0)
    x_high = jnp.concatenate([high0[...], high1[...]], axis=0)
    v = dot3(three[0], right3(x_low)) + dot3(three[1], right3(x_high))
    w = dot3(three[2], right3(v))
    v_ref[...] = v
    w_ref[...] = w
    m_ref[...] = at_row(2, sums_of(v, w))


def start_kernel(step, per, mats, three, v0, v1, m_in, w_ref, m_ref):
    keep(step, mats, three)
    w = dot3(three[0], right3(v0[...]))
    w_ref[...] = w
    m_ref[...] = m_in[...] + at_row(0, sums_of(v0[...], w)) + at_row(1, sums_of(v1[...], w))


def second_kernel(
    step, per, mats, three, x_low, x_high, w1, m_in, v_ref, left_ref, right_ref, m_ref
):
    keep(step, mats, three)
    v = dot3(three[0], right3(x_low[...])) + dot3(three[1], right3(x_high[...]))
    w = dot3(three[2], right3(v))
    v_ref[...] = v
    m_ref[...] = m_in[...] + at_row(3, sums_of(v, w1[...])) + at_row(4, sums_of(v, w))

    @pl.when(step < per)
    def _():
        left_ref[...] = w

    @pl.when(step >= per)
    def _():
        right_ref[...] = w


def side_kernel(step, per, mats, three, w_left, x_high, w_right, x_low, m_in, t_ref, m_ref):
    keep(step, mats, three)
    left = step < per
    x = jnp.where(left, x_high[...], x_low[...])
    w = jnp.where(left, w_left[...], w_right[...])
    t = dot3(three[jnp.where(left, 1, 0)], right3(x))
    t_ref[...] = t
    m_ref[...] = m_in[...] + at_row(5, 2.0 * sums_of(t, w))


def safe(num, den):
    return jnp.where(den > 0, num / jnp.where(den > 0, den, 1.0), 0.0)


def coefficients(mu):
    m0, m1, m2, m3, m4, m5 = mu
    l1, l2 = safe(m1, m0), safe(m2, m0)
    d1 = m2 - l1 * m1
    e = m3 - l1 * m2
    l21 = safe(e, d1)
    d2 = m4 - l2 * m2 - l21 * e
    y0 = -m3
    y1 = -m4 - l1 * y0
    y2 = -m5 - l2 * y0 - l21 * y1
    b2 = safe(y2, d2)
    b1 = safe(y1, d1) - l21 * b2
    b0 = safe(y0, m0) - l1 * b1 - l2 * b2
    scale = 1.0 / (b0 - b1 + b2 - 1.0)
    c0, c1, c2, c3 = b0 * scale, b1 * scale, b2 * scale, scale
    return (1.0 - c0, c3 - c2, -c3), (c0, c1, c2, c3)


def finish_kernel(
    step, per, mats, three, v0, w0, v1, w1, v2, t, w_left, x_low, w_right, x_high, sums, sol, res
):
    keep(step, mats, three)
    left = step < per
    far = jnp.where(left, x_low[...], x_high[...])
    w2 = jnp.where(left, w_left[...], w_right[...])
    v3 = t[...] + dot3(three[jnp.where(left, 0, 1)], right3(far))
    x, c = coefficients([sums[k : k + 1, :] for k in range(6)])
    sol[...] = x[0] * w0[...] + x[1] * w1[...] + x[2] * w2
    res[...] = c[0] * v0[...] + c[1] * v1[...] + c[2] * v2[...] + c[3] * v3


def butterfly(x, devices):
    for bit in (16, 64, 32, 8, 4, 2, 1):
        x = x + lax.ppermute(x, AXES, [(i, i ^ bit) for i in range(devices)])
    return x


def body(blocks, connect, owner_map, right_side):
    devices = lax.axis_size(AXES)
    own = right_side.shape[0]
    window = 2 * own
    up = [(i, (i + 1) % devices) for i in range(devices)]
    down = [(b, a) for a, b in up]

    def from_below(x):
        return lax.ppermute(x, AXES, up)

    def from_above(x):
        return lax.ppermute(x, AXES, down)

    base = jnp.stack([lax.axis_index(AXES) * own, own * devices]).astype(jnp.int32)
    r_low, r_high = {}, {}
    start = right_side[: own // 2]
    r_low[0] = from_below(start)
    r_high[0] = from_above(start)
    send0, send1 = pack(owner_map, connect.T, blocks, devices)

    def exchange(send):
        got = lax.all_to_all(
            send.reshape(devices, ROWS, 128), AXES, split_axis=0, concat_axis=0, tiled=True
        )
        return got.reshape(devices * ROWS, 128)

    got0 = exchange(send0)
    got1 = exchange(send1)
    rest, got0 = lax.optimization_barrier((right_side, got0))
    rest = rest[own // 2 :]
    r_low[1], r_high[1] = from_below(rest), from_above(rest)
    part = assemble(base, got0, window)
    center, high_band, lower = assemble(base, got1, window, part)
    lower = from_below(lower)
    inv = invert(center, lower)
    inv_low, inv_high = from_below(inv), from_above(inv)
    v0 = right_side
    v1, w1, sums = in_blocks(
        first_kernel,
        (lower, high_band, inv, inv_low, inv_high),
        (r_low[0], r_high[0], r_low[1], r_high[1]),
        (),
        (),
        (),
        ("whole", "whole", "sums"),
        3,
    )
    w1_low, w1_high = from_below(w1), from_above(w1)
    w0, sums = in_blocks(start_kernel, (inv,), (v0, v1), (), (), (sums,), ("whole", "sums"), 1)
    v2, w2_0, w2_1, sums = in_blocks(
        second_kernel,
        (lower, high_band, inv),
        (w1_low, w1_high, w1),
        (),
        (),
        (sums,),
        ("whole", "left", "right", "sums"),
        3,
    )
    near_0 = from_above(w2_0)
    near_1 = from_below(w2_1)
    far_0 = from_below(w2_0)
    far_1 = from_above(w2_1)
    bands = (lower, high_band)
    t, sums = in_blocks(
        side_kernel, bands, (), (w2_0, near_0), (w2_1, near_1), (sums,), ("whole", "sums"), 2
    )
    sums = butterfly(sums, devices)
    return in_blocks(
        finish_kernel,
        bands,
        (v0, w0, v1, w1, v2, t),
        (w2_0, far_0),
        (w2_1, far_1),
        (sums,),
        ("whole", "whole"),
        2,
    )


def solution(mesh):
    both = P(AXES, None)
    return jax.shard_map(
        body,
        mesh=mesh,
        in_specs=(both, both, P(AXES), both),
        out_specs=(both, both),
        check_vma=False,
    )
```

```python
import jax
import jax.numpy as jnp
from jax import lax
from jax.experimental import pallas as pl
from jax.experimental.pallas import tpu as pltpu
from jax.sharding import PartitionSpec as P


AXES = ("row", "col")
NB = 96
HALF = 48
ROWS = 40
GROUP = 4
HI = lax.Precision.HIGHEST


def vmem(mib):
    return pltpu.CompilerParams(vmem_limit_bytes=mib * 1024 * 1024)


def split2(x):
    high = x.astype(jnp.bfloat16)
    low = (x - high.astype(jnp.float32)).astype(jnp.bfloat16)
    return high, low


def pack_kernel(owner_ref, ids_ref, blocks_ref, out0_ref, out1_ref, tail_ref, x_ref, sem):
    subs = x_ref.shape[0]
    devs = out0_ref.shape[0] // ROWS
    sub = lax.broadcasted_iota(jnp.int32, (devs, subs), 0)
    here = sub == owner_ref[...]
    before = lax.broadcasted_iota(jnp.int32, (subs, subs), 0) < lax.broadcasted_iota(
        jnp.int32, (subs, subs), 1
    )
    count = jnp.dot(
        here.astype(jnp.bfloat16), before.astype(jnp.bfloat16), preferred_element_type=jnp.float32
    )
    first = jnp.where(here & (count < 0.5), 1.0, 0.0).astype(jnp.bfloat16)
    second = jnp.where(here & (count > 0.5), 1.0, 0.0).astype(jnp.bfloat16)
    pick = jnp.concatenate([first, second], axis=0)
    ids = ids_ref[...].astype(jnp.float32).T + 1.0
    ids = jnp.concatenate([ids, jnp.zeros((subs, 128 - NB), jnp.float32)], axis=1)
    pick = jnp.concatenate([pick, pick], axis=1)
    lane = lax.broadcasted_iota(jnp.int32, (subs, 128), 1)

    part = 12 * NB
    upper = HALF * NB
    copies = []
    for q in range(8):
        begin = (3 - q // 2) * part + (q % 2) * upper
        there = pl.ds(begin, part)
        copies.append(pltpu.make_async_copy(blocks_ref.at[:, there], x_ref.at[:, there], sem.at[q]))
        copies[-1].start()
    waited = [0]

    def arrive(i):
        needed = 2 * (4 - i // 12)
        while waited[0] < needed:
            copies[waited[0]].wait()
            waited[0] += 1

    def flat(start, need):
        tile, off = divmod(start, 128)
        if off == 0:
            return x_ref[:, tile * 128 : tile * 128 + 128]
        one = pltpu.roll(x_ref[:, tile * 128 : tile * 128 + 128], 128 - off, 1)
        if off + need <= 128:
            return one
        two = pltpu.roll(x_ref[:, tile * 128 + 128 : tile * 128 + 256], 128 - off, 1)
        return jnp.where(lane < 128 - off, one, two)

    diag = jnp.zeros((subs, 128), jnp.float32)

    def wrow(i, diag):
        arrive(i)
        top = flat(NB * i, NB)
        bottom = flat(NB * (i + HALF) + HALF, HALF)
        row = jnp.where(lane < i, bottom, jnp.where(lane == i, 0.5 * top, top))
        return row, jnp.where(lane == i, 0.5 * bottom, diag)

    for m in range(8):
        row, diag = wrow(ROWS + m, diag)
        tail_ref[m] = row
    order = [i for i in range(ROWS - 2, -2, -2) if i not in (26, 28)] + [26, 28]
    kept = {}
    for i0 in order:
        tiles = []
        if i0 == 26:
            for i in (26, 27, 28, 29):
                kept[i], diag = wrow(i, diag)
        for i in (i0, i0 + 1):
            if i in kept:
                row = kept[i]
            else:
                row, diag = wrow(i, diag)
            if i < 24:
                extra = pltpu.roll(tail_ref[i % 8], 96 - 32 * (i // 8), 1)
            elif i < 27:
                extra = pltpu.roll(ids, 96 - 32 * (i - 24), 1)
            elif i < 29:
                extra = pltpu.roll(diag, 96 - 32 * (i - 27), 1)
            else:
                extra = jnp.zeros_like(row)
            tiles.append(jnp.where(lane < NB, row, extra))
        high, low = split2(jnp.concatenate(tiles, axis=1))
        out = jnp.dot(
            pick, jnp.concatenate([high, low], axis=0), preferred_element_type=jnp.float32
        )
        for k in range(2):
            part = out[:, 128 * k : 128 * k + 128]
            out0_ref[pl.ds(i0 + k, devs, stride=ROWS), :] = part[:devs]
            out1_ref[pl.ds(i0 + k, devs, stride=ROWS), :] = part[devs:]


def pack(owner_map, ids, blocks, devices):
    shape = jax.ShapeDtypeStruct((devices * ROWS, 128), jnp.float32)
    return pl.pallas_call(
        pack_kernel,
        out_shape=(shape, shape),
        in_specs=[
            pl.BlockSpec(memory_space=pltpu.VMEM),
            pl.BlockSpec(memory_space=pltpu.VMEM),
            pl.BlockSpec(memory_space=pltpu.HBM),
        ],
        scratch_shapes=[
            pltpu.VMEM((8, blocks.shape[0], 128), jnp.float32),
            pltpu.VMEM(blocks.shape, jnp.float32),
            pltpu.SemaphoreType.DMA((8,)),
        ],
        compiler_params=vmem(24),
        name="pack",
    )(owner_map.reshape(1, -1), ids, blocks)


def assemble_kernel(last, base_ref, got_ref, *refs):
    place_ref, spread_ref, vec_ref, list_ref, sem = refs[-5:]
    if last:
        prev_ref, s11_ref, s12_ref, low_ref, acc_ref = refs[:5]
    else:
        acc_ref = refs[0]
    window = acc_ref.shape[0]
    half = window // 2
    slots = got_ref.shape[0] // ROWS
    lane = lax.broadcasted_iota(jnp.int32, (slots, slots), 1)
    sub = lax.broadcasted_iota(jnp.int32, (slots, slots), 0)
    filled = got_ref[pl.ds(24, slots, stride=ROWS), :][:, NB : NB + 1] > 0.5
    filled = jnp.broadcast_to(jnp.where(filled, 1.0, 0.0), (slots, slots))
    rank = jnp.dot(
        jnp.where(lane < sub, 1.0, 0.0).astype(jnp.bfloat16),
        filled.astype(jnp.bfloat16),
        preferred_element_type=jnp.float32,
    )
    subf = sub.astype(jnp.float32)
    hit = (filled > 0.5) & (rank == lane.astype(jnp.float32))
    count = jnp.sum(filled, axis=0, keepdims=True)
    spare = jnp.max(jnp.where(filled > 0.5, 0.0, subf), axis=0, keepdims=True)
    chosen = jnp.sum(jnp.where(hit, subf, 0.0), axis=0, keepdims=True)
    chosen = jnp.where(lane[:1].astype(jnp.float32) < count, chosen, spare)
    first_row = lax.broadcasted_iota(jnp.int32, (8, slots), 0) == 0
    vec_ref[...] = jnp.where(first_row, chosen, count).astype(jnp.int32)
    copy = pltpu.make_async_copy(vec_ref, list_ref, sem)
    copy.start()
    acc_ref[...] = prev_ref[...] if last else jnp.zeros_like(acc_ref)
    place_ref[1] = jnp.zeros(place_ref.shape[1:], jnp.bfloat16)
    spread_ref[1] = jnp.zeros(spread_ref.shape[1:], jnp.bfloat16)
    copy.wait()

    lane = lax.broadcasted_iota(jnp.int32, (HALF, 128), 1)
    row = lax.broadcasted_iota(jnp.int32, (HALF, 128), 0)
    lane1 = lax.broadcasted_iota(jnp.int32, (1, 128), 1)
    lane8 = lax.broadcasted_iota(jnp.int32, (8, 128), 1)
    target = lax.broadcasted_iota(jnp.int32, (window, 128), 0).astype(jnp.float32)
    start = base_ref[0].astype(jnp.float32)
    total = base_ref[1].astype(jnp.float32)

    def local(ids):
        moved = ids - 1.0 - start
        return jnp.where(ids > 0.5, jnp.where(moved < 0.0, moved + total, moved), -1.0)


    def lanes(pieces):
        out = pieces[3]
        for k in (2, 1, 0):
            out = jnp.where(lane1 < 32 * (k + 1), pieces[k], out)
        return out

    def onehot(ids):
        return jnp.where(target == local(ids), 1.0, 0.0).astype(jnp.bfloat16)

    def generate(buf, first):
        pieces = []
        for k in range(GROUP):
            slot = list_ref[0, first + k]
            base = pl.multiple_of(slot * ROWS, 8)
            got = got_ref[pl.ds(base, ROWS), :]
            rows = [got[24 + m : 25 + m] for m in range(3)]
            pieces += rows
            ids = lanes([pltpu.roll(rows[m], 32 * (m + 1), 1) for m in range(3)] + [jnp.zeros_like(rows[0])])
            half_diag = jnp.where(
                lane1 < 80, pltpu.roll(got[27:28], 80, 1), pltpu.roll(got[28:29], 112, 1)
            )
            tail = jnp.where(
                lane8 < 32,
                pltpu.roll(got[0:8], 32, 1),
                jnp.where(lane8 < 64, pltpu.roll(got[8:16], 64, 1), pltpu.roll(got[16:24], 96, 1)),
            )
            full = jnp.concatenate([got, tail], axis=0)
            top = jnp.where(lane >= row, full, 0.0)
            bottom = jnp.where(
                lane == row + HALF,
                half_diag,
                jnp.where((lane >= HALF) & (lane < row + HALF), pltpu.roll(full, HALF, 1), 0.0),
            )
            high, low = split2(jnp.concatenate([top, bottom], axis=0))
            spread = lax.dot_general(
                jnp.concatenate([high, low], axis=0),
                onehot(ids),
                (((1,), (1,)), ((), ())),
                preferred_element_type=jnp.float32,
            ).astype(jnp.bfloat16)
            spread_ref[buf, NB * k : NB * k + NB, :] = spread[:NB]
            spread_ref[buf, NB * (GROUP + k) : NB * (GROUP + k) + NB, :] = spread[NB:]
        for t in range(3):
            moved = [
                pltpu.roll(pieces[4 * t + q], (32 * (q + 1)) % 128, 1) if q < 3 else pieces[4 * t + q]
                for q in range(4)
            ]
            place = onehot(lanes(moved))
            place_ref[buf, :, 128 * t : 128 * t + 128] = place
            place_ref[buf, :, 128 * (t + 3) : 128 * (t + 3) + 128] = place

    def absorb(buf):
        acc_ref[...] += jnp.dot(
            place_ref[buf], spread_ref[buf], preferred_element_type=jnp.float32
        )

    def step(g, carry):
        generate(0, g * 2 * GROUP)
        absorb(1)
        generate(1, g * 2 * GROUP + GROUP)
        absorb(0)
        return carry

    lax.fori_loop(0, (list_ref[1, 0] + 2 * GROUP - 1) // (2 * GROUP), step, 0)
    absorb(1)
    if not last:
        return
    a11, a22 = acc_ref[:half, :half], acc_ref[half:, half:]
    s11_ref[...] = a11 + a11.T
    s12 = acc_ref[:half, half:] + acc_ref[half:, :half].T
    s12_ref[...] = s12
    s22 = a22 + a22.T
    edge = half // 2
    row = lax.broadcasted_iota(jnp.int32, (edge, edge), 0)
    col = lax.broadcasted_iota(jnp.int32, (edge, edge), 1)
    last_part = s22[edge:, edge:]
    low_ref[:half, :half] = s12.T
    low_ref[:edge, half:] = s22[:edge, edge:]
    low_ref[edge:half, half:] = jnp.where(col >= row, s22[:edge, :edge], last_part)
    diag = jnp.sum(jnp.where(col == row, last_part, 0.0), axis=0, keepdims=True)
    low_ref[half:, :half] = jnp.zeros((8, half), jnp.float32)
    low_ref[half:, half:] = jnp.broadcast_to(diag, (8, edge))


def assemble(base, got, window, prev=None):
    slots = got.shape[0] // ROWS
    half = window // 2
    last = prev is not None
    square = jax.ShapeDtypeStruct((half, half), jnp.float32)
    whole = jax.ShapeDtypeStruct((window, window), jnp.float32)
    scratch = [
        pltpu.VMEM((2, window, 2 * NB * GROUP), jnp.bfloat16),
        pltpu.VMEM((2, 2 * NB * GROUP, window), jnp.bfloat16),
        pltpu.VMEM((8, slots), jnp.int32),
        pltpu.SMEM((8, slots), jnp.int32),
        pltpu.SemaphoreType.DMA,
    ]
    if last:
        scratch = [pltpu.VMEM((window, window), jnp.float32)] + scratch
    folded = jax.ShapeDtypeStruct((half + 8, half + half // 2), jnp.float32)
    out = (square, square, folded) if last else whole
    return pl.pallas_call(
        lambda *refs: assemble_kernel(last, *refs),
        out_shape=out,
        in_specs=[pl.BlockSpec(memory_space=pltpu.SMEM)]
        + [pl.BlockSpec(memory_space=pltpu.VMEM)] * (2 if last else 1),
        scratch_shapes=scratch,
        compiler_params=vmem(20),
        name="assemble_last" if last else "assemble_first",
    )(*((base, got, prev) if last else (base, got)))


def inverse_kernel(upper_ref, lower_ref, out_ref, mat_ref):
    size = upper_ref.shape[0]
    eye = jnp.where(
        lax.broadcasted_iota(jnp.int32, (size, size), 0)
        == lax.broadcasted_iota(jnp.int32, (size, size), 1),
        1.0,
        0.0,
    )
    edge = size // 2
    row = lax.broadcasted_iota(jnp.int32, (edge, edge), 0)
    col = lax.broadcasted_iota(jnp.int32, (edge, edge), 1)
    side = lower_ref[:edge, size:]
    both = lower_ref[edge:size, size:]
    above = jnp.where(col > row, both, 0.0)
    below = jnp.where(col < row, both, 0.0)
    first = jnp.where(col >= row, both, 0.0) + above.T
    second = below + below.T + jnp.where(col == row, lower_ref[size : size + 1, size:], 0.0)
    lower = jnp.concatenate(
        [
            jnp.concatenate([first, side], axis=1),
            jnp.concatenate([side.T, second], axis=1),
        ],
        axis=0,
    )
    mat = upper_ref[...] + lower + eye
    mat_ref[...] = mat
    norm = jnp.max(jnp.sum(jnp.abs(mat), axis=0, keepdims=True))
    out_ref[...] = eye * (2.0 / (norm + 1.0))

    def cond(state):
        turn, gap = state
        return (turn < 48) & (gap > 1e-8)

    def turn(state):
        now = out_ref[...]
        miss = eye - jnp.dot(mat_ref[...], now, precision=HI, preferred_element_type=jnp.float32)
        out_ref[...] = now + jnp.dot(now, miss, precision=HI, preferred_element_type=jnp.float32)
        return state[0] + 1, jnp.sum(miss * miss)

    lax.while_loop(cond, turn, (0, jnp.float32(1.0)))


def invert(upper, lower):
    return pl.pallas_call(
        inverse_kernel,
        out_shape=jax.ShapeDtypeStruct(upper.shape, jnp.float32),
        scratch_shapes=[pltpu.VMEM(upper.shape, jnp.float32)],
        compiler_params=vmem(8),
        name="invert",
    )(upper, lower)


def mm(left, right):
    return jnp.dot(left, right, precision=HI, preferred_element_type=jnp.float32)


def left3(x):
    high, low = split2(x)
    return jnp.concatenate([high, high, low], axis=1)


def right3(x):
    high, low = split2(x)
    return jnp.concatenate([high, low, high], axis=0)


def dot3(left, right):
    return jnp.dot(left, right, preferred_element_type=jnp.float32)


def at_row(k, value):
    row = lax.broadcasted_iota(jnp.int32, (8, value.shape[1]), 0)
    return jnp.where(row == k, value, 0.0)


def sums_of(left, right):
    return jnp.sum(left * right, axis=0, keepdims=True)


BLOCK = 512


def in_blocks(kernel, matrices, wholes, lefts, rights, sums, outs, kept):
    rows = matrices[-1].shape[0]
    total = wholes[0].shape[1] if wholes else 2 * lefts[0].shape[1]
    per = total // 2 // BLOCK
    maps = {
        "whole": lambda j: (0, j),
        "left": lambda j: (0, jnp.minimum(j, per - 1)),
        "right": lambda j: (0, jnp.maximum(j - per, 0)),
        "sums": lambda j: (0, j),
    }
    shapes = {
        "whole": (rows, total),
        "left": (rows, total // 2),
        "right": (rows, total // 2),
        "sums": (8, total),
    }

    def spec(kind, height):
        return pl.BlockSpec((height, BLOCK), maps[kind])

    ins = [("whole", x) for x in wholes] + [("left", x) for x in lefts]
    ins += [("right", x) for x in rights] + [("sums", x) for x in sums]

    def run(*refs):
        mats, mid, three = refs[: len(matrices)], refs[len(matrices) : -1], refs[-1]
        kernel(pl.program_id(0), per, mats, three, *mid)

    return pl.pallas_call(
        run,
        grid=(2 * per,),
        in_specs=[pl.BlockSpec((rows, rows), lambda j: (0, 0)) for x in matrices]
        + [spec(kind, x.shape[0]) for kind, x in ins],
        out_specs=tuple(spec(kind, shapes[kind][0]) for kind in outs),
        out_shape=tuple(jax.ShapeDtypeStruct(shapes[kind], jnp.float32) for kind in outs),
        scratch_shapes=[pltpu.VMEM((kept, rows, 3 * rows), jnp.bfloat16)],
        compiler_params=vmem(24),
    )(*matrices, *(x for _, x in ins))


def keep(step, mats, three):
    @pl.when(step == 0)
    def _():
        for k, mat in enumerate(mats):
            three[k] = left3(mat[...])


def first_kernel(step, per, mats, three, low0, high0, low1, high1, v_ref, w_ref, m_ref):
    low, high, inv, inv_low, inv_high = mats

    @pl.when(step == 0)
    def _():
        three[0] = left3(mm(low[...], inv_low[...]))
        three[1] = left3(mm(high[...], inv_high[...]))
        three[2] = left3(inv[...])

    x_low = jnp.concatenate([low0[...], low1[...]], axis=0)
    x_high = jnp.concatenate([high0[...], high1[...]], axis=0)
    v = dot3(three[0], right3(x_low)) + dot3(three[1], right3(x_high))
    w = dot3(three[2], right3(v))
    v_ref[...] = v
    w_ref[...] = w
    m_ref[...] = at_row(2, sums_of(v, w))


def start_kernel(step, per, mats, three, v0, v1, m_in, w_ref, m_ref):
    keep(step, mats, three)
    w = dot3(three[0], right3(v0[...]))
    w_ref[...] = w
    m_ref[...] = m_in[...] + at_row(0, sums_of(v0[...], w)) + at_row(1, sums_of(v1[...], w))


def second_kernel(
    step, per, mats, three, x_low, x_high, w1, m_in, v_ref, left_ref, right_ref, m_ref
):
    keep(step, mats, three)
    v = dot3(three[0], right3(x_low[...])) + dot3(three[1], right3(x_high[...]))
    w = dot3(three[2], right3(v))
    v_ref[...] = v
    m_ref[...] = m_in[...] + at_row(3, sums_of(v, w1[...])) + at_row(4, sums_of(v, w))

    @pl.when(step < per)
    def _():
        left_ref[...] = w

    @pl.when(step >= per)
    def _():
        right_ref[...] = w


def side_kernel(step, per, mats, three, w_left, x_high, w_right, x_low, m_in, t_ref, m_ref):
    keep(step, mats, three)
    left = step < per
    x = jnp.where(left, x_high[...], x_low[...])
    w = jnp.where(left, w_left[...], w_right[...])
    t = dot3(three[jnp.where(left, 1, 0)], right3(x))
    t_ref[...] = t
    m_ref[...] = m_in[...] + at_row(5, 2.0 * sums_of(t, w))


def safe(num, den):
    return jnp.where(den > 0, num / jnp.where(den > 0, den, 1.0), 0.0)


def coefficients(mu):
    m0, m1, m2, m3, m4, m5 = mu
    l1, l2 = safe(m1, m0), safe(m2, m0)
    d1 = m2 - l1 * m1
    e = m3 - l1 * m2
    l21 = safe(e, d1)
    d2 = m4 - l2 * m2 - l21 * e
    y0 = -m3
    y1 = -m4 - l1 * y0
    y2 = -m5 - l2 * y0 - l21 * y1
    b2 = safe(y2, d2)
    b1 = safe(y1, d1) - l21 * b2
    b0 = safe(y0, m0) - l1 * b1 - l2 * b2
    scale = 1.0 / (b0 - b1 + b2 - 1.0)
    c0, c1, c2, c3 = b0 * scale, b1 * scale, b2 * scale, scale
    return (1.0 - c0, c3 - c2, -c3), (c0, c1, c2, c3)


def finish_kernel(
    step, per, mats, three, v0, w0, v1, w1, v2, t, w_left, x_low, w_right, x_high, sums, sol, res
):
    keep(step, mats, three)
    left = step < per
    far = jnp.where(left, x_low[...], x_high[...])
    w2 = jnp.where(left, w_left[...], w_right[...])
    v3 = t[...] + dot3(three[jnp.where(left, 0, 1)], right3(far))
    x, c = coefficients([sums[k : k + 1, :] for k in range(6)])
    sol[...] = x[0] * w0[...] + x[1] * w1[...] + x[2] * w2
    res[...] = c[0] * v0[...] + c[1] * v1[...] + c[2] * v2[...] + c[3] * v3


def butterfly(x, devices):
    for bit in (16, 32, 96, 4, 12, 1, 3):
        x = x + lax.ppermute(x, AXES, [(i, i ^ bit) for i in range(devices)])
    return x


def body(blocks, connect, owner_map, right_side):
    devices = lax.axis_size(AXES)
    own = right_side.shape[0]
    window = 2 * own
    up = [(i, (i + 1) % devices) for i in range(devices)]
    down = [(b, a) for a, b in up]

    def from_below(x):
        return lax.ppermute(x, AXES, up)

    def from_above(x):
        return lax.ppermute(x, AXES, down)

    base = jnp.stack([lax.axis_index(AXES) * own, own * devices]).astype(jnp.int32)
    r_low, r_high = {}, {}
    start = right_side[: own // 2]
    r_low[0] = from_below(start)
    r_high[0] = from_above(start)
    send0, send1 = pack(owner_map, connect.T, blocks, devices)

    def exchange(send):
        got = lax.all_to_all(
            send.reshape(devices, ROWS, 128), AXES, split_axis=0, concat_axis=0, tiled=True
        )
        return got.reshape(devices * ROWS, 128)

    got0 = exchange(send0)
    got1 = exchange(send1)
    rest, got0 = lax.optimization_barrier((right_side, got0))
    rest = rest[own // 2 :]
    r_low[1], r_high[1] = from_below(rest), from_above(rest)
    part = assemble(base, got0, window)
    center, high_band, lower = assemble(base, got1, window, part)
    lower = from_below(lower)
    inv = invert(center, lower)
    inv_low, inv_high = from_below(inv), from_above(inv)
    v0 = right_side
    v1, w1, sums = in_blocks(
        first_kernel,
        (lower, high_band, inv, inv_low, inv_high),
        (r_low[0], r_high[0], r_low[1], r_high[1]),
        (),
        (),
        (),
        ("whole", "whole", "sums"),
        3,
    )
    w1_low, w1_high = from_below(w1), from_above(w1)
    w0, sums = in_blocks(start_kernel, (inv,), (v0, v1), (), (), (sums,), ("whole", "sums"), 1)
    v2, w2_0, w2_1, sums = in_blocks(
        second_kernel,
        (lower, high_band, inv),
        (w1_low, w1_high, w1),
        (),
        (),
        (sums,),
        ("whole", "left", "right", "sums"),
        3,
    )
    near_0 = from_above(w2_0)
    near_1 = from_below(w2_1)
    near_0, near_1, later_0, later_1 = lax.optimization_barrier((near_0, near_1, w2_0, w2_1))
    far_0 = from_below(later_0)
    far_1 = from_above(later_1)
    bands = (lower, high_band)
    t, sums = in_blocks(
        side_kernel, bands, (), (w2_0, near_0), (w2_1, near_1), (sums,), ("whole", "sums"), 2
    )
    sums = butterfly(sums, devices)
    return in_blocks(
        finish_kernel,
        bands,
        (v0, w0, v1, w1, v2, t),
        (w2_0, far_0),
        (w2_1, far_1),
        (sums,),
        ("whole", "whole"),
        2,
    )


def solution(mesh):
    both = P(AXES, None)
    return jax.shard_map(
        body,
        mesh=mesh,
        in_specs=(both, both, P(AXES), both),
        out_specs=(both, both),
        check_vma=False,
    )
```

```python
import jax
import jax.numpy as jnp
from jax import lax
from jax.experimental import pallas as pl
from jax.experimental.pallas import tpu as pltpu
from jax.sharding import PartitionSpec as P


AXES = ("row", "col")
NB = 96
HALF = 48
ROWS = 40
GROUP = 4
HI = lax.Precision.HIGHEST


def vmem(mib):
    return pltpu.CompilerParams(vmem_limit_bytes=mib * 1024 * 1024)


def split2(x):
    high = x.astype(jnp.bfloat16)
    low = (x - high.astype(jnp.float32)).astype(jnp.bfloat16)
    return high, low


def pack_kernel(owner_ref, ids_ref, blocks_ref, out0_ref, out1_ref, tail_ref, x_ref, sem):
    subs = x_ref.shape[0]
    devs = out0_ref.shape[0] // ROWS
    sub = lax.broadcasted_iota(jnp.int32, (devs, subs), 0)
    here = sub == owner_ref[...]
    before = lax.broadcasted_iota(jnp.int32, (subs, subs), 0) < lax.broadcasted_iota(
        jnp.int32, (subs, subs), 1
    )
    count = jnp.dot(
        here.astype(jnp.bfloat16), before.astype(jnp.bfloat16), preferred_element_type=jnp.float32
    )
    first = jnp.where(here & (count < 0.5), 1.0, 0.0).astype(jnp.bfloat16)
    second = jnp.where(here & (count > 0.5), 1.0, 0.0).astype(jnp.bfloat16)
    pick = jnp.concatenate([first, second], axis=0)
    ids = ids_ref[...].astype(jnp.float32).T + 1.0
    ids = jnp.concatenate([ids, jnp.zeros((subs, 128 - NB), jnp.float32)], axis=1)
    pick = jnp.concatenate([pick, pick], axis=1)
    lane = lax.broadcasted_iota(jnp.int32, (subs, 128), 1)

    part = 12 * NB
    upper = HALF * NB
    copies = []
    for q in range(8):
        begin = (3 - q // 2) * part + (q % 2) * upper
        there = pl.ds(begin, part)
        copies.append(pltpu.make_async_copy(blocks_ref.at[:, there], x_ref.at[:, there], sem.at[q]))
        copies[-1].start()
    waited = [0]

    def arrive(i):
        needed = 2 * (4 - i // 12)
        while waited[0] < needed:
            copies[waited[0]].wait()
            waited[0] += 1

    def flat(start, need):
        tile, off = divmod(start, 128)
        if off == 0:
            return x_ref[:, tile * 128 : tile * 128 + 128]
        one = pltpu.roll(x_ref[:, tile * 128 : tile * 128 + 128], 128 - off, 1)
        if off + need <= 128:
            return one
        two = pltpu.roll(x_ref[:, tile * 128 + 128 : tile * 128 + 256], 128 - off, 1)
        return jnp.where(lane < 128 - off, one, two)

    diag = jnp.zeros((subs, 128), jnp.float32)

    def wrow(i, diag):
        arrive(i)
        top = flat(NB * i, NB)
        bottom = flat(NB * (i + HALF) + HALF, HALF)
        row = jnp.where(lane < i, bottom, jnp.where(lane == i, 0.5 * top, top))
        return row, jnp.where(lane == i, 0.5 * bottom, diag)

    for m in range(8):
        row, diag = wrow(ROWS + m, diag)
        tail_ref[m] = row
    order = [i for i in range(ROWS - 2, -2, -2) if i not in (26, 28)] + [26, 28]
    kept = {}
    for i0 in order:
        tiles = []
        if i0 == 26:
            for i in (26, 27, 28, 29):
                kept[i], diag = wrow(i, diag)
        for i in (i0, i0 + 1):
            if i in kept:
                row = kept[i]
            else:
                row, diag = wrow(i, diag)
            if i < 24:
                extra = pltpu.roll(tail_ref[i % 8], 96 - 32 * (i // 8), 1)
            elif i < 27:
                extra = pltpu.roll(ids, 96 - 32 * (i - 24), 1)
            elif i < 29:
                extra = pltpu.roll(diag, 96 - 32 * (i - 27), 1)
            else:
                extra = jnp.zeros_like(row)
            tiles.append(jnp.where(lane < NB, row, extra))
        high, low = split2(jnp.concatenate(tiles, axis=1))
        out = jnp.dot(
            pick, jnp.concatenate([high, low], axis=0), preferred_element_type=jnp.float32
        )
        for k in range(2):
            part = out[:, 128 * k : 128 * k + 128]
            out0_ref[pl.ds(i0 + k, devs, stride=ROWS), :] = part[:devs]
            out1_ref[pl.ds(i0 + k, devs, stride=ROWS), :] = part[devs:]


def pack(owner_map, ids, blocks, devices):
    shape = jax.ShapeDtypeStruct((devices * ROWS, 128), jnp.float32)
    return pl.pallas_call(
        pack_kernel,
        out_shape=(shape, shape),
        in_specs=[
            pl.BlockSpec(memory_space=pltpu.VMEM),
            pl.BlockSpec(memory_space=pltpu.VMEM),
            pl.BlockSpec(memory_space=pl.ANY),
        ],
        scratch_shapes=[
            pltpu.VMEM((8, blocks.shape[0], 128), jnp.float32),
            pltpu.VMEM(blocks.shape, jnp.float32),
            pltpu.SemaphoreType.DMA((8,)),
        ],
        compiler_params=vmem(24),
        name="pack",
    )(owner_map.reshape(1, -1), ids, blocks)


def assemble_kernel(last, base_ref, got_ref, *refs):
    place_ref, spread_ref, vec_ref, list_ref, sem = refs[-5:]
    if last:
        prev_ref, s11_ref, s12_ref, low_ref, acc_ref = refs[:5]
    else:
        acc_ref = refs[0]
    window = acc_ref.shape[0]
    half = window // 2
    slots = got_ref.shape[0] // ROWS
    lane = lax.broadcasted_iota(jnp.int32, (slots, slots), 1)
    sub = lax.broadcasted_iota(jnp.int32, (slots, slots), 0)
    filled = got_ref[pl.ds(24, slots, stride=ROWS), :][:, NB : NB + 1] > 0.5
    filled = jnp.broadcast_to(jnp.where(filled, 1.0, 0.0), (slots, slots))
    rank = jnp.dot(
        jnp.where(lane < sub, 1.0, 0.0).astype(jnp.bfloat16),
        filled.astype(jnp.bfloat16),
        preferred_element_type=jnp.float32,
    )
    subf = sub.astype(jnp.float32)
    hit = (filled > 0.5) & (rank == lane.astype(jnp.float32))
    count = jnp.sum(filled, axis=0, keepdims=True)
    spare = jnp.max(jnp.where(filled > 0.5, 0.0, subf), axis=0, keepdims=True)
    chosen = jnp.sum(jnp.where(hit, subf, 0.0), axis=0, keepdims=True)
    chosen = jnp.where(lane[:1].astype(jnp.float32) < count, chosen, spare)
    first_row = lax.broadcasted_iota(jnp.int32, (8, slots), 0) == 0
    vec_ref[...] = jnp.where(first_row, chosen, count).astype(jnp.int32)
    copy = pltpu.make_async_copy(vec_ref, list_ref, sem)
    copy.start()
    acc_ref[...] = prev_ref[...] if last else jnp.zeros_like(acc_ref)
    place_ref[1] = jnp.zeros(place_ref.shape[1:], jnp.bfloat16)
    spread_ref[1] = jnp.zeros(spread_ref.shape[1:], jnp.bfloat16)
    copy.wait()

    lane = lax.broadcasted_iota(jnp.int32, (HALF, 128), 1)
    row = lax.broadcasted_iota(jnp.int32, (HALF, 128), 0)
    lane1 = lax.broadcasted_iota(jnp.int32, (1, 128), 1)
    lane8 = lax.broadcasted_iota(jnp.int32, (8, 128), 1)
    target = lax.broadcasted_iota(jnp.int32, (window, 128), 0).astype(jnp.float32)
    start = base_ref[0].astype(jnp.float32)
    total = base_ref[1].astype(jnp.float32)

    def local(ids):
        moved = ids - 1.0 - start
        return jnp.where(ids > 0.5, jnp.where(moved < 0.0, moved + total, moved), -1.0)


    def lanes(pieces):
        out = pieces[3]
        for k in (2, 1, 0):
            out = jnp.where(lane1 < 32 * (k + 1), pieces[k], out)
        return out

    def onehot(ids):
        return jnp.where(target == local(ids), 1.0, 0.0).astype(jnp.bfloat16)

    def generate(buf, first):
        pieces = []
        for k in range(GROUP):
            slot = list_ref[0, first + k]
            base = pl.multiple_of(slot * ROWS, 8)
            got = got_ref[pl.ds(base, ROWS), :]
            rows = [got[24 + m : 25 + m] for m in range(3)]
            pieces += rows
            ids = lanes([pltpu.roll(rows[m], 32 * (m + 1), 1) for m in range(3)] + [jnp.zeros_like(rows[0])])
            half_diag = jnp.where(
                lane1 < 80, pltpu.roll(got[27:28], 80, 1), pltpu.roll(got[28:29], 112, 1)
            )
            tail = jnp.where(
                lane8 < 32,
                pltpu.roll(got[0:8], 32, 1),
                jnp.where(lane8 < 64, pltpu.roll(got[8:16], 64, 1), pltpu.roll(got[16:24], 96, 1)),
            )
            full = jnp.concatenate([got, tail], axis=0)
            top = jnp.where(lane >= row, full, 0.0)
            bottom = jnp.where(
                lane == row + HALF,
                half_diag,
                jnp.where((lane >= HALF) & (lane < row + HALF), pltpu.roll(full, HALF, 1), 0.0),
            )
            high, low = split2(jnp.concatenate([top, bottom], axis=0))
            spread = lax.dot_general(
                jnp.concatenate([high, low], axis=0),
                onehot(ids),
                (((1,), (1,)), ((), ())),
                preferred_element_type=jnp.float32,
            ).astype(jnp.bfloat16)
            spread_ref[buf, NB * k : NB * k + NB, :] = spread[:NB]
            spread_ref[buf, NB * (GROUP + k) : NB * (GROUP + k) + NB, :] = spread[NB:]
        for t in range(3):
            moved = [
                pltpu.roll(pieces[4 * t + q], (32 * (q + 1)) % 128, 1) if q < 3 else pieces[4 * t + q]
                for q in range(4)
            ]
            place = onehot(lanes(moved))
            place_ref[buf, :, 128 * t : 128 * t + 128] = place
            place_ref[buf, :, 128 * (t + 3) : 128 * (t + 3) + 128] = place

    def absorb(buf):
        acc_ref[...] += jnp.dot(
            place_ref[buf], spread_ref[buf], preferred_element_type=jnp.float32
        )

    def step(g, carry):
        generate(0, g * 2 * GROUP)
        absorb(1)
        generate(1, g * 2 * GROUP + GROUP)
        absorb(0)
        return carry

    lax.fori_loop(0, (list_ref[1, 0] + 2 * GROUP - 1) // (2 * GROUP), step, 0)
    absorb(1)
    if not last:
        return
    a11, a22 = acc_ref[:half, :half], acc_ref[half:, half:]
    s11_ref[...] = a11 + a11.T
    s12 = acc_ref[:half, half:] + acc_ref[half:, :half].T
    s12_ref[...] = s12
    s22 = a22 + a22.T
    edge = half // 2
    row = lax.broadcasted_iota(jnp.int32, (edge, edge), 0)
    col = lax.broadcasted_iota(jnp.int32, (edge, edge), 1)
    last_part = s22[edge:, edge:]
    low_ref[:half, :half] = s12.T
    low_ref[:edge, half:] = s22[:edge, edge:]
    low_ref[edge:half, half:] = jnp.where(col >= row, s22[:edge, :edge], last_part)
    diag = jnp.sum(jnp.where(col == row, last_part, 0.0), axis=0, keepdims=True)
    low_ref[half:, :half] = jnp.zeros((8, half), jnp.float32)
    low_ref[half:, half:] = jnp.broadcast_to(diag, (8, edge))


def assemble(base, got, window, prev=None):
    slots = got.shape[0] // ROWS
    half = window // 2
    last = prev is not None
    square = jax.ShapeDtypeStruct((half, half), jnp.float32)
    whole = jax.ShapeDtypeStruct((window, window), jnp.float32)
    scratch = [
        pltpu.VMEM((2, window, 2 * NB * GROUP), jnp.bfloat16),
        pltpu.VMEM((2, 2 * NB * GROUP, window), jnp.bfloat16),
        pltpu.VMEM((8, slots), jnp.int32),
        pltpu.SMEM((8, slots), jnp.int32),
        pltpu.SemaphoreType.DMA,
    ]
    if last:
        scratch = [pltpu.VMEM((window, window), jnp.float32)] + scratch
    folded = jax.ShapeDtypeStruct((half + 8, half + half // 2), jnp.float32)
    out = (square, square, folded) if last else whole
    return pl.pallas_call(
        lambda *refs: assemble_kernel(last, *refs),
        out_shape=out,
        in_specs=[pl.BlockSpec(memory_space=pltpu.SMEM)]
        + [pl.BlockSpec(memory_space=pltpu.VMEM)] * (2 if last else 1),
        scratch_shapes=scratch,
        compiler_params=vmem(20),
        name="assemble_last" if last else "assemble_first",
    )(*((base, got, prev) if last else (base, got)))


def inverse_kernel(upper_ref, lower_ref, out_ref, mat_ref):
    size = upper_ref.shape[0]
    eye = jnp.where(
        lax.broadcasted_iota(jnp.int32, (size, size), 0)
        == lax.broadcasted_iota(jnp.int32, (size, size), 1),
        1.0,
        0.0,
    )
    edge = size // 2
    row = lax.broadcasted_iota(jnp.int32, (edge, edge), 0)
    col = lax.broadcasted_iota(jnp.int32, (edge, edge), 1)
    side = lower_ref[:edge, size:]
    both = lower_ref[edge:size, size:]
    above = jnp.where(col > row, both, 0.0)
    below = jnp.where(col < row, both, 0.0)
    first = jnp.where(col >= row, both, 0.0) + above.T
    second = below + below.T + jnp.where(col == row, lower_ref[size : size + 1, size:], 0.0)
    lower = jnp.concatenate(
        [
            jnp.concatenate([first, side], axis=1),
            jnp.concatenate([side.T, second], axis=1),
        ],
        axis=0,
    )
    mat = upper_ref[...] + lower + eye
    mat_ref[...] = mat
    norm = jnp.max(jnp.sum(jnp.abs(mat), axis=0, keepdims=True))
    out_ref[...] = eye * (2.0 / (norm + 1.0))

    def cond(state):
        turn, gap = state
        return (turn < 48) & (gap > 1e-8)

    def turn(state):
        now = out_ref[...]
        miss = eye - jnp.dot(mat_ref[...], now, precision=HI, preferred_element_type=jnp.float32)
        out_ref[...] = now + jnp.dot(now, miss, precision=HI, preferred_element_type=jnp.float32)
        return state[0] + 1, jnp.sum(miss * miss)

    lax.while_loop(cond, turn, (0, jnp.float32(1.0)))


def invert(upper, lower):
    return pl.pallas_call(
        inverse_kernel,
        out_shape=jax.ShapeDtypeStruct(upper.shape, jnp.float32),
        scratch_shapes=[pltpu.VMEM(upper.shape, jnp.float32)],
        compiler_params=vmem(8),
        name="invert",
    )(upper, lower)


def mm(left, right):
    return jnp.dot(left, right, precision=HI, preferred_element_type=jnp.float32)


def left3(x):
    high, low = split2(x)
    return jnp.concatenate([high, high, low], axis=1)


def right3(x):
    high, low = split2(x)
    return jnp.concatenate([high, low, high], axis=0)


def dot3(left, right):
    return jnp.dot(left, right, preferred_element_type=jnp.float32)


def at_row(k, value):
    row = lax.broadcasted_iota(jnp.int32, (8, value.shape[1]), 0)
    return jnp.where(row == k, value, 0.0)


def sums_of(left, right):
    return jnp.sum(left * right, axis=0, keepdims=True)


BLOCK = 512


def in_blocks(kernel, matrices, wholes, lefts, rights, sums, outs, kept):
    rows = matrices[-1].shape[0]
    total = wholes[0].shape[1] if wholes else 2 * lefts[0].shape[1]
    per = total // 2 // BLOCK
    maps = {
        "whole": lambda j: (0, j),
        "left": lambda j: (0, jnp.minimum(j, per - 1)),
        "right": lambda j: (0, jnp.maximum(j - per, 0)),
        "sums": lambda j: (0, j),
    }
    shapes = {
        "whole": (rows, total),
        "left": (rows, total // 2),
        "right": (rows, total // 2),
        "sums": (8, total),
    }

    def spec(kind, height):
        return pl.BlockSpec((height, BLOCK), maps[kind])

    ins = [("whole", x) for x in wholes] + [("left", x) for x in lefts]
    ins += [("right", x) for x in rights] + [("sums", x) for x in sums]

    def run(*refs):
        mats, mid, three = refs[: len(matrices)], refs[len(matrices) : -1], refs[-1]
        kernel(pl.program_id(0), per, mats, three, *mid)

    return pl.pallas_call(
        run,
        grid=(2 * per,),
        in_specs=[pl.BlockSpec((rows, rows), lambda j: (0, 0)) for x in matrices]
        + [spec(kind, x.shape[0]) for kind, x in ins],
        out_specs=tuple(spec(kind, shapes[kind][0]) for kind in outs),
        out_shape=tuple(jax.ShapeDtypeStruct(shapes[kind], jnp.float32) for kind in outs),
        scratch_shapes=[pltpu.VMEM((kept, rows, 3 * rows), jnp.bfloat16)],
        compiler_params=vmem(24),
    )(*matrices, *(x for _, x in ins))


def keep(step, mats, three):
    @pl.when(step == 0)
    def _():
        for k, mat in enumerate(mats):
            three[k] = left3(mat[...])


def first_kernel(step, per, mats, three, low0, high0, low1, high1, v_ref, w_ref, m_ref):
    low, high, inv, inv_low, inv_high = mats

    @pl.when(step == 0)
    def _():
        three[0] = left3(mm(low[...], inv_low[...]))
        three[1] = left3(mm(high[...], inv_high[...]))
        three[2] = left3(inv[...])

    x_low = jnp.concatenate([low0[...], low1[...]], axis=0)
    x_high = jnp.concatenate([high0[...], high1[...]], axis=0)
    v = dot3(three[0], right3(x_low)) + dot3(three[1], right3(x_high))
    w = dot3(three[2], right3(v))
    v_ref[...] = v
    w_ref[...] = w
    m_ref[...] = at_row(2, sums_of(v, w))


def start_kernel(step, per, mats, three, v0, v1, m_in, w_ref, m_ref):
    keep(step, mats, three)
    w = dot3(three[0], right3(v0[...]))
    w_ref[...] = w
    m_ref[...] = m_in[...] + at_row(0, sums_of(v0[...], w)) + at_row(1, sums_of(v1[...], w))


def second_kernel(
    step, per, mats, three, x_low, x_high, w1, m_in, v_ref, left_ref, right_ref, m_ref
):
    keep(step, mats, three)
    v = dot3(three[0], right3(x_low[...])) + dot3(three[1], right3(x_high[...]))
    w = dot3(three[2], right3(v))
    v_ref[...] = v
    m_ref[...] = m_in[...] + at_row(3, sums_of(v, w1[...])) + at_row(4, sums_of(v, w))

    @pl.when(step < per)
    def _():
        left_ref[...] = w

    @pl.when(step >= per)
    def _():
        right_ref[...] = w


def side_kernel(step, per, mats, three, w_left, x_high, w_right, x_low, m_in, t_ref, m_ref):
    keep(step, mats, three)
    left = step < per
    x = jnp.where(left, x_high[...], x_low[...])
    w = jnp.where(left, w_left[...], w_right[...])
    t = dot3(three[jnp.where(left, 1, 0)], right3(x))
    t_ref[...] = t
    m_ref[...] = m_in[...] + at_row(5, 2.0 * sums_of(t, w))


def safe(num, den):
    return jnp.where(den > 0, num / jnp.where(den > 0, den, 1.0), 0.0)


def coefficients(mu):
    m0, m1, m2, m3, m4, m5 = mu
    l1, l2 = safe(m1, m0), safe(m2, m0)
    d1 = m2 - l1 * m1
    e = m3 - l1 * m2
    l21 = safe(e, d1)
    d2 = m4 - l2 * m2 - l21 * e
    y0 = -m3
    y1 = -m4 - l1 * y0
    y2 = -m5 - l2 * y0 - l21 * y1
    b2 = safe(y2, d2)
    b1 = safe(y1, d1) - l21 * b2
    b0 = safe(y0, m0) - l1 * b1 - l2 * b2
    scale = 1.0 / (b0 - b1 + b2 - 1.0)
    c0, c1, c2, c3 = b0 * scale, b1 * scale, b2 * scale, scale
    return (1.0 - c0, c3 - c2, -c3), (c0, c1, c2, c3)


def finish_kernel(
    step, per, mats, three, v0, w0, v1, w1, v2, t, w_left, x_low, w_right, x_high, sums, sol, res
):
    keep(step, mats, three)
    left = step < per
    far = jnp.where(left, x_low[...], x_high[...])
    w2 = jnp.where(left, w_left[...], w_right[...])
    v3 = t[...] + dot3(three[jnp.where(left, 0, 1)], right3(far))
    x, c = coefficients([sums[k : k + 1, :] for k in range(6)])
    sol[...] = x[0] * w0[...] + x[1] * w1[...] + x[2] * w2
    res[...] = c[0] * v0[...] + c[1] * v1[...] + c[2] * v2[...] + c[3] * v3


def butterfly(x, devices):
    for bit in (16, 32, 96, 4, 12, 1, 3):
        x = x + lax.ppermute(x, AXES, [(i, i ^ bit) for i in range(devices)])
    return x


def body(blocks, connect, owner_map, right_side):
    devices = lax.axis_size(AXES)
    own = right_side.shape[0]
    window = 2 * own
    up = [(i, (i + 1) % devices) for i in range(devices)]
    down = [(b, a) for a, b in up]

    def from_below(x):
        return lax.ppermute(x, AXES, up)

    def from_above(x):
        return lax.ppermute(x, AXES, down)

    base = jnp.stack([lax.axis_index(AXES) * own, own * devices]).astype(jnp.int32)
    r_low, r_high = {}, {}
    start = right_side[: own // 2]
    r_low[0] = from_below(start)
    r_high[0] = from_above(start)
    send0, send1 = pack(owner_map, connect.T, blocks, devices)

    def exchange(send):
        got = lax.all_to_all(
            send.reshape(devices, ROWS, 128), AXES, split_axis=0, concat_axis=0, tiled=True
        )
        return got.reshape(devices * ROWS, 128)

    got0 = exchange(send0)
    got1 = exchange(send1)
    rest, got0 = lax.optimization_barrier((right_side, got0))
    rest = rest[own // 2 :]
    r_high[1] = from_above(rest)
    part = assemble(base, got0, window)
    center, high_band, lower = assemble(base, got1, window, part)
    lower, rest = lax.optimization_barrier((lower, rest))
    lower = from_below(lower)
    r_low[1] = from_below(rest)
    inv = invert(center, lower)
    inv_low, inv_high = from_below(inv), from_above(inv)
    v0 = right_side
    v1, w1, sums = in_blocks(
        first_kernel,
        (lower, high_band, inv, inv_low, inv_high),
        (r_low[0], r_high[0], r_low[1], r_high[1]),
        (),
        (),
        (),
        ("whole", "whole", "sums"),
        3,
    )
    w1_low, w1_high = from_below(w1), from_above(w1)
    w0, sums = in_blocks(start_kernel, (inv,), (v0, v1), (), (), (sums,), ("whole", "sums"), 1)
    v2, w2_0, w2_1, sums = in_blocks(
        second_kernel,
        (lower, high_band, inv),
        (w1_low, w1_high, w1),
        (),
        (),
        (sums,),
        ("whole", "left", "right", "sums"),
        3,
    )
    near_0 = from_above(w2_0)
    near_1 = from_below(w2_1)
    far_0 = from_below(w2_0)
    far_1 = from_above(w2_1)
    bands = (lower, high_band)
    t, sums = in_blocks(
        side_kernel, bands, (), (w2_0, near_0), (w2_1, near_1), (sums,), ("whole", "sums"), 2
    )
    sums = butterfly(sums, devices)
    return in_blocks(
        finish_kernel,
        bands,
        (v0, w0, v1, w1, v2, t),
        (w2_0, far_0),
        (w2_1, far_1),
        (sums,),
        ("whole", "whole"),
        2,
    )


def solution(mesh):
    both = P(AXES, None)
    return jax.shard_map(
        body,
        mesh=mesh,
        in_specs=(both, both, P(AXES), both),
        out_specs=(both, both),
        check_vma=False,
    )
```

```python
import jax
import jax.numpy as jnp
from jax import lax
from jax.experimental import pallas as pl
from jax.experimental.pallas import tpu as pltpu
from jax.sharding import PartitionSpec as P


AXES = ("row", "col")
NB = 96
HALF = 48
ROWS = 40
GROUP = 4
HI = lax.Precision.HIGHEST


def vmem(mib):
    return pltpu.CompilerParams(vmem_limit_bytes=mib * 1024 * 1024)


def split2(x):
    high = x.astype(jnp.bfloat16)
    low = (x - high.astype(jnp.float32)).astype(jnp.bfloat16)
    return high, low


def pack_kernel(owner_ref, ids_ref, blocks_ref, out0_ref, out1_ref, tail_ref, x_ref, sem):
    subs = x_ref.shape[0]
    devs = out0_ref.shape[0] // ROWS
    sub = lax.broadcasted_iota(jnp.int32, (devs, subs), 0)
    here = sub == owner_ref[...]
    before = lax.broadcasted_iota(jnp.int32, (subs, subs), 0) < lax.broadcasted_iota(
        jnp.int32, (subs, subs), 1
    )
    count = jnp.dot(
        here.astype(jnp.bfloat16), before.astype(jnp.bfloat16), preferred_element_type=jnp.float32
    )
    first = jnp.where(here & (count < 0.5), 1.0, 0.0).astype(jnp.bfloat16)
    second = jnp.where(here & (count > 0.5), 1.0, 0.0).astype(jnp.bfloat16)
    pick = jnp.concatenate([first, second], axis=0)
    ids = ids_ref[...].astype(jnp.float32).T + 1.0
    ids = jnp.concatenate([ids, jnp.zeros((subs, 128 - NB), jnp.float32)], axis=1)
    pick = jnp.concatenate([pick, pick], axis=1)
    lane = lax.broadcasted_iota(jnp.int32, (subs, 128), 1)

    part = 12 * NB
    upper = HALF * NB
    copies = []
    for q in range(8):
        begin = (3 - q // 2) * part + (q % 2) * upper
        there = pl.ds(begin, part)
        copies.append(pltpu.make_async_copy(blocks_ref.at[:, there], x_ref.at[:, there], sem.at[q]))
        copies[-1].start()
    waited = [0]

    def arrive(i):
        needed = 2 * (4 - i // 12)
        while waited[0] < needed:
            copies[waited[0]].wait()
            waited[0] += 1

    def flat(start, need):
        tile, off = divmod(start, 128)
        if off == 0:
            return x_ref[:, tile * 128 : tile * 128 + 128]
        one = pltpu.roll(x_ref[:, tile * 128 : tile * 128 + 128], 128 - off, 1)
        if off + need <= 128:
            return one
        two = pltpu.roll(x_ref[:, tile * 128 + 128 : tile * 128 + 256], 128 - off, 1)
        return jnp.where(lane < 128 - off, one, two)

    diag = jnp.zeros((subs, 128), jnp.float32)

    def wrow(i, diag):
        arrive(i)
        top = flat(NB * i, NB)
        bottom = flat(NB * (i + HALF) + HALF, HALF)
        row = jnp.where(lane < i, bottom, jnp.where(lane == i, 0.5 * top, top))
        return row, jnp.where(lane == i, 0.5 * bottom, diag)

    for m in range(8):
        row, diag = wrow(ROWS + m, diag)
        tail_ref[m] = row
    order = [i for i in range(ROWS - 2, -2, -2) if i not in (26, 28)] + [26, 28]
    kept = {}
    for i0 in order:
        tiles = []
        if i0 == 26:
            for i in (26, 27, 28, 29):
                kept[i], diag = wrow(i, diag)
        for i in (i0, i0 + 1):
            if i in kept:
                row = kept[i]
            else:
                row, diag = wrow(i, diag)
            if i < 24:
                extra = pltpu.roll(tail_ref[i % 8], 96 - 32 * (i // 8), 1)
            elif i < 27:
                extra = pltpu.roll(ids, 96 - 32 * (i - 24), 1)
            elif i < 29:
                extra = pltpu.roll(diag, 96 - 32 * (i - 27), 1)
            else:
                extra = jnp.zeros_like(row)
            tiles.append(jnp.where(lane < NB, row, extra))
        high, low = split2(jnp.concatenate(tiles, axis=1))
        out = jnp.dot(
            pick, jnp.concatenate([high, low], axis=0), preferred_element_type=jnp.float32
        )
        for k in range(2):
            part = out[:, 128 * k : 128 * k + 128]
            out0_ref[pl.ds(i0 + k, devs, stride=ROWS), :] = part[:devs]
            out1_ref[pl.ds(i0 + k, devs, stride=ROWS), :] = part[devs:]


def pack(owner_map, ids, blocks, devices):
    shape = jax.ShapeDtypeStruct((devices * ROWS, 128), jnp.float32)
    return pl.pallas_call(
        pack_kernel,
        out_shape=(shape, shape),
        in_specs=[
            pl.BlockSpec(memory_space=pltpu.VMEM),
            pl.BlockSpec(memory_space=pltpu.VMEM),
            pl.BlockSpec(memory_space=pl.ANY),
        ],
        scratch_shapes=[
            pltpu.VMEM((8, blocks.shape[0], 128), jnp.float32),
            pltpu.VMEM(blocks.shape, jnp.float32),
            pltpu.SemaphoreType.DMA((8,)),
        ],
        compiler_params=vmem(24),
        name="pack",
    )(owner_map.reshape(1, -1), ids, blocks)


def assemble_kernel(last, base_ref, got_ref, *refs):
    place_ref, spread_ref, vec_ref, list_ref, sem = refs[-5:]
    if last:
        prev_ref, s11_ref, s12_ref, low_ref, acc_ref = refs[:5]
    else:
        acc_ref = refs[0]
    window = acc_ref.shape[0]
    half = window // 2
    slots = got_ref.shape[0] // ROWS
    lane = lax.broadcasted_iota(jnp.int32, (slots, slots), 1)
    sub = lax.broadcasted_iota(jnp.int32, (slots, slots), 0)
    filled = got_ref[pl.ds(24, slots, stride=ROWS), :][:, NB : NB + 1] > 0.5
    filled = jnp.broadcast_to(jnp.where(filled, 1.0, 0.0), (slots, slots))
    rank = jnp.dot(
        jnp.where(lane < sub, 1.0, 0.0).astype(jnp.bfloat16),
        filled.astype(jnp.bfloat16),
        preferred_element_type=jnp.float32,
    )
    subf = sub.astype(jnp.float32)
    hit = (filled > 0.5) & (rank == lane.astype(jnp.float32))
    count = jnp.sum(filled, axis=0, keepdims=True)
    spare = jnp.max(jnp.where(filled > 0.5, 0.0, subf), axis=0, keepdims=True)
    chosen = jnp.sum(jnp.where(hit, subf, 0.0), axis=0, keepdims=True)
    chosen = jnp.where(lane[:1].astype(jnp.float32) < count, chosen, spare)
    first_row = lax.broadcasted_iota(jnp.int32, (8, slots), 0) == 0
    vec_ref[...] = jnp.where(first_row, chosen, count).astype(jnp.int32)
    copy = pltpu.make_async_copy(vec_ref, list_ref, sem)
    copy.start()
    acc_ref[...] = prev_ref[...] if last else jnp.zeros_like(acc_ref)
    place_ref[1] = jnp.zeros(place_ref.shape[1:], jnp.bfloat16)
    spread_ref[1] = jnp.zeros(spread_ref.shape[1:], jnp.bfloat16)
    copy.wait()

    lane = lax.broadcasted_iota(jnp.int32, (HALF, 128), 1)
    row = lax.broadcasted_iota(jnp.int32, (HALF, 128), 0)
    lane1 = lax.broadcasted_iota(jnp.int32, (1, 128), 1)
    lane8 = lax.broadcasted_iota(jnp.int32, (8, 128), 1)
    target = lax.broadcasted_iota(jnp.int32, (window, 128), 0).astype(jnp.float32)
    start = base_ref[0].astype(jnp.float32)
    total = base_ref[1].astype(jnp.float32)

    def local(ids):
        moved = ids - 1.0 - start
        return jnp.where(ids > 0.5, jnp.where(moved < 0.0, moved + total, moved), -1.0)


    def lanes(pieces):
        out = pieces[3]
        for k in (2, 1, 0):
            out = jnp.where(lane1 < 32 * (k + 1), pieces[k], out)
        return out

    def onehot(ids):
        return jnp.where(target == local(ids), 1.0, 0.0).astype(jnp.bfloat16)

    def generate(buf, first):
        pieces = []
        for k in range(GROUP):
            slot = list_ref[0, first + k]
            base = pl.multiple_of(slot * ROWS, 8)
            got = got_ref[pl.ds(base, ROWS), :]
            rows = [got[24 + m : 25 + m] for m in range(3)]
            pieces += rows
            ids = lanes([pltpu.roll(rows[m], 32 * (m + 1), 1) for m in range(3)] + [jnp.zeros_like(rows[0])])
            half_diag = jnp.where(
                lane1 < 80, pltpu.roll(got[27:28], 80, 1), pltpu.roll(got[28:29], 112, 1)
            )
            tail = jnp.where(
                lane8 < 32,
                pltpu.roll(got[0:8], 32, 1),
                jnp.where(lane8 < 64, pltpu.roll(got[8:16], 64, 1), pltpu.roll(got[16:24], 96, 1)),
            )
            full = jnp.concatenate([got, tail], axis=0)
            top = jnp.where(lane >= row, full, 0.0)
            bottom = jnp.where(
                lane == row + HALF,
                half_diag,
                jnp.where((lane >= HALF) & (lane < row + HALF), pltpu.roll(full, HALF, 1), 0.0),
            )
            high, low = split2(jnp.concatenate([top, bottom], axis=0))
            spread = lax.dot_general(
                jnp.concatenate([high, low], axis=0),
                onehot(ids),
                (((1,), (1,)), ((), ())),
                preferred_element_type=jnp.float32,
            ).astype(jnp.bfloat16)
            spread_ref[buf, NB * k : NB * k + NB, :] = spread[:NB]
            spread_ref[buf, NB * (GROUP + k) : NB * (GROUP + k) + NB, :] = spread[NB:]
        for t in range(3):
            moved = [
                pltpu.roll(pieces[4 * t + q], (32 * (q + 1)) % 128, 1) if q < 3 else pieces[4 * t + q]
                for q in range(4)
            ]
            place = onehot(lanes(moved))
            place_ref[buf, :, 128 * t : 128 * t + 128] = place
            place_ref[buf, :, 128 * (t + 3) : 128 * (t + 3) + 128] = place

    def absorb(buf):
        acc_ref[...] += jnp.dot(
            place_ref[buf], spread_ref[buf], preferred_element_type=jnp.float32
        )

    def step(g, carry):
        generate(0, g * 2 * GROUP)
        absorb(1)
        generate(1, g * 2 * GROUP + GROUP)
        absorb(0)
        return carry

    lax.fori_loop(0, (list_ref[1, 0] + 2 * GROUP - 1) // (2 * GROUP), step, 0)
    absorb(1)
    if not last:
        return
    a11, a22 = acc_ref[:half, :half], acc_ref[half:, half:]
    s11_ref[...] = a11 + a11.T
    s12 = acc_ref[:half, half:] + acc_ref[half:, :half].T
    s12_ref[...] = s12
    s22 = a22 + a22.T
    edge = half // 2
    row = lax.broadcasted_iota(jnp.int32, (edge, edge), 0)
    col = lax.broadcasted_iota(jnp.int32, (edge, edge), 1)
    last_part = s22[edge:, edge:]
    low_ref[:half, :half] = s12.T
    low_ref[:edge, half:] = s22[:edge, edge:]
    low_ref[edge:half, half:] = jnp.where(col >= row, s22[:edge, :edge], last_part)
    diag = jnp.sum(jnp.where(col == row, last_part, 0.0), axis=0, keepdims=True)
    low_ref[half:, :half] = jnp.zeros((8, half), jnp.float32)
    low_ref[half:, half:] = jnp.broadcast_to(diag, (8, edge))


def assemble(base, got, window, prev=None):
    slots = got.shape[0] // ROWS
    half = window // 2
    last = prev is not None
    square = jax.ShapeDtypeStruct((half, half), jnp.float32)
    whole = jax.ShapeDtypeStruct((window, window), jnp.float32)
    scratch = [
        pltpu.VMEM((2, window, 2 * NB * GROUP), jnp.bfloat16),
        pltpu.VMEM((2, 2 * NB * GROUP, window), jnp.bfloat16),
        pltpu.VMEM((8, slots), jnp.int32),
        pltpu.SMEM((8, slots), jnp.int32),
        pltpu.SemaphoreType.DMA,
    ]
    if last:
        scratch = [pltpu.VMEM((window, window), jnp.float32)] + scratch
    folded = jax.ShapeDtypeStruct((half + 8, half + half // 2), jnp.float32)
    out = (square, square, folded) if last else whole
    return pl.pallas_call(
        lambda *refs: assemble_kernel(last, *refs),
        out_shape=out,
        in_specs=[pl.BlockSpec(memory_space=pltpu.SMEM)]
        + [pl.BlockSpec(memory_space=pltpu.VMEM)] * (2 if last else 1),
        scratch_shapes=scratch,
        compiler_params=vmem(20),
        name="assemble_last" if last else "assemble_first",
    )(*((base, got, prev) if last else (base, got)))


def inverse_kernel(upper_ref, lower_ref, out_ref, mat_ref):
    size = upper_ref.shape[0]
    eye = jnp.where(
        lax.broadcasted_iota(jnp.int32, (size, size), 0)
        == lax.broadcasted_iota(jnp.int32, (size, size), 1),
        1.0,
        0.0,
    )
    edge = size // 2
    row = lax.broadcasted_iota(jnp.int32, (edge, edge), 0)
    col = lax.broadcasted_iota(jnp.int32, (edge, edge), 1)
    side = lower_ref[:edge, size:]
    both = lower_ref[edge:size, size:]
    above = jnp.where(col > row, both, 0.0)
    below = jnp.where(col < row, both, 0.0)
    first = jnp.where(col >= row, both, 0.0) + above.T
    second = below + below.T + jnp.where(col == row, lower_ref[size : size + 1, size:], 0.0)
    lower = jnp.concatenate(
        [
            jnp.concatenate([first, side], axis=1),
            jnp.concatenate([side.T, second], axis=1),
        ],
        axis=0,
    )
    mat = upper_ref[...] + lower + eye
    mat_ref[...] = mat
    norm = jnp.max(jnp.sum(jnp.abs(mat), axis=0, keepdims=True))
    out_ref[...] = eye * (2.0 / (norm + 1.0))

    def cond(state):
        turn, gap = state
        return (turn < 48) & (gap > 1e-8)

    def turn(state):
        now = out_ref[...]
        miss = eye - jnp.dot(mat_ref[...], now, precision=HI, preferred_element_type=jnp.float32)
        out_ref[...] = now + jnp.dot(now, miss, precision=HI, preferred_element_type=jnp.float32)
        return state[0] + 1, jnp.sum(miss * miss)

    lax.while_loop(cond, turn, (0, jnp.float32(1.0)))


def invert(upper, lower):
    return pl.pallas_call(
        inverse_kernel,
        out_shape=jax.ShapeDtypeStruct(upper.shape, jnp.float32),
        scratch_shapes=[pltpu.VMEM(upper.shape, jnp.float32)],
        compiler_params=vmem(8),
        name="invert",
    )(upper, lower)


def mm(left, right):
    return jnp.dot(left, right, precision=HI, preferred_element_type=jnp.float32)


def left3(x):
    high, low = split2(x)
    return jnp.concatenate([high, high, low], axis=1)


def right3(x):
    high, low = split2(x)
    return jnp.concatenate([high, low, high], axis=0)


def dot3(left, right):
    return jnp.dot(left, right, preferred_element_type=jnp.float32)


def at_row(k, value):
    row = lax.broadcasted_iota(jnp.int32, (8, value.shape[1]), 0)
    return jnp.where(row == k, value, 0.0)


def sums_of(left, right):
    return jnp.sum(left * right, axis=0, keepdims=True)


BLOCK = 512


def in_blocks(kernel, matrices, wholes, lefts, rights, sums, outs, kept):
    rows = matrices[-1].shape[0]
    total = wholes[0].shape[1] if wholes else 2 * lefts[0].shape[1]
    per = total // 2 // BLOCK
    maps = {
        "whole": lambda j: (0, j),
        "left": lambda j: (0, jnp.minimum(j, per - 1)),
        "right": lambda j: (0, jnp.maximum(j - per, 0)),
        "sums": lambda j: (0, j),
    }
    shapes = {
        "whole": (rows, total),
        "left": (rows, total // 2),
        "right": (rows, total // 2),
        "sums": (8, total),
    }

    def spec(kind, height):
        return pl.BlockSpec((height, BLOCK), maps[kind])

    ins = [("whole", x) for x in wholes] + [("left", x) for x in lefts]
    ins += [("right", x) for x in rights] + [("sums", x) for x in sums]

    def run(*refs):
        mats, mid, three = refs[: len(matrices)], refs[len(matrices) : -1], refs[-1]
        kernel(pl.program_id(0), per, mats, three, *mid)

    return pl.pallas_call(
        run,
        grid=(2 * per,),
        in_specs=[pl.BlockSpec((rows, rows), lambda j: (0, 0)) for x in matrices]
        + [spec(kind, x.shape[0]) for kind, x in ins],
        out_specs=tuple(spec(kind, shapes[kind][0]) for kind in outs),
        out_shape=tuple(jax.ShapeDtypeStruct(shapes[kind], jnp.float32) for kind in outs),
        scratch_shapes=[pltpu.VMEM((kept, rows, 3 * rows), jnp.bfloat16)],
        compiler_params=vmem(24),
    )(*matrices, *(x for _, x in ins))


def keep(step, mats, three):
    @pl.when(step == 0)
    def _():
        for k, mat in enumerate(mats):
            three[k] = left3(mat[...])


def first_kernel(step, per, mats, three, low0, high0, low1, high1, v_ref, w_ref, m_ref):
    low, high, inv, inv_low, inv_high = mats

    @pl.when(step == 0)
    def _():
        three[0] = left3(mm(low[...], inv_low[...]))
        three[1] = left3(mm(high[...], inv_high[...]))
        three[2] = left3(inv[...])

    x_low = jnp.concatenate([low0[...], low1[...]], axis=0)
    x_high = jnp.concatenate([high0[...], high1[...]], axis=0)
    v = dot3(three[0], right3(x_low)) + dot3(three[1], right3(x_high))
    w = dot3(three[2], right3(v))
    v_ref[...] = v
    w_ref[...] = w
    m_ref[...] = at_row(2, sums_of(v, w))


def start_kernel(step, per, mats, three, v0, v1, m_in, w_ref, m_ref):
    keep(step, mats, three)
    w = dot3(three[0], right3(v0[...]))
    w_ref[...] = w
    m_ref[...] = m_in[...] + at_row(0, sums_of(v0[...], w)) + at_row(1, sums_of(v1[...], w))


def second_kernel(
    step, per, mats, three, x_low, x_high, w1, m_in, v_ref, left_ref, right_ref, m_ref
):
    keep(step, mats, three)
    v = dot3(three[0], right3(x_low[...])) + dot3(three[1], right3(x_high[...]))
    w = dot3(three[2], right3(v))
    v_ref[...] = v
    m_ref[...] = m_in[...] + at_row(3, sums_of(v, w1[...])) + at_row(4, sums_of(v, w))

    @pl.when(step < per)
    def _():
        left_ref[...] = w

    @pl.when(step >= per)
    def _():
        right_ref[...] = w


def side_kernel(step, per, mats, three, w_left, x_high, w_right, x_low, m_in, t_ref, m_ref):
    keep(step, mats, three)
    left = step < per
    x = jnp.where(left, x_high[...], x_low[...])
    w = jnp.where(left, w_left[...], w_right[...])
    t = dot3(three[jnp.where(left, 1, 0)], right3(x))
    t_ref[...] = t
    m_ref[...] = m_in[...] + at_row(5, 2.0 * sums_of(t, w))


def safe(num, den):
    return jnp.where(den > 0, num / jnp.where(den > 0, den, 1.0), 0.0)


def coefficients(mu):
    m0, m1, m2, m3, m4, m5 = mu
    l1, l2 = safe(m1, m0), safe(m2, m0)
    d1 = m2 - l1 * m1
    e = m3 - l1 * m2
    l21 = safe(e, d1)
    d2 = m4 - l2 * m2 - l21 * e
    y0 = -m3
    y1 = -m4 - l1 * y0
    y2 = -m5 - l2 * y0 - l21 * y1
    b2 = safe(y2, d2)
    b1 = safe(y1, d1) - l21 * b2
    b0 = safe(y0, m0) - l1 * b1 - l2 * b2
    scale = 1.0 / (b0 - b1 + b2 - 1.0)
    c0, c1, c2, c3 = b0 * scale, b1 * scale, b2 * scale, scale
    return (1.0 - c0, c3 - c2, -c3), (c0, c1, c2, c3)


def finish_kernel(
    step, per, mats, three, v0, w0, v1, w1, v2, t, w_left, x_low, w_right, x_high, sums, sol, res
):
    keep(step, mats, three)
    left = step < per
    far = jnp.where(left, x_low[...], x_high[...])
    w2 = jnp.where(left, w_left[...], w_right[...])
    v3 = t[...] + dot3(three[jnp.where(left, 0, 1)], right3(far))
    x, c = coefficients([sums[k : k + 1, :] for k in range(6)])
    sol[...] = x[0] * w0[...] + x[1] * w1[...] + x[2] * w2
    res[...] = c[0] * v0[...] + c[1] * v1[...] + c[2] * v2[...] + c[3] * v3


def butterfly(x, devices):
    for bit in (16, 32, 96, 4, 12, 1, 3):
        x = x + lax.ppermute(x, AXES, [(i, i ^ bit) for i in range(devices)])
    return x


def body(blocks, connect, owner_map, right_side):
    devices = lax.axis_size(AXES)
    own = right_side.shape[0]
    window = 2 * own
    up = [(i, (i + 1) % devices) for i in range(devices)]
    down = [(b, a) for a, b in up]

    def from_below(x):
        return lax.ppermute(x, AXES, up)

    def from_above(x):
        return lax.ppermute(x, AXES, down)

    base = jnp.stack([lax.axis_index(AXES) * own, own * devices]).astype(jnp.int32)
    r_low, r_high = {}, {}
    start = right_side[: own * 5 // 8]
    r_low[0] = from_below(start)
    r_high[0] = from_above(start)
    send0, send1 = pack(owner_map, connect.T, blocks, devices)

    def exchange(send):
        got = lax.all_to_all(
            send.reshape(devices, ROWS, 128), AXES, split_axis=0, concat_axis=0, tiled=True
        )
        return got.reshape(devices * ROWS, 128)

    got0 = exchange(send0)
    got1 = exchange(send1)
    rest, got0 = lax.optimization_barrier((right_side, got0))
    rest = rest[own * 5 // 8 :]
    r_low[1], r_high[1] = from_below(rest), from_above(rest)
    part = assemble(base, got0, window)
    center, high_band, lower = assemble(base, got1, window, part)
    lower = from_below(lower)
    inv = invert(center, lower)
    inv_low, inv_high = from_below(inv), from_above(inv)
    v0 = right_side
    v1, w1, sums = in_blocks(
        first_kernel,
        (lower, high_band, inv, inv_low, inv_high),
        (r_low[0], r_high[0], r_low[1], r_high[1]),
        (),
        (),
        (),
        ("whole", "whole", "sums"),
        3,
    )
    w1_low, w1_high = from_below(w1), from_above(w1)
    w0, sums = in_blocks(start_kernel, (inv,), (v0, v1), (), (), (sums,), ("whole", "sums"), 1)
    v2, w2_0, w2_1, sums = in_blocks(
        second_kernel,
        (lower, high_band, inv),
        (w1_low, w1_high, w1),
        (),
        (),
        (sums,),
        ("whole", "left", "right", "sums"),
        3,
    )
    near_0 = from_above(w2_0)
    near_1 = from_below(w2_1)
    far_0 = from_below(w2_0)
    far_1 = from_above(w2_1)
    bands = (lower, high_band)
    t, sums = in_blocks(
        side_kernel, bands, (), (w2_0, near_0), (w2_1, near_1), (sums,), ("whole", "sums"), 2
    )
    sums = butterfly(sums, devices)
    return in_blocks(
        finish_kernel,
        bands,
        (v0, w0, v1, w1, v2, t),
        (w2_0, far_0),
        (w2_1, far_1),
        (sums,),
        ("whole", "whole"),
        2,
    )


def solution(mesh):
    both = P(AXES, None)
    return jax.shard_map(
        body,
        mesh=mesh,
        in_specs=(both, both, P(AXES), both),
        out_specs=(both, both),
        check_vma=False,
    )
```
